128 devices in a mesh: model: 16 (over z, y), data: 8 (over x, core).
Axes of the slice: x: 4, y: 4, z: 4, core: 2. Of those that a mesh axis runs over, the one named last changes fastest.
Arguments:
- grad_in: bfloat16 [8, 24, 512, 2048], P('data', None, None, 'model')
- w_in: float32 [24, 512, 2048], P(None, 'data', 'model')
- row_in: float32 [24, 512], P(None, 'data')
- col_in: float32 [24, 2048], P(None, 'model')
- grad_out: bfloat16 [8, 12, 2048, 512], P('data', None, 'model')
- w_out: float32 [12, 2048, 512], P(None, 'model', 'data')
- row_out: float32 [12, 2048], P(None, 'model')
- col_out: float32 [12, 512], P(None, 'data')
- grad_qkv: bfloat16 [8, 54, 512, 512], P('data', None, None, 'model')
- w_qkv: float32 [54, 512, 512], P(None, 'data', 'model')
- row_qkv: float32 [54, 512], P(None, 'data')
- col_qkv: float32 [54, 512], P(None, 'model')
- grad_o: bfloat16 [8, 18, 512, 512], P('data', None, 'model')
- w_o: float32 [18, 512, 512], P(None, 'model', 'data')
- row_o: float32 [18, 512], P(None, 'model')
- col_o: float32 [18, 512], P(None, 'data')
Outputs:
- output 1: float32 [24, 512, 2048], P(None, 'data', 'model')
- output 2: float32 [24, 512], P(None, 'data')
- output 3: float32 [24, 2048], P(None, 'model')
- output 4: float32 [12, 2048, 512], P(None, 'model', 'data')
- output 5: float32 [12, 2048], P(None, 'model')
- output 6: float32 [12, 512], P(None, 'data')
- output 7: float32 [54, 512, 512], P(None, 'data', 'model')
- output 8: float32 [54, 512], P(None, 'data')
- output 9: float32 [54, 512], P(None, 'model')
- output 10: float32 [18, 512, 512], P(None, 'model', 'data')
- output 11: float32 [18, 512], P(None, 'model')
- output 12: float32 [18, 512], P(None, 'data')
All inputs are finite; a program needn't handle non-finite values.
Results may differ from the reference program's by a relative error of at most 0.001.
Values sent between devices are 32-bit elements.
A program may use at most 1 GiB of HBM per device.

```python
import jax
import jax.numpy as jnp
from jax import lax

D = 512
FF = 2048
HEADS = 8
HEAD = 64
LAYERS = 6
DATA_RANKS = 8
OPT_STEP = 4

ATTN_WIDTH = HEADS * HEAD
MATS_IN = 4 * LAYERS
MATS_OUT = 2 * LAYERS
MATS_QKV = 9 * LAYERS
MATS_O = 3 * LAYERS
EPS_SQ = 1e-30
BETA_TWO = 1.0 - OPT_STEP ** -0.8
LR_BASE = min(1e-2, OPT_STEP ** -0.5)


def draw_group(key, count, rows, cols):
    sub_keys = jax.random.split(key, 8)
    row_scale = jnp.exp(jax.random.uniform(sub_keys[0], (count, rows), minval=-1.0, maxval=1.0))
    col_scale = jnp.exp(jax.random.uniform(sub_keys[1], (count, cols), minval=-1.0, maxval=1.0))
    grad_scale = (DATA_RANKS ** 0.5) * row_scale[:, :, None] * col_scale[:, None, :]

    def draw_rank(rank_key):
        return (jax.random.normal(rank_key, (count, rows, cols)) * grad_scale).astype(jnp.bfloat16)

    grad_parts = lax.map(draw_rank, jax.random.split(sub_keys[2], DATA_RANKS))
    level_low = jax.random.uniform(sub_keys[3], (count,), minval=0.02, maxval=0.3)
    level_high = jax.random.uniform(sub_keys[4], (count,), minval=1.5, maxval=3.0)
    mom_level = jnp.where(jnp.arange(count) % 2 == 0, level_low, level_high)
    weight = jax.random.normal(sub_keys[5], (count, rows, cols)) * (rows ** -0.5)
    row_jitter = jax.random.uniform(sub_keys[6], (count, rows), minval=0.5, maxval=1.5)
    col_jitter = jax.random.uniform(sub_keys[7], (count, cols), minval=0.5, maxval=1.5)
    row_mom = (row_scale ** 2) * jnp.mean(col_scale ** 2, axis=1, keepdims=True) * mom_level[:, None] * row_jitter
    col_mom = (col_scale ** 2) * jnp.mean(row_scale ** 2, axis=1, keepdims=True) * mom_level[:, None] * col_jitter
    return grad_parts, weight, row_mom, col_mom


def setup_inputs(seed: int = 0) -> dict:
    sub_keys = jax.random.split(jax.random.key(seed), 4)
    grad_in, w_in, row_in, col_in = draw_group(sub_keys[0], MATS_IN, D, FF)
    grad_out, w_out, row_out, col_out = draw_group(sub_keys[1], MATS_OUT, FF, D)
    grad_qkv, w_qkv, row_qkv, col_qkv = draw_group(sub_keys[2], MATS_QKV, D, ATTN_WIDTH)
    grad_o, w_o, row_o, col_o = draw_group(sub_keys[3], MATS_O, ATTN_WIDTH, D)
    return {'grad_in': grad_in, 'w_in': w_in, 'row_in': row_in, 'col_in': col_in,
            'grad_out': grad_out, 'w_out': w_out, 'row_out': row_out, 'col_out': col_out,
            'grad_qkv': grad_qkv, 'w_qkv': w_qkv, 'row_qkv': row_qkv, 'col_qkv': col_qkv,
            'grad_o': grad_o, 'w_o': w_o, 'row_o': row_o, 'col_o': col_o}


def update_group(grad_parts, weight, row_mom, col_mom):
    grad_mean = jnp.sum(grad_parts, axis=0, dtype=jnp.float32) / DATA_RANKS
    grad_sq = grad_mean * grad_mean + EPS_SQ
    new_row = BETA_TWO * row_mom + (1.0 - BETA_TWO) * jnp.mean(grad_sq, axis=2)
    new_col = BETA_TWO * col_mom + (1.0 - BETA_TWO) * jnp.mean(grad_sq, axis=1)
    row_rel = new_row / jnp.mean(new_row, axis=1, keepdims=True)
    update = grad_mean / jnp.sqrt(row_rel[:, :, None] * new_col[:, None, :])
    upd_rms = jnp.sqrt(jnp.mean(update * update, axis=(1, 2), keepdims=True))
    update = update / jnp.maximum(1.0, upd_rms)
    w_rms = jnp.sqrt(jnp.mean(weight * weight, axis=(1, 2), keepdims=True))
    return weight - LR_BASE * jnp.maximum(1e-3, w_rms) * update, new_row, new_col


def reference(grad_in, w_in, row_in, col_in, grad_out, w_out, row_out, col_out,
              grad_qkv, w_qkv, row_qkv, col_qkv, grad_o, w_o, row_o, col_o):
    w_in_new, row_in_new, col_in_new = update_group(grad_in, w_in, row_in, col_in)
    w_out_new, row_out_new, col_out_new = update_group(grad_out, w_out, row_out, col_out)
    w_qkv_new, row_qkv_new, col_qkv_new = update_group(grad_qkv, w_qkv, row_qkv, col_qkv)
    w_o_new, row_o_new, col_o_new = update_group(grad_o, w_o, row_o, col_o)
    return (w_in_new, row_in_new, col_in_new, w_out_new, row_out_new, col_out_new,
            w_qkv_new, row_qkv_new, col_qkv_new, w_o_new, row_o_new, col_o_new)
```

```python
import functools

import jax
import jax.numpy as jnp
from jax import lax
from jax.experimental import pallas as pl
from jax.experimental.pallas import tpu as pltpu
from jax.sharding import PartitionSpec as P

OPT_STEP = 4
EPS_SQ = 1e-30
BETA_TWO = 1.0 - OPT_STEP ** -0.8
GAIN = 1.0 - BETA_TWO
LR_BASE = min(1e-2, OPT_STEP ** -0.5)
F32 = jnp.float32

N_IN, N_B, N_OUT = 24, 18, 12
N_SUP = N_IN + N_B + N_OUT
FIRST_B, FIRST_OUT = N_IN, N_IN + N_B
ROW_IN, ROW_OUT, ROW_B = 0, 24, 40
CHUNKS = tuple(('in', 6 * i, 6) for i in range(4)) + tuple(('b', FIRST_B + 6 * i, 6) for i in range(3)) \
    + tuple(('out', FIRST_OUT + 6 * i, 6) for i in range(2))
N_CH = len(CHUNKS)
GROUPS = ('in', 'b', 'out')
LAST_CHUNK = {f: max(i for i, c in enumerate(CHUNKS) if c[0] == f) for f in GROUPS}
D2D, OPP_A, OPP_B, OWN_R, OWN_L, MRG_R, MRG_L = range(7)
EX_SLOT = {'in': 0, 'b': 1, 'out': 2, 'w': 3}


def kernel(n_data, n_model, gin_h, gout_h, gq_h, go_h, win_h, wout_h, wq_h, wo_h,
           row_in, col_in, row_out, col_out, sub_b, lane_b, row_o,
           win_o, wout_o, wq_o, wo_o, row_in_o, col_in_o, row_out_o, col_out_o, sub_b_o, lane_b_o,
           gin, gout, gb, part, peer, opp_in, left_in, right_in, grad, wa, wb, w_all, ht,
           lane_sum, rlane, acc_t, comp_b, tab, rsub, wtab, vtab, mod_in, mod_b, mod_out, mod_w,
           scal, dat_in, dat_b, dat_out, got_in, got_b, got_out, got_w, got_s,
           load_sem, w_sem, out_sem, snd, rcv, dsnd, drcv, msnd, mrcv, ssnd, srcv):
    me = lax.axis_index('data')
    mod = lax.axis_index('model')
    n_chips = n_data // 2
    x, c = lax.div(me, 2), lax.rem(me, 2)
    xr, xl, xo = lax.rem(x + 1, n_chips), lax.rem(x + 3, n_chips), lax.rem(x + 2, n_chips)
    partner, right, left = 2 * x + 1 - c, 2 * xr + c, 2 * xl + c
    full = {'in': n_model * 128, 'out': n_model * 128, 'b': n_model * 32}
    count = {'in': N_IN, 'b': N_B, 'out': N_OUT}
    mats = {'in': N_IN, 'b': 4 * N_B, 'out': N_OUT}
    first = {'in': 0, 'b': FIRST_B, 'out': FIRST_OUT}
    row0 = {'in': ROW_IN, 'b': ROW_B, 'out': ROW_OUT}
    mod_blk = {'in': mod_in, 'b': mod_b, 'out': mod_out}
    dat_got = {'in': dat_in, 'b': dat_b, 'out': dat_out}
    mod_got = {'in': got_in, 'b': got_b, 'out': got_out}
    lane_rows = {'in': (0, 24), 'b': (24, 24), 'out': (48, 16)}

    loads = [pltpu.make_async_copy(gin_h.at[pl.ds(6 * i, 6)], gin.at[pl.ds(6 * i, 6)], load_sem.at[i]) for i in range(4)]
    loads.append(pltpu.make_async_copy(gq_h, gb.at[pl.ds(0, 54)], load_sem.at[4]))
    loads.append(pltpu.make_async_copy(go_h, gb.at[pl.ds(54, 18)], load_sem.at[5]))
    loads.append(pltpu.make_async_copy(gout_h, gout, load_sem.at[6]))
    w_loads = [pltpu.make_async_copy(win_h, wa.at[pl.ds(0, 24)], w_sem.at[0]),
               pltpu.make_async_copy(wout_h, wa.at[pl.ds(24, 12)], w_sem.at[1]),
               pltpu.make_async_copy(wq_h, wb.at[pl.ds(0, 54)], w_sem.at[2]),
               pltpu.make_async_copy(wo_h, wb.at[pl.ds(54, 18)], w_sem.at[3])]
    for cp in loads + w_loads:
        cp.start()

    barrier = pltpu.get_barrier_semaphore()

    def hello_data(d, carry):
        pl.semaphore_signal(barrier, inc=1, device_id={'data': lax.rem(me + d, n_data)}, device_id_type=pl.DeviceIdType.MESH)
        return carry

    def hello_model(d, carry):
        pl.semaphore_signal(barrier, inc=1, device_id={'model': lax.rem(mod + d, n_model)}, device_id_type=pl.DeviceIdType.MESH)
        return carry

    lax.fori_loop(1, n_data, hello_data, 0)
    lax.fori_loop(1, n_model, hello_model, 0)

    def remote(src, dst, ssem, rsem, axis, who):
        return pltpu.make_async_remote_copy(src_ref=src, dst_ref=dst, send_sem=ssem, recv_sem=rsem,
                                            device_id={axis: who}, device_id_type=pl.DeviceIdType.MESH)

    def transfer(kind, ch):
        _, b0, n = CHUNKS[ch]
        n_a = n // 2
        every, half_a, half_b = pl.ds(b0, n), pl.ds(b0, n_a), pl.ds(b0 + n_a, n - n_a)
        src, dst, who = {
            D2D: lambda: (part.at[1 - c, :, every], peer.at[:, every], partner),
            OPP_A: lambda: (part.at[c, xo, half_a], opp_in.at[half_a], right),
            OPP_B: lambda: (part.at[c, xo, half_b], opp_in.at[half_b], left),
            OWN_R: lambda: (part.at[c, xr, half_b], left_in.at[half_b], right),
            OWN_L: lambda: (part.at[c, xl, half_a], right_in.at[half_a], left),
            MRG_R: lambda: (part.at[c, xr, half_a], left_in.at[half_a], right),
            MRG_L: lambda: (part.at[c, xl, half_b], right_in.at[half_b], left),
        }[kind]()
        return remote(src, dst, snd.at[kind, ch], rcv.at[kind, ch], 'data', who)

    def convert(ch):
        family, b0, n = CHUNKS[ch]
        if family == 'in':
            loads[ch].wait()
        elif ch == 4:
            loads[4].wait()
            loads[5].wait()
        elif family == 'out' and b0 == FIRST_OUT:
            loads[6].wait()

        def body(i, carry):
            b = b0 + i
            for t in range(n_chips):
                if family == 'in':
                    tile = gin[b, pl.ds(128 * t, 128), :].astype(F32)
                elif family == 'out':
                    tile = gout[b - FIRST_OUT, :, pl.ds(128 * t, 128)].astype(F32).T
                else:
                    four = gb[pl.ds(4 * (b - FIRST_B), 4), :, pl.ds(128 * t, 128)].astype(F32)
                    tile = four.reshape(128, 128).T
                part[0, t, b] = tile[:64]
                part[1, t, b] = tile[64:]
            return carry

        lax.fori_loop(0, n, body, 0)

    def pair(ch):
        _, b0, n = CHUNKS[ch]
        transfer(D2D, ch).wait_recv()

        def add(dest):
            def body(i, carry):
                b = b0 + i
                part[c, dest, b] = part[c, dest, b] + peer[dest, b]
                return carry
            lax.fori_loop(0, n, body, 0)

        add(xo)
        transfer(OPP_A, ch).start()
        transfer(OPP_B, ch).start()
        add(xr)
        transfer(OWN_R, ch).start()
        add(xl)
        transfer(OWN_L, ch).start()
        add(x)

    def merge(ch):
        _, b0, n = CHUNKS[ch]
        n_a = n // 2

        def add(dest, lo, hi):
            def body(b, carry):
                part[c, dest, b] = part[c, dest, b] + opp_in[b]
                return carry
            lax.fori_loop(lo, hi, body, 0)

        transfer(OPP_A, ch).wait_recv()
        add(xr, b0, b0 + n_a)
        transfer(MRG_R, ch).start()
        transfer(OPP_B, ch).wait_recv()
        add(xl, b0 + n_a, b0 + n)
        transfer(MRG_L, ch).start()

    lane_iota = lax.broadcasted_iota(jnp.int32, (64, 128), 1)

    def finish(ch):
        family, b0, n = CHUNKS[ch]
        for kind in (OWN_R, OWN_L, MRG_R, MRG_L):
            transfer(kind, ch).wait_recv()
        base = lane_rows[family][0] - first[family]

        def block(b):
            g = (part[c, x, b] + left_in[b] + right_in[b]) * (1.0 / n_data)
            grad[b] = g
            sq = g * g + EPS_SQ
            lane_sum[pl.ds(base + b, 1), :] = jnp.sum(sq, axis=0, keepdims=True)
            return g, sq

        if family == 'b':
            def body(i, carry):
                b = b0 + i
                g, _ = block(b)
                gt = g.T
                st = (gt * gt + EPS_SQ).reshape(4, 32, 64)
                comp_b[pl.ds(b - FIRST_B, 1), :, 0:64] = jnp.sum(st, axis=1)[None]
                return carry
            lax.fori_loop(0, n, body, 0)
        else:
            which = 0 if family == 'in' else 1

            def body(i, acc):
                b = b0 + i
                _, sq = block(b)
                return jnp.where(lane_iota == b - first[family], jnp.sum(sq, axis=1, keepdims=True), acc)
            acc_t[which] = lax.fori_loop(0, n, body, acc_t[which])

    def gather(src, dst, sems, slot, axis, op):
        send, recv = sems
        rank, n = (me, n_data) if axis == 'data' else (mod, n_model)

        def body(d, carry):
            p = lax.rem(rank + d, n)
            if op == 'start':
                remote(src, dst.at[rank], send.at[slot, p], recv.at[slot, rank], axis, p).start()
            elif op == 'recv':
                remote(src, dst.at[p], send.at[slot, p], recv.at[slot, p], axis, p).wait_recv()
            else:
                remote(src, dst.at[rank], send.at[slot, p], recv.at[slot, rank], axis, p).wait_send()
            return carry

        if op == 'start':
            dst[rank] = src[...]
        lax.fori_loop(1, n, body, 0)

    def total(dst, n):
        acc = dst[0]
        for r in range(1, n):
            acc = acc + dst[r]
        return acc

    d_sems, m_sems, s_sems = (dsnd, drcv), (msnd, mrcv), (ssnd, srcv)

    def lane_ex(family, op):
        r0, n = lane_rows[family]
        gather(lane_sum.at[pl.ds(r0, n)], dat_got[family], d_sems, EX_SLOT[family], 'data', op)

    def model_ex(family, op):
        gather(mod_blk[family], mod_got[family], m_sems, EX_SLOT[family], 'model', op)

    def scal_ex(family, op):
        gather(scal.at[EX_SLOT[family]], got_s.at[EX_SLOT[family]], s_sems, EX_SLOT[family], 'data', op)

    def weights_start():
        for cp in w_loads:
            cp.wait()
        wtab[...] = jnp.zeros_like(wtab)
        vtab[...] = jnp.zeros_like(vtab)

        def body_a(b, carry):
            w = wa[b]
            wtab[pl.ds(b, 1), :] = jnp.sum(w * w, axis=0, keepdims=True)
            return carry

        def body_b(b, carry):
            w = wb[b]
            wtab[pl.ds(ROW_B + b, 1), 0:64] = jnp.sum(w * w, axis=0, keepdims=True)
            return carry

        lax.fori_loop(0, N_IN + N_OUT, body_a, 0)
        lax.fori_loop(0, 4 * N_B, body_b, 0)
        vtab[ROW_OUT:ROW_OUT + N_OUT, :] = row_out[...]
        vtab[ROW_B + 54:ROW_B + 72, 0:32] = row_o[...]
        mod_w[...] = jnp.zeros_like(mod_w)
        mod_w[0:1, :] = jnp.sum(wtab[...].T, axis=0, keepdims=True)
        mod_w[1:2, :] = jnp.sum(vtab[...].T, axis=0, keepdims=True) / n_data
        gather(mod_w, got_w, m_sems, EX_SLOT['w'], 'model', 'start')

    def weights_next():
        gather(mod_w, got_w, m_sems, EX_SLOT['w'], 'model', 'recv')
        scal[EX_SLOT['w']] = total(got_w, n_model)
        scal_ex('w', 'start')

    def weights_done():
        scal_ex('w', 'recv')
        w_all[...] = total(got_s.at[EX_SLOT['w']], n_data)

    def after_lanes(family):
        r0, _ = lane_rows[family]
        n = count[family]
        lane_ex(family, 'recv')
        mom, out = {'in': (col_in, col_in_o), 'out': (row_out, row_out_o), 'b': (lane_b, lane_b_o)}[family]
        new = BETA_TWO * mom[...] + GAIN * (total(dat_got[family], n_data)[:n] / 512.0)
        out[...] = new
        rlane[r0:r0 + n, :] = lax.rsqrt(new)
        if family == 'b':
            def body(s, carry):
                h = grad[FIRST_B + s] * rlane[pl.ds(r0 + s, 1), :]
                t = h.T.reshape(4, 32, 64)
                ht[pl.ds(4 * s, 4)] = t
                comp_b[pl.ds(s, 1), :, 64:128] = jnp.sum(t * t, axis=1)[None]
                return carry
            lax.fori_loop(0, N_B, body, 0)
            mod_b[...] = comp_b[...].reshape(4 * N_B, 128)
        else:
            which = 0 if family == 'in' else 1

            def body(b, acc):
                h = grad[first[family] + b] * rlane[pl.ds(r0 + b, 1), :]
                grad[first[family] + b] = h
                return jnp.where(lane_iota == b, jnp.sum(h * h, axis=1, keepdims=True), acc)
            acc_z = lax.fori_loop(0, n, body, jnp.zeros((64, 128), F32))
            both = jnp.concatenate([acc_t[which], acc_z], axis=0).T
            mod_blk[family][...] = both[:mod_blk[family].shape[0]]
        model_ex(family, 'start')

    def after_model(family):
        n = mats[family]
        model_ex(family, 'recv')
        both = total(mod_got[family], n_model)[:n]
        sums, z = both[:, 0:64], both[:, 64:128]
        mom, out = {'in': (row_in, row_in_o), 'out': (col_out, col_out_o), 'b': (sub_b, sub_b_o)}[family]
        new = BETA_TWO * mom[...] + GAIN * (sums / full[family])
        out[...] = new
        ratio = z / new
        mean_part = GAIN * (sums / 512.0)
        if family == 'in':
            term = new
        elif family == 'out':
            term = mean_part
        else:
            term = jnp.where(lax.broadcasted_iota(jnp.int32, (n, 64), 0) < 54, new, mean_part)
        r0 = row0[family]
        tab[r0:r0 + n, 0:64] = ratio
        tab[r0:r0 + n, 64:128] = term
        turned = tab[...].T
        e = EX_SLOT[family]
        scal[e] = jnp.zeros((8, 128), F32)
        scal[e, 0:1, :] = jnp.sum(turned[:64], axis=0, keepdims=True)
        scal[e, 1:2, :] = jnp.sum(turned[64:], axis=0, keepdims=True)
        scal_ex(family, 'start')
        if family == 'b':
            rsub[e, r0:r0 + n, 0:64] = lax.rsqrt(new)
        else:
            tab[r0:r0 + n, 0:64] = lax.rsqrt(new)
            rsub[e] = tab[...].T

    def after_scalars(family):
        e = EX_SLOT[family]
        scal_ex(family, 'recv')
        tot = total(got_s.at[e], n_data)
        q, s = tot[0:1], tot[1:2]
        w, v = w_all[0:1, :], w_all[1:2, :]
        rows = 512.0 if family == 'in' else float(full[family])
        size = 512.0 * full[family]
        m = (s if family == 'in' else BETA_TWO * v + s) / rows
        scale = jnp.sqrt(m) * (LR_BASE * jnp.maximum(1e-3, jnp.sqrt(w / size))) / jnp.maximum(1.0, jnp.sqrt(m * q / size))
        r0 = row0[family]
        if family == 'b':
            n = mats[family]
            tab[...] = jnp.broadcast_to(scale, (128, 128)).T
            rsub[e, r0:r0 + n, 0:64] = rsub[e, r0:r0 + n, 0:64] * tab[r0:r0 + n, 0:64]

            def body(b, carry):
                wb[b] = wb[b] - ht[b] * rsub[e, pl.ds(r0 + b, 1), 0:64]
                return carry
            lax.fori_loop(0, n, body, 0)
            outs = (pltpu.make_async_copy(wb.at[pl.ds(0, 54)], wq_o, out_sem.at[2]),
                    pltpu.make_async_copy(wb.at[pl.ds(54, 18)], wo_o, out_sem.at[3]))
        else:
            fac = rsub[e, 0:64, :] * scale

            def body(b, carry):
                f = jnp.sum(jnp.where(lane_iota == r0 + b, fac, 0.0), axis=1, keepdims=True)
                wa[r0 + b] = wa[r0 + b] - grad[first[family] + b] * f
                return carry
            lax.fori_loop(0, count[family], body, 0)
            outs = (pltpu.make_async_copy(wa.at[pl.ds(r0, count[family])], win_o if family == 'in' else wout_o,
                                          out_sem.at[0 if family == 'in' else 1]),)
        for cp in outs:
            cp.start()
        return outs

    acc_t[...] = jnp.zeros_like(acc_t)
    tab[...] = jnp.zeros_like(tab)
    lane_sum[...] = jnp.zeros_like(lane_sum)

    convert(0)
    pl.semaphore_wait(barrier, n_data - 1 + n_model - 1)
    pending = []
    for k in range(N_CH + 8):
        if 0 < k < N_CH:
            convert(k)
        if k < N_CH:
            transfer(D2D, k).start()
        if 1 <= k <= N_CH:
            pair(k - 1)
        if 2 <= k <= N_CH + 1:
            merge(k - 2)
        if 3 <= k <= N_CH + 2:
            finish(k - 3)
        if k == 2:
            weights_start()
        if k == 3:
            weights_next()
        if k == 4:
            weights_done()
        for family in GROUPS:
            done = k - (LAST_CHUNK[family] + 3)
            if done == 0:
                lane_ex(family, 'start')
            if done == 1:
                after_lanes(family)
            if done == 2:
                after_model(family)
            if done == 3:
                pending.extend(after_scalars(family))

    for ch in range(N_CH):
        for kind in range(7):
            transfer(kind, ch).wait_send()
    for family in GROUPS:
        lane_ex(family, 'send')
        model_ex(family, 'send')
        scal_ex(family, 'send')
    gather(mod_w, got_w, m_sems, EX_SLOT['w'], 'model', 'send')
    scal_ex('w', 'send')
    for cp in pending:
        cp.wait()


def solution(mesh):
    axis_sizes = dict(mesh.shape)
    n_data, n_model = axis_sizes['data'], axis_sizes['model']
    n_chips = n_data // 2
    rows_data = (P('data', None, None, 'model'), P(None, 'data', 'model'), P(None, 'data'), P(None, 'model'))
    rows_model = (P('data', None, 'model', None), P(None, 'model', 'data'), P(None, 'model'), P(None, 'data'))

    def shape(*dims):
        return jax.ShapeDtypeStruct(dims, F32)

    def vmem(*dims):
        return pltpu.VMEM(dims, F32)

    scratch = [
        pltpu.VMEM((24, 512, 128), jnp.bfloat16), pltpu.VMEM((12, 128, 512), jnp.bfloat16),
        pltpu.VMEM((72, 32, 512), jnp.bfloat16),
        vmem(2, n_chips, N_SUP, 64, 128), vmem(n_chips, N_SUP, 64, 128),
        vmem(N_SUP, 64, 128), vmem(N_SUP, 64, 128), vmem(N_SUP, 64, 128), vmem(N_SUP, 64, 128),
        vmem(36, 64, 128), vmem(72, 32, 64), vmem(8, 128), vmem(72, 32, 64),
        vmem(64, 128), vmem(64, 128), vmem(2, 64, 128), vmem(N_B, 4, 128),
        vmem(128, 128), vmem(3, 128, 128), vmem(128, 128), vmem(128, 128),
        vmem(24, 128), vmem(72, 128), vmem(16, 128), vmem(8, 128),
        vmem(4, 8, 128), vmem(n_data, 24, 128), vmem(n_data, 24, 128), vmem(n_data, 16, 128),
        vmem(n_model, 24, 128), vmem(n_model, 72, 128), vmem(n_model, 16, 128), vmem(n_model, 8, 128),
        vmem(4, n_data, 8, 128),
        pltpu.SemaphoreType.DMA((7,)), pltpu.SemaphoreType.DMA((4,)), pltpu.SemaphoreType.DMA((4,)),
        pltpu.SemaphoreType.DMA((7, N_CH)), pltpu.SemaphoreType.DMA((7, N_CH)),
        pltpu.SemaphoreType.DMA((3, n_data)), pltpu.SemaphoreType.DMA((3, n_data)),
        pltpu.SemaphoreType.DMA((4, n_model)), pltpu.SemaphoreType.DMA((4, n_model)),
        pltpu.SemaphoreType.DMA((4, n_data)), pltpu.SemaphoreType.DMA((4, n_data)),
    ]
    hbm, in_vmem = pl.BlockSpec(memory_space=pl.ANY), pl.BlockSpec(memory_space=pltpu.VMEM)

    def step_all(grad_in, w_in, row_in, col_in, grad_out, w_out, row_out, col_out,
                 grad_qkv, w_qkv, row_qkv, col_qkv, grad_o, w_o, row_o, col_o):
        sub_b = jnp.concatenate([row_qkv, col_o], axis=0)
        lane_b = jnp.concatenate([col_qkv, row_o], axis=0).reshape(N_B, 128)
        outs = pl.pallas_call(
            functools.partial(kernel, n_data, n_model),
            name='adafactor_step',
            out_shape=(shape(24, 64, 128), shape(12, 64, 128), shape(54, 32, 64), shape(18, 32, 64),
                       shape(24, 64), shape(24, 128), shape(12, 128), shape(12, 64), shape(72, 64), shape(N_B, 128)),
            in_specs=[hbm] * 8 + [in_vmem] * 7,
            out_specs=[hbm] * 4 + [in_vmem] * 6,
            scratch_shapes=scratch,
            compiler_params=pltpu.CompilerParams(collective_id=0, has_side_effects=True, vmem_limit_bytes=60 * 1024 * 1024),
        )(grad_in[0], grad_out[0], grad_qkv[0].transpose(0, 2, 1), grad_o[0],
          w_in, w_out.transpose(0, 2, 1), w_qkv.transpose(0, 2, 1), w_o,
          row_in, col_in, row_out, col_out, sub_b, lane_b, row_o)
        w_in_new, w_out_new, w_qkv_new, w_o_new, row_in_new, col_in_new, row_out_new, col_out_new, sub_new, lane_new = outs
        lane_new = lane_new.reshape(72, 32)
        return (w_in_new, row_in_new, col_in_new, w_out_new.transpose(0, 2, 1), row_out_new, col_out_new,
                w_qkv_new.transpose(0, 2, 1), sub_new[:54], lane_new[:54], w_o_new, lane_new[54:], sub_new[54:])

    in_specs = rows_data + rows_model + rows_data + rows_model
    out_specs = rows_data[1:] + rows_model[1:] + rows_data[1:] + rows_model[1:]
    return jax.shard_map(step_all, mesh=mesh, in_specs=in_specs, out_specs=out_specs, check_vma=False)
```

```python
import functools

import jax
import jax.numpy as jnp
from jax import lax
from jax.experimental import pallas as pl
from jax.experimental.pallas import tpu as pltpu
from jax.sharding import PartitionSpec as P

OPT_STEP = 4
EPS_SQ = 1e-30
BETA_TWO = 1.0 - OPT_STEP ** -0.8
GAIN = 1.0 - BETA_TWO
LR_BASE = min(1e-2, OPT_STEP ** -0.5)
F32 = jnp.float32
LANES, ROWS, WIDE = 128, 64, 32
VMEM_LIMIT = 60 * 10 ** 6

N_IN, N_B, N_OUT = 24, 18, 12
N_SUP = N_IN + N_B + N_OUT
FIRST_B, FIRST_IN, FIRST_OUT = 0, N_B, N_B + N_IN
N_QKV, N_O = 54, 18
ROW_IN, ROW_OUT, ROW_B = 0, 24, 40
SIZES = (('b', (2, 4, 6, 6)), ('in', (6, 6, 6, 6)), ('out', (6, 4, 2)))


def cut():
    chunks, at = [], 0
    for family, sizes in SIZES:
        for n in sizes:
            chunks.append((family, at, n))
            at += n
    return tuple(chunks)


CHUNKS = cut()
N_CH = len(CHUNKS)
GROUPS = ('out', 'in', 'b')
LAST_CHUNK = {f: max(i for i, c in enumerate(CHUNKS) if c[0] == f) for f in GROUPS}
D2D, OPP_A, OPP_B, OWN_R, OWN_L, MRG_R, MRG_L = range(7)
EX_SLOT = {'in': 0, 'b': 1, 'out': 2, 'w': 3}
AHEAD, EARLY_OWN, LAG_MERGE, LAG_FINISH = 2, 3, 2, 3
LAG_STATS = {'b': (1, 3, 5), 'in': (1, 3, 4), 'out': (1, 2, 3)}


def kernel(n_data, n_model, gin_h, gout_h, gq_h, go_h, win_h, wout_h, wq_h, wo_h,
           row_in_h, col_in_h, row_out_h, col_out_h, row_q_h, col_q_h, row_o_h, col_o_h,
           w_in, w_out, w_q, w_o, row_in_o, col_in_o, row_out_o, col_out_o, row_q_o, col_q_o, row_o_o, col_o_o,
           row_in, col_in, row_out, col_out, row_q, col_q, row_o, col_o, lane_b, turn,
           gin, gout, gb, part, peer, opp_in, left_in, right_in, grad, w_all, ht,
           lane_sum, rlane, acc_t, comp_b, tab, rsub, wtab, vtab, mod_in, mod_b, mod_out, mod_w,
           scal, dat_in, dat_b, dat_out, got_in, got_b, got_out, got_w, got_s,
           load_sem, w_sem, small_sem, snd, rcv, dsnd, drcv, msnd, mrcv, ssnd, srcv):
    me = lax.axis_index('data')
    mod = lax.axis_index('model')
    n_chips = n_data // 2
    x, c = lax.div(me, 2), lax.rem(me, 2)
    xr, xl, xo = lax.rem(x + 1, n_chips), lax.rem(x + 3, n_chips), lax.rem(x + 2, n_chips)
    partner, right, left = 2 * x + 1 - c, 2 * xr + c, 2 * xl + c
    full = {'in': n_model * LANES, 'out': n_model * LANES, 'b': n_model * WIDE}
    count = {'in': N_IN, 'b': N_B, 'out': N_OUT}
    mats = {'in': N_IN, 'b': 4 * N_B, 'out': N_OUT}
    first = {'in': FIRST_IN, 'b': FIRST_B, 'out': FIRST_OUT}
    row0 = {'in': ROW_IN, 'b': ROW_B, 'out': ROW_OUT}
    mod_blk = {'in': mod_in, 'b': mod_b, 'out': mod_out}
    dat_got = {'in': dat_in, 'b': dat_b, 'out': dat_out}
    mod_got = {'in': got_in, 'b': got_b, 'out': got_out}
    lane_rows = {'in': (0, 24), 'b': (24, 24), 'out': (48, 16)}

    loads = [pltpu.make_async_copy(gq_h.at[pl.ds(0, 8)], gb.at[pl.ds(0, 8)], load_sem.at[0]),
             pltpu.make_async_copy(gq_h.at[pl.ds(8, 46)], gb.at[pl.ds(8, 46)], load_sem.at[1]),
             pltpu.make_async_copy(go_h, gb.at[pl.ds(54, 18)], load_sem.at[2]),
             pltpu.make_async_copy(gin_h, gin, load_sem.at[3]),
             pltpu.make_async_copy(gout_h, gout, load_sem.at[4])]
    w_loads = [pltpu.make_async_copy(win_h, w_in, w_sem.at[0]),
               pltpu.make_async_copy(wout_h, w_out, w_sem.at[1]),
               pltpu.make_async_copy(wq_h, w_q, w_sem.at[2]),
               pltpu.make_async_copy(wo_h, w_o, w_sem.at[3])]
    small = [pltpu.make_async_copy(src, dst, small_sem.at[i]) for i, (src, dst) in enumerate((
        (row_in_h, row_in), (col_in_h, col_in), (row_out_h, row_out), (col_out_h, col_out),
        (row_q_h, row_q), (col_q_h, col_q), (row_o_h, row_o), (col_o_h, col_o)))]
    for cp in loads:
        cp.start()

    barrier = pltpu.get_barrier_semaphore()

    def hello_data(d, carry):
        pl.semaphore_signal(barrier, inc=1, device_id={'data': lax.rem(me + d, n_data)}, device_id_type=pl.DeviceIdType.MESH)
        return carry

    def hello_model(d, carry):
        pl.semaphore_signal(barrier, inc=1, device_id={'model': lax.rem(mod + d, n_model)}, device_id_type=pl.DeviceIdType.MESH)
        return carry

    lax.fori_loop(1, n_data, hello_data, 0)
    lax.fori_loop(1, n_model, hello_model, 0)

    def remote(src, dst, ssem, rsem, axis, who):
        return pltpu.make_async_remote_copy(src_ref=src, dst_ref=dst, send_sem=ssem, recv_sem=rsem,
                                            device_id={axis: who}, device_id_type=pl.DeviceIdType.MESH)

    def transfer(kind, ch):
        _, b0, n = CHUNKS[ch]
        n_a = n // 2
        every, half_a, half_b = pl.ds(b0, n), pl.ds(b0, n_a), pl.ds(b0 + n_a, n - n_a)
        src, dst, who = {
            D2D: lambda: (part.at[1 - c, :, every], peer.at[:, every], partner),
            OPP_A: lambda: (part.at[c, xo, half_a], opp_in.at[half_a], right),
            OPP_B: lambda: (part.at[c, xo, half_b], opp_in.at[half_b], left),
            OWN_R: lambda: (part.at[c, xr, half_b], left_in.at[half_b], right),
            OWN_L: lambda: (part.at[c, xl, half_a], right_in.at[half_a], left),
            MRG_R: lambda: (part.at[c, xr, half_a], left_in.at[half_a], right),
            MRG_L: lambda: (part.at[c, xl, half_b], right_in.at[half_b], left),
        }[kind]()
        return remote(src, dst, snd.at[kind, ch], rcv.at[kind, ch], 'data', who)

    def convert(ch):
        family, b0, n = CHUNKS[ch]
        if ch == 0:
            loads[0].wait()
        elif ch == 1:
            loads[1].wait()
            loads[2].wait()
        elif b0 == FIRST_IN:
            loads[3].wait()
        elif b0 == FIRST_OUT:
            loads[4].wait()

        def body(i, carry):
            b = b0 + i
            for t in range(n_chips):
                if family == 'in':
                    tile = gin[b - FIRST_IN, pl.ds(LANES * t, LANES), :].astype(F32)
                elif family == 'out':
                    tile = gout[b - FIRST_OUT, :, pl.ds(LANES * t, LANES)].astype(F32).T
                else:
                    four = gb[pl.ds(4 * (b - FIRST_B), 4), :, pl.ds(LANES * t, LANES)].astype(F32)
                    tile = four.reshape(LANES, LANES).T
                part[0, t, b] = tile[:ROWS]
                part[1, t, b] = tile[ROWS:]
            return carry

        lax.fori_loop(0, n, body, 0)

    def add_peer(ch, dest):
        _, b0, n = CHUNKS[ch]

        def body(i, carry):
            b = b0 + i
            part[c, dest, b] = part[c, dest, b] + peer[dest, b]
            return carry
        lax.fori_loop(0, n, body, 0, unroll=2)

    def opposite(ch):
        transfer(D2D, ch).wait_recv()
        add_peer(ch, xo)
        transfer(OPP_A, ch).start()
        transfer(OPP_B, ch).start()
        add_peer(ch, xr)
        add_peer(ch, xl)
        if ch < EARLY_OWN:
            own(ch)
        add_peer(ch, x)

    def own(ch):
        transfer(OWN_R, ch).start()
        transfer(OWN_L, ch).start()

    def merge(ch):
        _, b0, n = CHUNKS[ch]
        n_a = n // 2

        def add(dest, lo, hi):
            def body(b, carry):
                part[c, dest, b] = part[c, dest, b] + opp_in[b]
                return carry
            lax.fori_loop(lo, hi, body, 0)

        transfer(OPP_A, ch).wait_recv()
        add(xr, b0, b0 + n_a)
        transfer(MRG_R, ch).start()
        transfer(OPP_B, ch).wait_recv()
        add(xl, b0 + n_a, b0 + n)
        transfer(MRG_L, ch).start()
        if ch >= EARLY_OWN:
            own(ch)

    lane_iota = lax.broadcasted_iota(jnp.int32, (ROWS, LANES), 1)

    def finish(ch):
        family, b0, n = CHUNKS[ch]
        for kind in (OWN_R, OWN_L, MRG_R, MRG_L):
            transfer(kind, ch).wait_recv()
        base = lane_rows[family][0] - first[family]

        def block(b):
            g = (part[c, x, b] + left_in[b] + right_in[b]) * (1.0 / n_data)
            grad[b] = g
            sq = g * g + EPS_SQ
            lane_sum[pl.ds(base + b, 1), :] = jnp.sum(sq, axis=0, keepdims=True)
            return g, sq

        if family == 'b':
            def body(i, carry):
                b = b0 + i
                g, _ = block(b)
                gt = g.T
                st = (gt * gt + EPS_SQ).reshape(4, WIDE, ROWS)
                comp_b[pl.ds(b - FIRST_B, 1), :, 0:ROWS] = jnp.sum(st, axis=1)[None]
                return carry
            lax.fori_loop(0, n, body, 0, unroll=2)
        else:
            which = 0 if family == 'in' else 1

            def body(i, acc):
                b = b0 + i
                _, sq = block(b)
                return jnp.where(lane_iota == b - first[family], jnp.sum(sq, axis=1, keepdims=True), acc)
            acc_t[which] = lax.fori_loop(0, n, body, acc_t[which], unroll=2)

    def gather(src, dst, sems, slot, axis, op):
        send, recv = sems
        rank, n = (me, n_data) if axis == 'data' else (mod, n_model)

        def body(d, carry):
            p = lax.rem(rank + d, n)
            if op == 'start':
                remote(src, dst.at[rank], send.at[slot, p], recv.at[slot, rank], axis, p).start()
            elif op == 'recv':
                remote(src, dst.at[p], send.at[slot, p], recv.at[slot, p], axis, p).wait_recv()
            else:
                remote(src, dst.at[rank], send.at[slot, p], recv.at[slot, rank], axis, p).wait_send()
            return carry

        if op == 'start':
            dst[rank] = src[...]
        lax.fori_loop(1, n, body, 0)

    def total(dst, n):
        acc = dst[0]
        for r in range(1, n):
            acc = acc + dst[r]
        return acc

    d_sems, m_sems, s_sems = (dsnd, drcv), (msnd, mrcv), (ssnd, srcv)

    def lane_ex(family, op):
        r0, n = lane_rows[family]
        gather(lane_sum.at[pl.ds(r0, n)], dat_got[family], d_sems, EX_SLOT[family], 'data', op)

    def model_ex(family, op):
        gather(mod_blk[family], mod_got[family], m_sems, EX_SLOT[family], 'model', op)

    def scal_ex(family, op):
        gather(scal.at[EX_SLOT[family]], got_s.at[EX_SLOT[family]], s_sems, EX_SLOT[family], 'data', op)

    def weights_start():
        for cp in w_loads + small:
            cp.wait()
        turn[...] = jnp.zeros_like(turn)
        turn[0:WIDE, 0:N_QKV] = col_q[...]
        turn[...] = turn[...].T
        turn[N_QKV:N_QKV + N_O, 0:WIDE] = row_o[...]
        row = turn[pl.ds(0, N_B, stride=4), :]
        for q in range(1, 4):
            row = row + pltpu.roll(turn[pl.ds(q, N_B, stride=4), :], WIDE * q, 1)
        lane_b[...] = row
        wtab[...] = jnp.zeros_like(wtab)
        vtab[...] = jnp.zeros_like(vtab)

        def squares(ref, row, width):
            def body(b, carry):
                w = ref[b]
                wtab[pl.ds(row + b, 1), 0:width] = jnp.sum(w * w, axis=0, keepdims=True)
                return carry
            lax.fori_loop(0, ref.shape[0], body, 0, unroll=6)

        squares(w_in, ROW_IN, LANES)
        squares(w_out, ROW_OUT, LANES)
        squares(w_q, ROW_B, ROWS)
        squares(w_o, ROW_B + N_QKV, ROWS)
        vtab[ROW_OUT:ROW_OUT + N_OUT, :] = row_out[...]
        vtab[ROW_B + 54:ROW_B + 72, 0:WIDE] = row_o[...]
        mod_w[...] = jnp.zeros_like(mod_w)
        mod_w[0:1, :] = jnp.sum(wtab[...].T, axis=0, keepdims=True)
        mod_w[1:2, :] = jnp.sum(vtab[...].T, axis=0, keepdims=True) / n_data
        gather(mod_w, got_w, m_sems, EX_SLOT['w'], 'model', 'start')

    def weights_next():
        gather(mod_w, got_w, m_sems, EX_SLOT['w'], 'model', 'recv')
        scal[EX_SLOT['w']] = total(got_w, n_model)
        scal_ex('w', 'start')

    def weights_done():
        scal_ex('w', 'recv')
        w_all[...] = total(got_s.at[EX_SLOT['w']], n_data)

    def after_lanes(family):
        r0, _ = lane_rows[family]
        n = count[family]
        lane_ex(family, 'recv')
        mom, out = {'in': (col_in, col_in_o), 'out': (row_out, row_out_o), 'b': (lane_b, None)}[family]
        new = BETA_TWO * mom[...] + GAIN * (total(dat_got[family], n_data)[:n] / 512.0)
        rlane[r0:r0 + n, :] = lax.rsqrt(new)
        if family == 'b':
            def body(s, carry):
                h = grad[FIRST_B + s] * rlane[pl.ds(r0 + s, 1), :]
                t = h.T.reshape(4, WIDE, ROWS)
                ht[pl.ds(4 * s, 4)] = t
                comp_b[pl.ds(s, 1), :, ROWS:LANES] = jnp.sum(t * t, axis=1)[None]
                return carry
            lax.fori_loop(0, N_B, body, 0, unroll=3)
            mod_b[...] = comp_b[...].reshape(4 * N_B, LANES)
        else:
            which = 0 if family == 'in' else 1

            def body(b, acc):
                h = grad[first[family] + b] * rlane[pl.ds(r0 + b, 1), :]
                grad[first[family] + b] = h
                return jnp.where(lane_iota == b, jnp.sum(h * h, axis=1, keepdims=True), acc)
            acc_z = lax.fori_loop(0, n, body, jnp.zeros((ROWS, LANES), F32), unroll=4)
            both = jnp.concatenate([acc_t[which], acc_z], axis=0).T
            mod_blk[family][...] = both[:mod_blk[family].shape[0]]
        model_ex(family, 'start')
        if family == 'b':
            turn[...] = jnp.zeros_like(turn)
            for q in range(4):
                turn[pl.ds(q, N_B, stride=4), :] = pltpu.roll(new, (LANES - WIDE * q) % LANES, 1)
            row_o_o[...] = turn[N_QKV:N_QKV + N_O, 0:WIDE]
            turn[...] = turn[...].T
            col_q_o[...] = turn[0:WIDE, 0:N_QKV]
        else:
            out[...] = new

    def after_model(family):
        n = mats[family]
        model_ex(family, 'recv')
        both = total(mod_got[family], n_model)[:n]
        sums, z = both[:, 0:ROWS], both[:, ROWS:LANES]
        if family == 'b':
            mom = jnp.concatenate([row_q[...], col_o[...]], axis=0)
        else:
            mom = (row_in if family == 'in' else col_out)[...]
        new = BETA_TWO * mom + GAIN * (sums / full[family])
        ratio = z / new
        mean_part = GAIN * (sums / 512.0)
        if family == 'in':
            term = new
        elif family == 'out':
            term = mean_part
        else:
            term = jnp.where(lax.broadcasted_iota(jnp.int32, (n, ROWS), 0) < 54, new, mean_part)
        r0 = row0[family]
        tab[r0:r0 + n, 0:ROWS] = ratio
        tab[r0:r0 + n, ROWS:LANES] = term
        turned = tab[...].T
        e = EX_SLOT[family]
        scal[e] = jnp.zeros((8, LANES), F32)
        scal[e, 0:1, :] = jnp.sum(turned[:ROWS], axis=0, keepdims=True)
        scal[e, 1:2, :] = jnp.sum(turned[ROWS:], axis=0, keepdims=True)
        scal_ex(family, 'start')
        if family == 'b':
            row_q_o[...] = new[:N_QKV]
            col_o_o[...] = new[N_QKV:]
            rsub[e, r0:r0 + n, 0:ROWS] = lax.rsqrt(new)
        else:
            (row_in_o if family == 'in' else col_out_o)[...] = new
            tab[r0:r0 + n, 0:ROWS] = lax.rsqrt(new)
            rsub[e] = tab[...].T

    def after_scalars(family):
        e = EX_SLOT[family]
        scal_ex(family, 'recv')
        tot = total(got_s.at[e], n_data)
        q, s = tot[0:1], tot[1:2]
        w, v = w_all[0:1, :], w_all[1:2, :]
        rows = 512.0 if family == 'in' else float(full[family])
        size = 512.0 * full[family]
        m = (s if family == 'in' else BETA_TWO * v + s) / rows
        scale = jnp.sqrt(m) * (LR_BASE * jnp.maximum(1e-3, jnp.sqrt(w / size))) / jnp.maximum(1.0, jnp.sqrt(m * q / size))
        r0 = row0[family]
        if family == 'b':
            n = mats[family]
            tab[...] = jnp.broadcast_to(scale, (LANES, LANES)).T
            rsub[e, r0:r0 + n, 0:ROWS] = rsub[e, r0:r0 + n, 0:ROWS] * tab[r0:r0 + n, 0:ROWS]

            for ref, b0 in ((w_q, 0), (w_o, N_QKV)):
                def body(b, carry, ref=ref, b0=b0):
                    ref[b] = ref[b] - ht[b0 + b] * rsub[e, pl.ds(r0 + b0 + b, 1), 0:ROWS]
                    return carry
                lax.fori_loop(0, ref.shape[0], body, 0, unroll=6)
        else:
            ref = w_in if family == 'in' else w_out
            fac = rsub[e, 0:ROWS, :] * scale

            def body(b, carry):
                f = jnp.sum(jnp.where(lane_iota == r0 + b, fac, 0.0), axis=1, keepdims=True)
                ref[b] = ref[b] - grad[first[family] + b] * f
                return carry
            lax.fori_loop(0, count[family], body, 0, unroll=4)

    def sent_early():
        for ch in range(N_CH):
            for kind in range(7):
                transfer(kind, ch).wait_send()
        gather(mod_w, got_w, m_sems, EX_SLOT['w'], 'model', 'send')
        scal_ex('w', 'send')
        for family in ('b', 'in'):
            lane_ex(family, 'send')
            model_ex(family, 'send')
            scal_ex(family, 'send')

    def sent_late():
        lane_ex('out', 'send')
        model_ex('out', 'send')
        scal_ex('out', 'send')

    acc_t[...] = jnp.zeros_like(acc_t)
    tab[...] = jnp.zeros_like(tab)
    lane_sum[...] = jnp.zeros_like(lane_sum)

    convert(0)
    for cp in small + w_loads:
        cp.start()
    pl.semaphore_wait(barrier, n_data - 1 + n_model - 1)
    transfer(D2D, 0).start()
    last = N_CH - 1 + LAG_FINISH
    for k in range(1 - AHEAD, last + 1 + LAG_STATS['out'][2]):
        if k + AHEAD < N_CH:
            convert(k + AHEAD)
            transfer(D2D, k + AHEAD).start()
        if 0 <= k < N_CH:
            opposite(k)
        if 0 <= k - LAG_MERGE < N_CH:
            merge(k - LAG_MERGE)
        if 0 <= k - LAG_FINISH < N_CH:
            finish(k - LAG_FINISH)
        if k == 4:
            weights_start()
        if k == 5:
            weights_next()
        if k == 6:
            weights_done()
        for family in GROUPS:
            after = k - (LAST_CHUNK[family] + LAG_FINISH)
            if after == 0:
                lane_ex(family, 'start')
            if after == LAG_STATS[family][0]:
                after_lanes(family)
            if after == LAG_STATS[family][1]:
                after_model(family)
            if after == LAG_STATS[family][2]:
                after_scalars(family)
        if k == last + 1:
            sent_early()
    sent_late()


def deliver(*refs):
    srcs, dsts, sem = refs[:12], refs[12:24], refs[24]
    copies = [pltpu.make_async_copy(src, dst, sem.at[i]) for i, (src, dst) in enumerate(zip(srcs, dsts))]
    for cp in copies:
        cp.start()
    for cp in copies:
        cp.wait()


def solution(mesh):
    axis_sizes = dict(mesh.shape)
    n_data, n_model = axis_sizes['data'], axis_sizes['model']
    n_chips = n_data // 2
    rows_data = (P('data', None, None, 'model'), P(None, 'data', 'model'), P(None, 'data'), P(None, 'model'))
    rows_model = (P('data', None, 'model', None), P(None, 'model', 'data'), P(None, 'model'), P(None, 'data'))

    def vmem(*dims):
        return pltpu.VMEM(dims, F32)

    small = (vmem(24, ROWS), vmem(24, LANES), vmem(12, LANES), vmem(12, ROWS), vmem(54, ROWS), vmem(WIDE, 54), vmem(18, WIDE), vmem(18, ROWS))
    results = (vmem(24, ROWS, LANES), vmem(12, ROWS, LANES), vmem(54, WIDE, ROWS), vmem(18, WIDE, ROWS), *small)
    scratch = [
        *small, vmem(N_B, LANES), vmem(LANES, LANES),
        pltpu.VMEM((24, 512, LANES), jnp.bfloat16), pltpu.VMEM((12, LANES, 512), jnp.bfloat16),
        pltpu.VMEM((72, WIDE, 512), jnp.bfloat16),
        vmem(2, n_chips, N_SUP, ROWS, LANES), vmem(n_chips, N_SUP, ROWS, LANES),
        vmem(N_SUP, ROWS, LANES), vmem(N_SUP, ROWS, LANES), vmem(N_SUP, ROWS, LANES), vmem(N_SUP, ROWS, LANES),
        vmem(8, LANES), vmem(72, WIDE, ROWS),
        vmem(ROWS, LANES), vmem(ROWS, LANES), vmem(2, ROWS, LANES), vmem(N_B, 4, LANES),
        vmem(LANES, LANES), vmem(3, LANES, LANES), vmem(LANES, LANES), vmem(LANES, LANES),
        vmem(24, LANES), vmem(72, LANES), vmem(16, LANES), vmem(8, LANES),
        vmem(4, 8, LANES), vmem(n_data, 24, LANES), vmem(n_data, 24, LANES), vmem(n_data, 16, LANES),
        vmem(n_model, 24, LANES), vmem(n_model, 72, LANES), vmem(n_model, 16, LANES), vmem(n_model, 8, LANES),
        vmem(4, n_data, 8, LANES),
        pltpu.SemaphoreType.DMA((5,)), pltpu.SemaphoreType.DMA((4,)), pltpu.SemaphoreType.DMA((8,)),
        pltpu.SemaphoreType.DMA((7, N_CH)), pltpu.SemaphoreType.DMA((7, N_CH)),
        pltpu.SemaphoreType.DMA((3, n_data)), pltpu.SemaphoreType.DMA((3, n_data)),
        pltpu.SemaphoreType.DMA((4, n_model)), pltpu.SemaphoreType.DMA((4, n_model)),
        pltpu.SemaphoreType.DMA((4, n_data)), pltpu.SemaphoreType.DMA((4, n_data)),
    ]
    hbm, in_vmem = pl.BlockSpec(memory_space=pltpu.HBM), pl.BlockSpec(memory_space=pltpu.VMEM)

    def step_all(grad_in, w_in, row_in, col_in, grad_out, w_out, row_out, col_out,
                 grad_qkv, w_qkv, row_qkv, col_qkv, grad_o, w_o, row_o, col_o):
        kept = pl.pallas_call(
            functools.partial(kernel, n_data, n_model),
            name='adafactor_step',
            out_shape=results,
            in_specs=[hbm] * 16,
            out_specs=[in_vmem] * 12,
            scratch_shapes=scratch,
            compiler_params=pltpu.CompilerParams(collective_id=0, has_side_effects=True, vmem_limit_bytes=VMEM_LIMIT),
        )(grad_in[0], grad_out[0], grad_qkv[0].transpose(0, 2, 1), grad_o[0],
          w_in, w_out.transpose(0, 2, 1), w_qkv.transpose(0, 2, 1), w_o,
          row_in, col_in, row_out, col_out, row_qkv, col_qkv.T, row_o, col_o)
        (w_in_new, w_out_new, w_qkv_new, w_o_new, row_in_new, col_in_new, row_out_new, col_out_new,
         row_qkv_new, col_qkv_new, row_o_new, col_o_new) = pl.pallas_call(
            deliver,
            name='deliver',
            out_shape=[jax.ShapeDtypeStruct(r.shape, F32) for r in results],
            in_specs=[in_vmem] * 12,
            out_specs=[hbm] * 12,
            scratch_shapes=[pltpu.SemaphoreType.DMA((12,))],
            compiler_params=pltpu.CompilerParams(vmem_limit_bytes=10 ** 6),
        )(*(pltpu.with_memory_space_constraint(a, pltpu.VMEM) for a in kept))
        return (w_in_new, row_in_new, col_in_new, w_out_new.transpose(0, 2, 1), row_out_new, col_out_new,
                w_qkv_new.transpose(0, 2, 1), row_qkv_new, col_qkv_new.T, w_o_new, row_o_new, col_o_new)

    in_specs = rows_data + rows_model + rows_data + rows_model
    out_specs = rows_data[1:] + rows_model[1:] + rows_data[1:] + rows_model[1:]
    return jax.shard_map(step_all, mesh=mesh, in_specs=in_specs, out_specs=out_specs, check_vma=False)
```

```python
import functools

import jax
import jax.numpy as jnp
from jax import lax
from jax.experimental import pallas as pl
from jax.experimental.pallas import tpu as pltpu
from jax.sharding import PartitionSpec as P

OPT_STEP = 4
EPS_SQ = 1e-30
BETA_TWO = 1.0 - OPT_STEP ** -0.8
GAIN = 1.0 - BETA_TWO
LR_BASE = min(1e-2, OPT_STEP ** -0.5)
F32 = jnp.float32
LANES, ROWS, WIDE = 128, 64, 32
VMEM_LIMIT = 60 * 10 ** 6

N_IN, N_B, N_OUT = 24, 18, 12
N_SUP = N_IN + N_B + N_OUT
FIRST_B, FIRST_IN, FIRST_OUT = 0, N_B, N_B + N_IN
N_QKV, N_O = 54, 18
ROW_IN, ROW_OUT, ROW_B = 0, 24, 40
SIZES = (('b', (2, 4, 6, 6)), ('in', (6, 6, 6, 6)), ('out', (6, 4, 2)))


def cut():
    chunks, at = [], 0
    for family, sizes in SIZES:
        for n in sizes:
            chunks.append((family, at, n))
            at += n
    return tuple(chunks)


CHUNKS = cut()
N_CH = len(CHUNKS)
GROUPS = ('b', 'in', 'out')
LAST_CHUNK = {f: max(i for i, c in enumerate(CHUNKS) if c[0] == f) for f in GROUPS}
D2D, OPP_A, OPP_B, OWN_R, OWN_L, MRG_R, MRG_L = range(7)
SEND = (0, 1, 1, 2, 3, 2, 3)
LEFT, RIGHT = 3, 4
RECV = (D2D, OPP_A, OPP_B, LEFT, RIGHT, LEFT, RIGHT)
EX_SLOT = {'in': 0, 'b': 1, 'out': 2, 'w': 3}
AHEAD, EARLY_OWN, LAG_MERGE, LAG_FINISH = 2, 3, 2, 3
LAG_STATS = {'b': (1, 3, 5), 'in': (1, 4, 5), 'out': (1, 2, 3)}


def kernel(n_data, n_model, gin_h, gout_h, gq_h, go_h, win_h, wout_h, wq_h, wo_h,
           row_in_h, col_in_h, row_out_h, col_out_h, row_q_h, col_q_h, row_o_h, col_o_h,
           w_in, w_out, w_q, w_o, row_in_o, col_in_o, row_out_o, col_out_o, row_q_o, col_q_o, row_o_o, col_o_o,
           row_in, col_in, row_out, col_out, row_q, col_q, row_o, col_o, lane_b, turn,
           gin, gout, gb, part, peer, opp_in, left_in, right_in, grad, w_all, ht,
           lane_sum, rlane, acc_t, comp_b, tab, rsub, wtab, vtab, mod_in, mod_b, mod_out, mod_w,
           scal, dat_in, dat_b, dat_out, got_in, got_b, got_out, got_w, got_s,
           load_sem, w_sem, small_sem, snd, rcv, dsnd, drcv, msnd, mrcv, ssnd, srcv):
    me = lax.axis_index('data')
    mod = lax.axis_index('model')
    n_chips = n_data // 2
    x, c = lax.div(me, 2), lax.rem(me, 2)
    xr, xl, xo = lax.rem(x + 1, n_chips), lax.rem(x + 3, n_chips), lax.rem(x + 2, n_chips)
    partner, right, left = 2 * x + 1 - c, 2 * xr + c, 2 * xl + c
    full = {'in': n_model * LANES, 'out': n_model * LANES, 'b': n_model * WIDE}
    count = {'in': N_IN, 'b': N_B, 'out': N_OUT}
    mats = {'in': N_IN, 'b': 4 * N_B, 'out': N_OUT}
    first = {'in': FIRST_IN, 'b': FIRST_B, 'out': FIRST_OUT}
    row0 = {'in': ROW_IN, 'b': ROW_B, 'out': ROW_OUT}
    mod_blk = {'in': mod_in, 'b': mod_b, 'out': mod_out}
    dat_got = {'in': dat_in, 'b': dat_b, 'out': dat_out}
    mod_got = {'in': got_in, 'b': got_b, 'out': got_out}
    lane_rows = {'in': (0, 24), 'b': (24, 24), 'out': (48, 16)}

    loads = [pltpu.make_async_copy(gq_h.at[pl.ds(0, 8)], gb.at[pl.ds(0, 8)], load_sem.at[0]),
             pltpu.make_async_copy(gq_h.at[pl.ds(8, 46)], gb.at[pl.ds(8, 46)], load_sem.at[1]),
             pltpu.make_async_copy(go_h, gb.at[pl.ds(54, 18)], load_sem.at[2]),
             pltpu.make_async_copy(gin_h, gin, load_sem.at[3]),
             pltpu.make_async_copy(gout_h, gout, load_sem.at[4])]
    w_loads = [pltpu.make_async_copy(win_h, w_in, w_sem.at[0]),
               pltpu.make_async_copy(wout_h, w_out, w_sem.at[1]),
               pltpu.make_async_copy(wq_h, w_q, w_sem.at[2]),
               pltpu.make_async_copy(wo_h, w_o, w_sem.at[3])]
    small = [pltpu.make_async_copy(src, dst, small_sem.at[i]) for i, (src, dst) in enumerate((
        (row_in_h, row_in), (col_in_h, col_in), (row_out_h, row_out), (col_out_h, col_out),
        (row_q_h, row_q), (col_q_h, col_q), (row_o_h, row_o), (col_o_h, col_o)))]
    for cp in loads:
        cp.start()

    barrier = pltpu.get_barrier_semaphore()

    def others(axis):
        side = 2 if axis == 'data' else 4
        n, rank = (n_data, me) if axis == 'data' else (n_model, mod)
        high, low, rows = lax.div(rank, side), lax.rem(rank, side), n // side

        def hops(d):
            up, over = d // side, d % side
            return min(up, rows - up) * (side - 1) + min(over, side - over)

        for d in sorted(range(1, n), key=lambda d: -hops(d)):
            yield lax.rem(high + d // side, rows) * side + lax.rem(low + d % side, side)

    for axis in ('model', 'data'):
        for who in others(axis):
            pl.semaphore_signal(barrier, inc=1, device_id={axis: who}, device_id_type=pl.DeviceIdType.MESH)

    def remote(src, dst, ssem, rsem, axis, who):
        return pltpu.make_async_remote_copy(src_ref=src, dst_ref=dst, send_sem=ssem, recv_sem=rsem,
                                            device_id={axis: who}, device_id_type=pl.DeviceIdType.MESH)

    def transfer(kind, ch):
        _, b0, n = CHUNKS[ch]
        n_a = n // 2
        every, half_a, half_b = pl.ds(b0, n), pl.ds(b0, n_a), pl.ds(b0 + n_a, n - n_a)
        src, dst, who = {
            D2D: lambda: (part.at[1 - c, :, every], peer.at[:, every], partner),
            OPP_A: lambda: (part.at[c, xo, half_a], opp_in.at[half_a], right),
            OPP_B: lambda: (part.at[c, xo, half_b], opp_in.at[half_b], left),
            OWN_R: lambda: (part.at[c, xr, half_b], left_in.at[half_b], right),
            OWN_L: lambda: (part.at[c, xl, half_a], right_in.at[half_a], left),
            MRG_R: lambda: (part.at[c, xr, half_a], left_in.at[half_a], right),
            MRG_L: lambda: (part.at[c, xl, half_b], right_in.at[half_b], left),
        }[kind]()
        return remote(src, dst, snd.at[SEND[kind]], rcv.at[RECV[kind], ch], 'data', who)

    def convert(ch):
        family, b0, n = CHUNKS[ch]
        if ch == 0:
            loads[0].wait()
        elif ch == 1:
            loads[1].wait()
            loads[2].wait()
        elif b0 == FIRST_IN:
            loads[3].wait()
        elif b0 == FIRST_OUT:
            loads[4].wait()

        def body(i, carry):
            b = b0 + i
            for t in range(n_chips):
                if family == 'in':
                    tile = gin[b - FIRST_IN, pl.ds(LANES * t, LANES), :].astype(F32)
                elif family == 'out':
                    tile = gout[b - FIRST_OUT, :, pl.ds(LANES * t, LANES)].astype(F32).T
                else:
                    four = gb[pl.ds(4 * (b - FIRST_B), 4), :, pl.ds(LANES * t, LANES)].astype(F32)
                    tile = four.reshape(LANES, LANES).T
                part[0, t, b] = tile[:ROWS]
                part[1, t, b] = tile[ROWS:]
            return carry

        lax.fori_loop(0, n, body, 0)

    def add_peer(ch, dest):
        _, b0, n = CHUNKS[ch]

        def body(i, carry):
            b = b0 + i
            part[c, dest, b] = part[c, dest, b] + peer[dest, b]
            return carry
        lax.fori_loop(0, n, body, 0, unroll=2)

    def opposite(ch):
        transfer(D2D, ch).wait_recv()
        add_peer(ch, xo)
        transfer(OPP_A, ch).start()
        transfer(OPP_B, ch).start()
        add_peer(ch, xr)
        add_peer(ch, xl)
        if ch < EARLY_OWN:
            own(ch)
        add_peer(ch, x)

    def own(ch):
        transfer(OWN_R, ch).start()
        transfer(OWN_L, ch).start()

    def merge(ch):
        _, b0, n = CHUNKS[ch]
        n_a = n // 2

        def add(dest, lo, hi):
            def body(b, carry):
                part[c, dest, b] = part[c, dest, b] + opp_in[b]
                return carry
            lax.fori_loop(lo, hi, body, 0)

        transfer(OPP_A, ch).wait_recv()
        add(xr, b0, b0 + n_a)
        transfer(MRG_R, ch).start()
        transfer(OPP_B, ch).wait_recv()
        add(xl, b0 + n_a, b0 + n)
        transfer(MRG_L, ch).start()
        if ch >= EARLY_OWN:
            own(ch)

    lane_iota = lax.broadcasted_iota(jnp.int32, (ROWS, LANES), 1)

    def finish(ch):
        family, b0, n = CHUNKS[ch]
        every = pl.ds(b0, n)
        remote(left_in.at[every], left_in.at[every], snd.at[2], rcv.at[LEFT, ch], 'data', right).wait_recv()
        remote(right_in.at[every], right_in.at[every], snd.at[3], rcv.at[RIGHT, ch], 'data', left).wait_recv()
        base = lane_rows[family][0] - first[family]

        def block(b):
            g = (part[c, x, b] + left_in[b] + right_in[b]) * (1.0 / n_data)
            grad[b] = g
            sq = g * g + EPS_SQ
            lane_sum[pl.ds(base + b, 1), :] = jnp.sum(sq, axis=0, keepdims=True)
            return g, sq

        if family == 'b':
            def body(i, carry):
                b = b0 + i
                g, _ = block(b)
                gt = g.T
                st = (gt * gt + EPS_SQ).reshape(4, WIDE, ROWS)
                comp_b[pl.ds(b - FIRST_B, 1), :, 0:ROWS] = jnp.sum(st, axis=1)[None]
                return carry
            lax.fori_loop(0, n, body, 0, unroll=2)
        else:
            which = 0 if family == 'in' else 1

            def body(i, acc):
                b = b0 + i
                _, sq = block(b)
                return jnp.where(lane_iota == b - first[family], jnp.sum(sq, axis=1, keepdims=True), acc)
            acc_t[which] = lax.fori_loop(0, n, body, acc_t[which], unroll=2)

    def gather(src, dst, sems, slot, axis, op):
        send, recv = sems[0].at[slot], sems[1].at[slot]
        rank, n = (me, n_data) if axis == 'data' else (mod, n_model)
        if op == 'start':
            dst[rank] = src[...]
            for who in others(axis):
                remote(src, dst.at[rank], send, recv, axis, who).start()
            return
        rest = dst.at[pl.ds(0, n - 1)]
        done = remote(rest, rest, send, recv, axis, rank)
        if op == 'recv':
            done.wait_recv()
        else:
            done.wait_send()

    def total(dst, n):
        acc = dst[0]
        for r in range(1, n):
            acc = acc + dst[r]
        return acc

    d_sems, m_sems, s_sems = (dsnd, drcv), (msnd, mrcv), (ssnd, srcv)

    def lane_ex(family, op):
        r0, n = lane_rows[family]
        gather(lane_sum.at[pl.ds(r0, n)], dat_got[family], d_sems, EX_SLOT[family], 'data', op)

    def model_ex(family, op):
        gather(mod_blk[family], mod_got[family], m_sems, EX_SLOT[family], 'model', op)

    def scal_ex(family, op):
        gather(scal.at[EX_SLOT[family]], got_s.at[EX_SLOT[family]], s_sems, EX_SLOT[family], 'data', op)

    def weights_start():
        for cp in w_loads + small:
            cp.wait()
        turn[...] = jnp.zeros_like(turn)
        turn[0:WIDE, 0:N_QKV] = col_q[...]
        turn[...] = turn[...].T
        turn[N_QKV:N_QKV + N_O, 0:WIDE] = row_o[...]
        row = turn[pl.ds(0, N_B, stride=4), :]
        for q in range(1, 4):
            row = row + pltpu.roll(turn[pl.ds(q, N_B, stride=4), :], WIDE * q, 1)
        lane_b[...] = row
        wtab[...] = jnp.zeros_like(wtab)
        vtab[...] = jnp.zeros_like(vtab)

        def squares(ref, row, width):
            def body(b, carry):
                w = ref[b]
                wtab[pl.ds(row + b, 1), 0:width] = jnp.sum(w * w, axis=0, keepdims=True)
                return carry
            lax.fori_loop(0, ref.shape[0], body, 0, unroll=6)

        squares(w_in, ROW_IN, LANES)
        squares(w_out, ROW_OUT, LANES)
        squares(w_q, ROW_B, ROWS)
        squares(w_o, ROW_B + N_QKV, ROWS)
        vtab[ROW_OUT:ROW_OUT + N_OUT, :] = row_out[...]
        vtab[ROW_B + 54:ROW_B + 72, 0:WIDE] = row_o[...]
        mod_w[0:1, :] = jnp.sum(wtab[...].T, axis=0, keepdims=True)
        mod_w[1:2, :] = jnp.sum(vtab[...].T, axis=0, keepdims=True) / n_data
        gather(mod_w, got_w, m_sems, EX_SLOT['w'], 'model', 'start')

    def weights_next():
        gather(mod_w, got_w, m_sems, EX_SLOT['w'], 'model', 'recv')
        scal[EX_SLOT['w']] = total(got_w, n_model)
        scal_ex('w', 'start')

    def weights_done():
        scal_ex('w', 'recv')
        w_all[...] = total(got_s.at[EX_SLOT['w']], n_data)

    def after_lanes(family):
        r0, _ = lane_rows[family]
        n = count[family]
        lane_ex(family, 'recv')
        mom, out = {'in': (col_in, col_in_o), 'out': (row_out, row_out_o), 'b': (lane_b, None)}[family]
        new = BETA_TWO * mom[...] + GAIN * (total(dat_got[family], n_data)[:n] / 512.0)
        rlane[r0:r0 + n, :] = lax.rsqrt(new)
        if family == 'b':
            def body(s, carry):
                h = grad[FIRST_B + s] * rlane[pl.ds(r0 + s, 1), :]
                t = h.T.reshape(4, WIDE, ROWS)
                ht[pl.ds(4 * s, 4)] = t
                comp_b[pl.ds(s, 1), :, ROWS:LANES] = jnp.sum(t * t, axis=1)[None]
                return carry
            lax.fori_loop(0, N_B, body, 0, unroll=3)
            mod_b[...] = comp_b[...].reshape(4 * N_B, LANES)
        else:
            which = 0 if family == 'in' else 1

            def body(b, acc):
                h = grad[first[family] + b] * rlane[pl.ds(r0 + b, 1), :]
                grad[first[family] + b] = h
                return jnp.where(lane_iota == b, jnp.sum(h * h, axis=1, keepdims=True), acc)
            acc_z = lax.fori_loop(0, n, body, jnp.zeros((ROWS, LANES), F32), unroll=4)
            both = jnp.concatenate([acc_t[which], acc_z], axis=0).T
            mod_blk[family][...] = both[:mod_blk[family].shape[0]]
        model_ex(family, 'start')
        if family == 'b':
            turn[...] = jnp.zeros_like(turn)
            for q in range(4):
                turn[pl.ds(q, N_B, stride=4), :] = pltpu.roll(new, (LANES - WIDE * q) % LANES, 1)
            row_o_o[...] = turn[N_QKV:N_QKV + N_O, 0:WIDE]
            turn[...] = turn[...].T
            col_q_o[...] = turn[0:WIDE, 0:N_QKV]
        else:
            out[...] = new

    def after_model(family):
        n = mats[family]
        model_ex(family, 'recv')
        both = total(mod_got[family], n_model)[:n]
        sums, z = both[:, 0:ROWS], both[:, ROWS:LANES]
        if family == 'b':
            mom = jnp.concatenate([row_q[...], col_o[...]], axis=0)
        else:
            mom = (row_in if family == 'in' else col_out)[...]
        new = BETA_TWO * mom + GAIN * (sums / full[family])
        ratio = z / new
        mean_part = GAIN * (sums / 512.0)
        if family == 'in':
            term = new
        elif family == 'out':
            term = mean_part
        else:
            term = jnp.where(lax.broadcasted_iota(jnp.int32, (n, ROWS), 0) < 54, new, mean_part)
        r0 = row0[family]
        tab[r0:r0 + n, 0:ROWS] = ratio
        tab[r0:r0 + n, ROWS:LANES] = term
        turned = tab[...].T
        e = EX_SLOT[family]
        scal[e, 0:1, :] = jnp.sum(turned[:ROWS], axis=0, keepdims=True)
        scal[e, 1:2, :] = jnp.sum(turned[ROWS:], axis=0, keepdims=True)
        scal_ex(family, 'start')
        if family == 'b':
            row_q_o[...] = new[:N_QKV]
            col_o_o[...] = new[N_QKV:]
            rsub[e, r0:r0 + n, 0:ROWS] = lax.rsqrt(new)
        else:
            (row_in_o if family == 'in' else col_out_o)[...] = new
            tab[r0:r0 + n, 0:ROWS] = lax.rsqrt(new)
            rsub[e] = tab[...].T

    def after_scalars(family):
        e = EX_SLOT[family]
        scal_ex(family, 'recv')
        tot = total(got_s.at[e], n_data)
        q, s = tot[0:1], tot[1:2]
        w, v = w_all[0:1, :], w_all[1:2, :]
        rows = 512.0 if family == 'in' else float(full[family])
        size = 512.0 * full[family]
        m = (s if family == 'in' else BETA_TWO * v + s) / rows
        scale = jnp.sqrt(m) * (LR_BASE * jnp.maximum(1e-3, jnp.sqrt(w / size))) / jnp.maximum(1.0, jnp.sqrt(m * q / size))
        r0 = row0[family]
        if family == 'b':
            n = mats[family]
            tab[...] = jnp.broadcast_to(scale, (LANES, LANES)).T
            rsub[e, r0:r0 + n, 0:ROWS] = rsub[e, r0:r0 + n, 0:ROWS] * tab[r0:r0 + n, 0:ROWS]

            for ref, b0 in ((w_q, 0), (w_o, N_QKV)):
                def body(b, carry, ref=ref, b0=b0):
                    ref[b] = ref[b] - ht[b0 + b] * rsub[e, pl.ds(r0 + b0 + b, 1), 0:ROWS]
                    return carry
                lax.fori_loop(0, ref.shape[0], body, 0, unroll=6)
        else:
            ref = w_in if family == 'in' else w_out
            fac = rsub[e, 0:ROWS, :] * scale

            def body(b, carry):
                f = jnp.sum(jnp.where(lane_iota == r0 + b, fac, 0.0), axis=1, keepdims=True)
                ref[b] = ref[b] - grad[first[family] + b] * f
                return carry
            lax.fori_loop(0, count[family], body, 0, unroll=4)

    def sent_early():
        for i, ref in enumerate((peer, opp_in, left_in, right_in)):
            remote(ref, ref, snd.at[i], rcv.at[0, 0], 'data', partner).wait_send()
        gather(mod_w, got_w, m_sems, EX_SLOT['w'], 'model', 'send')
        scal_ex('w', 'send')
        for family in ('b', 'in'):
            lane_ex(family, 'send')
            model_ex(family, 'send')
            scal_ex(family, 'send')

    def sent_late():
        lane_ex('out', 'send')
        model_ex('out', 'send')
        scal_ex('out', 'send')

    acc_t[...] = jnp.zeros_like(acc_t)
    tab[...] = jnp.zeros_like(tab)
    lane_sum[...] = jnp.zeros_like(lane_sum)

    convert(0)
    for cp in small + w_loads:
        cp.start()
    pl.semaphore_wait(barrier, n_data - 1 + n_model - 1)
    transfer(D2D, 0).start()
    last = N_CH - 1 + LAG_FINISH
    for k in range(1 - AHEAD, last + 1 + LAG_STATS['out'][2]):
        if 0 <= k < N_CH:
            opposite(k)
        if k + AHEAD < N_CH:
            convert(k + AHEAD)
            transfer(D2D, k + AHEAD).start()
        for ch in range(N_CH):
            if k == ch + (LAG_MERGE if ch < N_CH - 1 else 1):
                merge(ch)
        if k == 4:
            weights_start()
        if k == 6:
            weights_next()
        if k == 8:
            weights_done()
        if k == last + 2:
            sent_early()
        for family in GROUPS:
            after = k - (LAST_CHUNK[family] + LAG_FINISH)
            if after == LAG_STATS[family][0]:
                after_lanes(family)
            if after == LAG_STATS[family][1]:
                after_model(family)
            if after == LAG_STATS[family][2]:
                after_scalars(family)
        if 0 <= k - LAG_FINISH < N_CH:
            finish(k - LAG_FINISH)
        for family in GROUPS:
            if k == LAST_CHUNK[family] + LAG_FINISH:
                lane_ex(family, 'start')
    sent_late()


def deliver(*refs):
    srcs, dsts, sem = refs[:12], refs[12:24], refs[24]
    copies = [pltpu.make_async_copy(src, dst, sem.at[i]) for i, (src, dst) in enumerate(zip(srcs, dsts))]
    for cp in copies:
        cp.start()
    for cp in copies:
        cp.wait()


def solution(mesh):
    axis_sizes = dict(mesh.shape)
    n_data, n_model = axis_sizes['data'], axis_sizes['model']
    n_chips = n_data // 2
    rows_data = (P('data', None, None, 'model'), P(None, 'data', 'model'), P(None, 'data'), P(None, 'model'))
    rows_model = (P('data', None, 'model', None), P(None, 'model', 'data'), P(None, 'model'), P(None, 'data'))

    def vmem(*dims):
        return pltpu.VMEM(dims, F32)

    small = (vmem(24, ROWS), vmem(24, LANES), vmem(12, LANES), vmem(12, ROWS), vmem(54, ROWS), vmem(WIDE, 54), vmem(18, WIDE), vmem(18, ROWS))
    results = (vmem(24, ROWS, LANES), vmem(12, ROWS, LANES), vmem(54, WIDE, ROWS), vmem(18, WIDE, ROWS), *small)
    scratch = [
        *small, vmem(N_B, LANES), vmem(LANES, LANES),
        pltpu.VMEM((24, 512, LANES), jnp.bfloat16), pltpu.VMEM((12, LANES, 512), jnp.bfloat16),
        pltpu.VMEM((72, WIDE, 512), jnp.bfloat16),
        vmem(2, n_chips, N_SUP, ROWS, LANES), vmem(n_chips, N_SUP, ROWS, LANES),
        vmem(N_SUP, ROWS, LANES), vmem(N_SUP, ROWS, LANES), vmem(N_SUP, ROWS, LANES), vmem(N_SUP, ROWS, LANES),
        vmem(2, LANES), vmem(72, WIDE, ROWS),
        vmem(ROWS, LANES), vmem(ROWS, LANES), vmem(2, ROWS, LANES), vmem(N_B, 4, LANES),
        vmem(LANES, LANES), vmem(3, LANES, LANES), vmem(LANES, LANES), vmem(LANES, LANES),
        vmem(24, LANES), vmem(72, LANES), vmem(16, LANES), vmem(2, LANES),
        vmem(4, 2, LANES), vmem(n_data, 24, LANES), vmem(n_data, 24, LANES), vmem(n_data, 16, LANES),
        vmem(n_model, 24, LANES), vmem(n_model, 72, LANES), vmem(n_model, 16, LANES), vmem(n_model, 2, LANES),
        vmem(4, n_data, 2, LANES),
        pltpu.SemaphoreType.DMA((5,)), pltpu.SemaphoreType.DMA((4,)), pltpu.SemaphoreType.DMA((8,)),
        pltpu.SemaphoreType.DMA((4,)), pltpu.SemaphoreType.DMA((5, N_CH)),
        *(pltpu.SemaphoreType.DMA((n,)) for n in (3, 3, 4, 4, 4, 4)),
    ]
    hbm, in_vmem = pl.BlockSpec(memory_space=pltpu.HBM), pl.BlockSpec(memory_space=pltpu.VMEM)

    def step_all(grad_in, w_in, row_in, col_in, grad_out, w_out, row_out, col_out,
                 grad_qkv, w_qkv, row_qkv, col_qkv, grad_o, w_o, row_o, col_o):
        kept = pl.pallas_call(
            functools.partial(kernel, n_data, n_model),
            name='adafactor_step',
            out_shape=results,
            in_specs=[hbm] * 16,
            out_specs=[in_vmem] * 12,
            scratch_shapes=scratch,
            compiler_params=pltpu.CompilerParams(collective_id=0, has_side_effects=True, vmem_limit_bytes=VMEM_LIMIT),
        )(grad_in[0], grad_out[0], grad_qkv[0].transpose(0, 2, 1), grad_o[0],
          w_in, w_out.transpose(0, 2, 1), w_qkv.transpose(0, 2, 1), w_o,
          row_in, col_in, row_out, col_out, row_qkv, col_qkv.T, row_o, col_o)
        (w_in_new, w_out_new, w_qkv_new, w_o_new, row_in_new, col_in_new, row_out_new, col_out_new,
         row_qkv_new, col_qkv_new, row_o_new, col_o_new) = pl.pallas_call(
            deliver,
            name='deliver',
            out_shape=[jax.ShapeDtypeStruct(r.shape, F32) for r in results],
            in_specs=[in_vmem] * 12,
            out_specs=[hbm] * 12,
            scratch_shapes=[pltpu.SemaphoreType.DMA((12,))],
            compiler_params=pltpu.CompilerParams(vmem_limit_bytes=10 ** 6),
        )(*(pltpu.with_memory_space_constraint(a, pltpu.VMEM) for a in kept))
        return (w_in_new, row_in_new, col_in_new, w_out_new.transpose(0, 2, 1), row_out_new, col_out_new,
                w_qkv_new.transpose(0, 2, 1), row_qkv_new, col_qkv_new.T, w_o_new, row_o_new, col_o_new)

    in_specs = rows_data + rows_model + rows_data + rows_model
    out_specs = rows_data[1:] + rows_model[1:] + rows_data[1:] + rows_model[1:]
    return jax.shard_map(step_all, mesh=mesh, in_specs=in_specs, out_specs=out_specs, check_vma=False)
```

```python
import functools

import jax
import jax.numpy as jnp
from jax import lax
from jax.experimental import pallas as pl
from jax.experimental.pallas import tpu as pltpu
from jax.sharding import PartitionSpec as P

OPT_STEP = 4
EPS_SQ = 1e-30
BETA_TWO = 1.0 - OPT_STEP ** -0.8
GAIN = 1.0 - BETA_TWO
LR_BASE = min(1e-2, OPT_STEP ** -0.5)
F32 = jnp.float32
LANES, ROWS, WIDE = 128, 64, 32
VMEM_LIMIT = 60 * 10 ** 6

N_IN, N_B, N_OUT = 24, 18, 12
N_SUP = N_IN + N_B + N_OUT
FIRST_B, FIRST_IN, FIRST_OUT = 0, N_B, N_B + N_IN
N_QKV, N_O = 54, 18
ROW_IN, ROW_OUT, ROW_B = 0, 24, 40
GROUPS = {'b': ('b', FIRST_B, N_B), 'in': ('in', FIRST_IN, N_IN), 'out_a': ('out', FIRST_OUT, 8), 'out_b': ('out', FIRST_OUT + 8, 4)}
SIZES = (('b', (2, 4, 6, 6)), ('in', (6, 6, 6, 6)), ('out_a', (4, 4)), ('out_b', (2, 2)))


def cut():
    chunks, at = [], 0
    for group, sizes in SIZES:
        for n in sizes:
            chunks.append((group, at, n))
            at += n
    return tuple(chunks)


CHUNKS = cut()
N_CH = len(CHUNKS)
LAST_CHUNK = {g: max(i for i, c in enumerate(CHUNKS) if c[0] == g) for g in GROUPS}
D2D, OPP_A, OPP_B, OWN_R, OWN_L, MRG_R, MRG_L = range(7)
SEND = (0, 1, 1, 2, 3, 2, 3)
LEFT, RIGHT = 3, 4
RECV = (D2D, OPP_A, OPP_B, LEFT, RIGHT, LEFT, RIGHT)
SLOT = {'b': 0, 'in': 1, 'out_a': 2, 'out_b': 3, 'out': 2, 'w': 4}
LANE_ROW = {'b': 0, 'in': 24, 'out_a': 48, 'out_b': 56}
TAB_ROW = {'b': ROW_B, 'in': ROW_IN, 'out_a': ROW_OUT, 'out_b': ROW_OUT + 8}
AHEAD, EARLY_OWN, LAG_MERGE, LAG_FINISH = 2, 3, 2, 3


def kernel(n_data, n_model, gin_h, gout_h, gq_h, go_h, win_h, wout_h, wq_h, wo_h,
           row_in_h, col_in_h, row_out_h, col_out_h, row_q_h, col_q_h, row_o_h, col_o_h,
           w_in, w_out, w_q, w_o, row_in_o, col_in_o, row_out_o, col_out_o, row_q_o, col_q_o, row_o_o, col_o_o,
           row_in, col_in, row_out, col_out, row_q, col_q, row_o, col_o, lane_b, turn,
           gin, gout, gb, part, peer, opp_in, left_in, right_in, grad, w_all, ht,
           sum_b, sum_in, sum_a, sum_o, near_b, near_in, both_b, both_in, rlane, acc_t, comp_b, tab, rtab, rsub, wtab, vtab,
           mod_b, mod_in, mod_a, mod_o, mod_w, scal, dat_b, dat_in, dat_a, dat_o, got_b, got_in, got_a, got_o, got_w, got_s,
           load_sem, w_sem, small_sem, snd, rcv, psnd, prcv, dsnd, drcv, msnd, mrcv, ssnd, srcv):
    me = lax.axis_index('data')
    mod = lax.axis_index('model')
    n_chips = n_data // 2
    x, c = lax.div(me, 2), lax.rem(me, 2)
    xr, xl, xo = lax.rem(x + 1, n_chips), lax.rem(x + 3, n_chips), lax.rem(x + 2, n_chips)
    partner, right, left = 2 * x + 1 - c, 2 * xr + c, 2 * xl + c
    full = {'in': n_model * LANES, 'out': n_model * LANES, 'b': n_model * WIDE}
    lane_sum = {'b': sum_b, 'in': sum_in, 'out_a': sum_a, 'out_b': sum_o}
    near = {'b': near_b, 'in': near_in}
    both = {'b': both_b, 'in': both_in}
    dat_got = {'b': dat_b, 'in': dat_in, 'out_a': dat_a, 'out_b': dat_o}
    mod_blk = {'b': mod_b, 'in': mod_in, 'out_a': mod_a, 'out_b': mod_o}
    mod_got = {'b': got_b, 'in': got_in, 'out_a': got_a, 'out_b': got_o}

    loads = [pltpu.make_async_copy(gq_h.at[pl.ds(0, 8)], gb.at[pl.ds(0, 8)], load_sem.at[0]),
             pltpu.make_async_copy(gq_h.at[pl.ds(8, 46)], gb.at[pl.ds(8, 46)], load_sem.at[1]),
             pltpu.make_async_copy(go_h, gb.at[pl.ds(54, 18)], load_sem.at[2]),
             pltpu.make_async_copy(gin_h, gin, load_sem.at[3]),
             pltpu.make_async_copy(gout_h, gout, load_sem.at[4])]
    w_loads = [pltpu.make_async_copy(win_h, w_in, w_sem.at[0]),
               pltpu.make_async_copy(wout_h, w_out, w_sem.at[1]),
               pltpu.make_async_copy(wq_h, w_q, w_sem.at[2]),
               pltpu.make_async_copy(wo_h, w_o, w_sem.at[3])]
    small = [pltpu.make_async_copy(src, dst, small_sem.at[i]) for i, (src, dst) in enumerate((
        (row_in_h, row_in), (col_in_h, col_in), (row_out_h, row_out), (col_out_h, col_out),
        (row_q_h, row_q), (col_q_h, col_q), (row_o_h, row_o), (col_o_h, col_o)))]
    for cp in loads:
        cp.start()

    barrier = pltpu.get_barrier_semaphore()

    def others(axis):
        side = 4 if axis == 'model' else 2
        n, rank = (n_model, mod) if axis == 'model' else (n_data, me)
        high, low, rows = lax.div(rank, side), lax.rem(rank, side), n // side

        def hops(d):
            up, over = d // side, d % side
            return min(up, rows - up) * (side - 1) + min(over, side - over)

        for d in sorted(range(1, n), key=lambda d: -hops(d)):
            if axis != 'chip' or d % side == 0:
                yield lax.rem(high + d // side, rows) * side + lax.rem(low + d % side, side)

    for axis in ('model', 'data'):
        for who in others(axis):
            pl.semaphore_signal(barrier, inc=1, device_id={axis: who}, device_id_type=pl.DeviceIdType.MESH)

    def remote(src, dst, ssem, rsem, axis, who):
        return pltpu.make_async_remote_copy(src_ref=src, dst_ref=dst, send_sem=ssem, recv_sem=rsem,
                                            device_id={axis: who}, device_id_type=pl.DeviceIdType.MESH)

    def transfer(kind, ch):
        _, b0, n = CHUNKS[ch]
        n_a = n // 2
        every, half_a, half_b = pl.ds(b0, n), pl.ds(b0, n_a), pl.ds(b0 + n_a, n - n_a)
        src, dst, who = {
            D2D: lambda: (part.at[1 - c, :, every], peer.at[:, every], partner),
            OPP_A: lambda: (part.at[c, xo, half_a], opp_in.at[half_a], right),
            OPP_B: lambda: (part.at[c, xo, half_b], opp_in.at[half_b], left),
            OWN_R: lambda: (part.at[c, xr, half_b], left_in.at[half_b], right),
            OWN_L: lambda: (part.at[c, xl, half_a], right_in.at[half_a], left),
            MRG_R: lambda: (part.at[c, xr, half_a], left_in.at[half_a], right),
            MRG_L: lambda: (part.at[c, xl, half_b], right_in.at[half_b], left),
        }[kind]()
        return remote(src, dst, snd.at[SEND[kind]], rcv.at[RECV[kind], ch], 'data', who)

    def convert(ch):
        group, b0, n = CHUNKS[ch]
        family = GROUPS[group][0]
        if ch == 0:
            loads[0].wait()
        elif ch == 1:
            loads[1].wait()
            loads[2].wait()
        elif b0 == FIRST_IN:
            loads[3].wait()
        elif b0 == FIRST_OUT:
            loads[4].wait()

        def body(i, carry):
            b = b0 + i
            for t in range(n_chips):
                if family == 'in':
                    tile = gin[b - FIRST_IN, pl.ds(LANES * t, LANES), :].astype(F32)
                elif family == 'out':
                    tile = gout[b - FIRST_OUT, :, pl.ds(LANES * t, LANES)].astype(F32).T
                else:
                    four = gb[pl.ds(4 * (b - FIRST_B), 4), :, pl.ds(LANES * t, LANES)].astype(F32)
                    tile = four.reshape(LANES, LANES).T
                part[0, t, b] = tile[:ROWS]
                part[1, t, b] = tile[ROWS:]
            return carry

        lax.fori_loop(0, n, body, 0)

    def add_peer(ch, dest):
        _, b0, n = CHUNKS[ch]

        def body(i, carry):
            b = b0 + i
            part[c, dest, b] = part[c, dest, b] + peer[dest, b]
            return carry
        lax.fori_loop(0, n, body, 0, unroll=2)

    def opposite(ch):
        transfer(D2D, ch).wait_recv()
        add_peer(ch, xo)
        transfer(OPP_A, ch).start()
        transfer(OPP_B, ch).start()
        add_peer(ch, xr)
        add_peer(ch, xl)
        if ch < EARLY_OWN:
            own(ch)
        add_peer(ch, x)

    def own(ch):
        transfer(OWN_R, ch).start()
        transfer(OWN_L, ch).start()

    def merge(ch):
        _, b0, n = CHUNKS[ch]
        n_a = n // 2

        def add(dest, lo, hi):
            def body(b, carry):
                part[c, dest, b] = part[c, dest, b] + opp_in[b]
                return carry
            lax.fori_loop(lo, hi, body, 0)

        transfer(OPP_A, ch).wait_recv()
        add(xr, b0, b0 + n_a)
        transfer(MRG_R, ch).start()
        transfer(OPP_B, ch).wait_recv()
        add(xl, b0 + n_a, b0 + n)
        transfer(MRG_L, ch).start()
        if ch >= EARLY_OWN:
            own(ch)

    lane_iota = lax.broadcasted_iota(jnp.int32, (ROWS, LANES), 1)

    def finish(ch):
        group, b0, n = CHUNKS[ch]
        family, g0, _ = GROUPS[group]
        every = pl.ds(b0, n)
        remote(left_in.at[every], left_in.at[every], snd.at[2], rcv.at[LEFT, ch], 'data', right).wait_recv()
        remote(right_in.at[every], right_in.at[every], snd.at[3], rcv.at[RIGHT, ch], 'data', left).wait_recv()
        def block(b):
            g = (part[c, x, b] + left_in[b] + right_in[b]) * (1.0 / n_data)
            grad[b] = g
            sq = g * g + EPS_SQ
            lane_sum[group][pl.ds(b - g0, 1), :] = jnp.sum(sq, axis=0, keepdims=True)
            return g, sq

        if family == 'b':
            def body(i, carry):
                b = b0 + i
                g, _ = block(b)
                gt = g.T
                st = (gt * gt + EPS_SQ).reshape(4, WIDE, ROWS)
                comp_b[pl.ds(b - FIRST_B, 1), :, 0:ROWS] = jnp.sum(st, axis=1)[None]
                return carry
            lax.fori_loop(0, n, body, 0, unroll=2)
        else:
            which = 0 if family == 'in' else 1

            def body(i, acc):
                b = b0 + i
                _, sq = block(b)
                return jnp.where(lane_iota == b - (FIRST_IN if family == 'in' else FIRST_OUT), jnp.sum(sq, axis=1, keepdims=True), acc)
            acc_t[which] = lax.fori_loop(0, n, body, acc_t[which], unroll=2)

    def gather(src, dst, sems, slot, axis, op):
        send, recv = sems[0].at[slot], sems[1].at[slot]
        rank, n = {'data': (me, n_data), 'model': (mod, n_model), 'chip': (x, n_chips)}[axis]
        mesh_axis = 'model' if axis == 'model' else 'data'
        if op == 'start':
            dst[rank] = src[...]
            for who in others(axis):
                remote(src, dst.at[rank], send, recv, mesh_axis, who).start()
            return
        rest = dst.at[pl.ds(0, n - 1)]
        done = remote(rest, rest, send, recv, mesh_axis, partner if mesh_axis == 'data' else mod)
        if op == 'recv':
            done.wait_recv()
        else:
            done.wait_send()

    def total(dst, n):
        acc = dst[0]
        for r in range(1, n):
            acc = acc + dst[r]
        return acc

    d_sems, m_sems, s_sems = (dsnd, drcv), (msnd, mrcv), (ssnd, srcv)

    def pair_ex(group):
        i = SLOT[group]
        return remote(lane_sum[group], near[group], psnd.at[i], prcv.at[i], 'data', partner)

    def lane_ex(group, op):
        pairs = group in near
        gather((both if pairs else lane_sum)[group], dat_got[group], d_sems, SLOT[group], 'chip' if pairs else 'data', op)

    def lane_start(group):
        if group in near:
            pair_ex(group).start()
        else:
            lane_ex(group, 'start')

    def lane_pair(group):
        pair_ex(group).wait_recv()
        both[group][...] = lane_sum[group][...] + near[group][...]
        lane_ex(group, 'start')

    def model_ex(group, op):
        gather(mod_blk[group], mod_got[group], m_sems, SLOT[group], 'model', op)

    def scal_ex(family, op):
        gather(scal.at[SLOT[family]], got_s.at[SLOT[family]], s_sems, SLOT[family], 'data', op)

    def weights_start():
        for cp in w_loads + small:
            cp.wait()
        turn[...] = jnp.zeros_like(turn)
        turn[0:WIDE, 0:N_QKV] = col_q[...]
        turn[...] = turn[...].T
        turn[N_QKV:N_QKV + N_O, 0:WIDE] = row_o[...]
        row = turn[pl.ds(0, N_B, stride=4), :]
        for q in range(1, 4):
            row = row + pltpu.roll(turn[pl.ds(q, N_B, stride=4), :], WIDE * q, 1)
        lane_b[...] = row
        wtab[...] = jnp.zeros_like(wtab)
        vtab[...] = jnp.zeros_like(vtab)

        def squares(ref, row, width):
            def body(b, carry):
                w = ref[b]
                wtab[pl.ds(row + b, 1), 0:width] = jnp.sum(w * w, axis=0, keepdims=True)
                return carry
            lax.fori_loop(0, ref.shape[0], body, 0, unroll=6)

        squares(w_in, ROW_IN, LANES)
        squares(w_out, ROW_OUT, LANES)
        squares(w_q, ROW_B, ROWS)
        squares(w_o, ROW_B + N_QKV, ROWS)
        vtab[ROW_OUT:ROW_OUT + N_OUT, :] = row_out[...]
        vtab[ROW_B + 54:ROW_B + 72, 0:WIDE] = row_o[...]
        mod_w[0:1, :] = jnp.sum(wtab[...].T, axis=0, keepdims=True)
        mod_w[1:2, :] = jnp.sum(vtab[...].T, axis=0, keepdims=True) / n_data
        gather(mod_w, got_w, m_sems, SLOT['w'], 'model', 'start')

    def weights_next():
        gather(mod_w, got_w, m_sems, SLOT['w'], 'model', 'recv')
        scal[SLOT['w']] = total(got_w, n_model)
        scal_ex('w', 'start')

    def weights_done():
        scal_ex('w', 'recv')
        w_all[...] = total(got_s.at[SLOT['w']], n_data)

    def after_lanes(group):
        family, g0, n = GROUPS[group]
        r0 = LANE_ROW[group]
        lane_ex(group, 'recv')
        lo = g0 - (FIRST_OUT if family == 'out' else g0)
        if family == 'b':
            mom = lane_b[...]
        else:
            mom = (col_in if family == 'in' else row_out)[lo:lo + n, :]
        new = BETA_TWO * mom + GAIN * (total(dat_got[group], dat_got[group].shape[0]) / 512.0)
        rlane[r0:r0 + n, :] = lax.rsqrt(new)
        if family == 'b':
            def body(s, carry):
                h = grad[FIRST_B + s] * rlane[pl.ds(r0 + s, 1), :]
                t = h.T.reshape(4, WIDE, ROWS)
                ht[pl.ds(4 * s, 4)] = t
                comp_b[pl.ds(s, 1), :, ROWS:LANES] = jnp.sum(t * t, axis=1)[None]
                return carry
            lax.fori_loop(0, n, body, 0, unroll=3)
            mod_b[...] = comp_b[...].reshape(4 * N_B, LANES)
        else:
            def body(b, acc):
                h = grad[g0 + b] * rlane[pl.ds(r0 + b, 1), :]
                grad[g0 + b] = h
                return jnp.where(lane_iota == lo + b, jnp.sum(h * h, axis=1, keepdims=True), acc)
            acc_z = lax.fori_loop(0, n, body, jnp.zeros((ROWS, LANES), F32), unroll=4)
            turned = jnp.concatenate([acc_t[0 if family == 'in' else 1], acc_z], axis=0).T
            mod_blk[group][...] = turned[lo:lo + n]
        model_ex(group, 'start')
        if family == 'b':
            turn[...] = jnp.zeros_like(turn)
            for q in range(4):
                turn[pl.ds(q, N_B, stride=4), :] = pltpu.roll(new, (LANES - WIDE * q) % LANES, 1)
            row_o_o[...] = turn[N_QKV:N_QKV + N_O, 0:WIDE]
            turn[...] = turn[...].T
            col_q_o[...] = turn[0:WIDE, 0:N_QKV]
        else:
            (col_in_o if family == 'in' else row_out_o)[lo:lo + n, :] = new

    def after_model(group):
        family, g0, n = GROUPS[group]
        lo = g0 - (FIRST_OUT if family == 'out' else g0)
        model_ex(group, 'recv')
        sums_z = total(mod_got[group], n_model)
        sums, z = sums_z[:, 0:ROWS], sums_z[:, ROWS:LANES]
        if family == 'b':
            mom = jnp.concatenate([row_q[...], col_o[...]], axis=0)
        else:
            mom = (row_in if family == 'in' else col_out)[lo:lo + n, :]
        new = BETA_TWO * mom + GAIN * (sums / full[family])
        mean_part = GAIN * (sums / 512.0)
        if family == 'in':
            term = new
        elif family == 'out':
            term = mean_part
        else:
            term = jnp.where(lax.broadcasted_iota(jnp.int32, new.shape, 0) < N_QKV, new, mean_part)
        r0 = TAB_ROW[group]
        r1 = r0 + new.shape[0]
        tab[r0:r1, 0:ROWS] = z / new
        tab[r0:r1, ROWS:LANES] = term
        rtab[r0:r1, 0:ROWS] = lax.rsqrt(new)
        if family == 'b':
            row_q_o[...] = new[:N_QKV]
            col_o_o[...] = new[N_QKV:]
        else:
            (row_in_o if family == 'in' else col_out_o)[lo:lo + n, :] = new

    def scalars_start(family):
        e = SLOT[family]
        turned = tab[...].T
        scal[e, 0:1, :] = jnp.sum(turned[:ROWS], axis=0, keepdims=True)
        scal[e, 1:2, :] = jnp.sum(turned[ROWS:], axis=0, keepdims=True)
        scal_ex(family, 'start')
        if family != 'b':
            rsub[...] = rtab[:, 0:ROWS].T

    def after_scalars(family):
        e = SLOT[family]
        scal_ex(family, 'recv')
        tot = total(got_s.at[e], n_data)
        q, s = tot[0:1], tot[1:2]
        w, v = w_all[0:1, :], w_all[1:2, :]
        rows = 512.0 if family == 'in' else float(full[family])
        size = 512.0 * full[family]
        m = (s if family == 'in' else BETA_TWO * v + s) / rows
        scale = jnp.sqrt(m) * (LR_BASE * jnp.maximum(1e-3, jnp.sqrt(w / size))) / jnp.maximum(1.0, jnp.sqrt(m * q / size))
        if family == 'b':
            turn[...] = jnp.broadcast_to(scale, (LANES, LANES)).T
            rtab[ROW_B:ROW_B + 72, 0:ROWS] = rtab[ROW_B:ROW_B + 72, 0:ROWS] * turn[ROW_B:ROW_B + 72, 0:ROWS]
            for ref, b0 in ((w_q, 0), (w_o, N_QKV)):
                def body(b, carry, ref=ref, b0=b0):
                    ref[b] = ref[b] - ht[b0 + b] * rtab[pl.ds(ROW_B + b0 + b, 1), 0:ROWS]
                    return carry
                lax.fori_loop(0, ref.shape[0], body, 0, unroll=6)
        else:
            ref, r0, g0 = (w_in, ROW_IN, FIRST_IN) if family == 'in' else (w_out, ROW_OUT, FIRST_OUT)
            fac = rsub[...] * scale

            def body(b, carry):
                f = jnp.sum(jnp.where(lane_iota == r0 + b, fac, 0.0), axis=1, keepdims=True)
                ref[b] = ref[b] - grad[g0 + b] * f
                return carry
            lax.fori_loop(0, ref.shape[0], body, 0, unroll=4)

    def sent_early():
        for i, ref in enumerate((peer, opp_in, left_in, right_in)):
            remote(ref, ref, snd.at[i], rcv.at[0, 0], 'data', partner).wait_send()
        gather(mod_w, got_w, m_sems, SLOT['w'], 'model', 'send')
        for group in near:
            pair_ex(group).wait_send()
        for group in GROUPS:
            lane_ex(group, 'send')
            if group != 'out_b':
                model_ex(group, 'send')
        for family in ('w', 'b', 'in'):
            scal_ex(family, 'send')

    def sent_late():
        model_ex('out_b', 'send')
        scal_ex('out', 'send')

    acc_t[...] = jnp.zeros_like(acc_t)
    tab[...] = jnp.zeros_like(tab)
    rtab[...] = jnp.zeros_like(rtab)

    convert(0)
    for cp in small + w_loads:
        cp.start()
    pl.semaphore_wait(barrier, n_data - 1 + n_model - 1)
    transfer(D2D, 0).start()
    last = N_CH - 1 + LAG_FINISH
    steps = {}

    def at(k, do, *args):
        steps.setdefault(k, []).append((do, args))

    at(4, weights_start)
    at(6, weights_next)
    at(8, weights_done)
    k_b, k_in, k_a = (LAST_CHUNK[g] + LAG_FINISH for g in ('b', 'in', 'out_a'))
    at(k_b + 1, lane_pair, 'b')
    at(k_b + 3, after_lanes, 'b')
    at(k_b + 5, after_model, 'b')
    at(k_b + 5, scalars_start, 'b')
    at(k_b + 7, after_scalars, 'b')
    at(k_in + 1, lane_pair, 'in')
    at(k_in + 3, after_lanes, 'in')
    tail = ((after_lanes, 'out_a'), (after_lanes, 'out_b'), (after_model, 'in'), (scalars_start, 'in'), (after_model, 'out_a'),
            (sent_early,), (after_model, 'out_b'), (scalars_start, 'out'), (after_scalars, 'in'), (after_scalars, 'out'), (sent_late,))
    for k in range(1 - AHEAD, last + 1):
        if 0 <= k < N_CH:
            opposite(k)
        if k + AHEAD < N_CH:
            convert(k + AHEAD)
            transfer(D2D, k + AHEAD).start()
        for ch in range(N_CH):
            if k == ch + (LAG_MERGE if ch < N_CH - 1 else 1):
                merge(ch)
        for do, args in steps.get(k, ()):
            do(*args)
        if 0 <= k - LAG_FINISH < N_CH:
            finish(k - LAG_FINISH)
        for group in GROUPS:
            if k == LAST_CHUNK[group] + LAG_FINISH:
                lane_start(group)
    for do, *args in tail:
        do(*args)


def deliver(*refs):
    srcs, dsts, sem = refs[:12], refs[12:24], refs[24]
    copies = [pltpu.make_async_copy(src, dst, sem.at[i]) for i, (src, dst) in enumerate(zip(srcs, dsts))]
    for cp in copies:
        cp.start()
    for cp in copies:
        cp.wait()


def solution(mesh):
    axis_sizes = dict(mesh.shape)
    n_data, n_model = axis_sizes['data'], axis_sizes['model']
    n_chips = n_data // 2
    rows_data = (P('data', None, None, 'model'), P(None, 'data', 'model'), P(None, 'data'), P(None, 'model'))
    rows_model = (P('data', None, 'model', None), P(None, 'model', 'data'), P(None, 'model'), P(None, 'data'))

    def vmem(*dims):
        return pltpu.VMEM(dims, F32)

    small = (vmem(24, ROWS), vmem(24, LANES), vmem(12, LANES), vmem(12, ROWS), vmem(54, ROWS), vmem(WIDE, 54), vmem(18, WIDE), vmem(18, ROWS))
    results = (vmem(24, ROWS, LANES), vmem(12, ROWS, LANES), vmem(54, WIDE, ROWS), vmem(18, WIDE, ROWS), *small)
    scratch = [
        *small, vmem(N_B, LANES), vmem(LANES, LANES),
        pltpu.VMEM((24, 512, LANES), jnp.bfloat16), pltpu.VMEM((12, LANES, 512), jnp.bfloat16),
        pltpu.VMEM((72, WIDE, 512), jnp.bfloat16),
        vmem(2, n_chips, N_SUP, ROWS, LANES), vmem(n_chips, N_SUP, ROWS, LANES),
        vmem(N_SUP, ROWS, LANES), vmem(N_SUP, ROWS, LANES), vmem(N_SUP, ROWS, LANES), vmem(N_SUP, ROWS, LANES),
        vmem(2, LANES), vmem(72, WIDE, ROWS),
        vmem(18, LANES), vmem(24, LANES), vmem(8, LANES), vmem(4, LANES),
        vmem(18, LANES), vmem(24, LANES), vmem(18, LANES), vmem(24, LANES),
        vmem(ROWS, LANES), vmem(2, ROWS, LANES), vmem(N_B, 4, LANES),
        vmem(LANES, LANES), vmem(LANES, LANES), vmem(ROWS, LANES), vmem(LANES, LANES), vmem(LANES, LANES),
        vmem(72, LANES), vmem(24, LANES), vmem(8, LANES), vmem(4, LANES), vmem(2, LANES), vmem(5, 2, LANES),
        vmem(n_chips, 18, LANES), vmem(n_chips, 24, LANES), vmem(n_data, 8, LANES), vmem(n_data, 4, LANES),
        vmem(n_model, 72, LANES), vmem(n_model, 24, LANES), vmem(n_model, 8, LANES), vmem(n_model, 4, LANES),
        vmem(n_model, 2, LANES), vmem(5, n_data, 2, LANES),
        pltpu.SemaphoreType.DMA((5,)), pltpu.SemaphoreType.DMA((4,)), pltpu.SemaphoreType.DMA((8,)),
        pltpu.SemaphoreType.DMA((4,)), pltpu.SemaphoreType.DMA((5, N_CH)),
        *(pltpu.SemaphoreType.DMA((n,)) for n in (2, 2, 4, 4, 5, 5, 5, 5)),
    ]
    hbm, in_vmem = pl.BlockSpec(memory_space=pltpu.HBM), pl.BlockSpec(memory_space=pltpu.VMEM)

    def step_all(grad_in, w_in, row_in, col_in, grad_out, w_out, row_out, col_out,
                 grad_qkv, w_qkv, row_qkv, col_qkv, grad_o, w_o, row_o, col_o):
        kept = pl.pallas_call(
            functools.partial(kernel, n_data, n_model),
            name='adafactor_step',
            out_shape=results,
            in_specs=[hbm] * 16,
            out_specs=[in_vmem] * 12,
            scratch_shapes=scratch,
            compiler_params=pltpu.CompilerParams(collective_id=0, has_side_effects=True, vmem_limit_bytes=VMEM_LIMIT),
        )(grad_in[0], grad_out[0], grad_qkv[0].transpose(0, 2, 1), grad_o[0],
          w_in, w_out.transpose(0, 2, 1), w_qkv.transpose(0, 2, 1), w_o,
          row_in, col_in, row_out, col_out, row_qkv, col_qkv.T, row_o, col_o)
        (w_in_new, w_out_new, w_qkv_new, w_o_new, row_in_new, col_in_new, row_out_new, col_out_new,
         row_qkv_new, col_qkv_new, row_o_new, col_o_new) = pl.pallas_call(
            deliver,
            name='deliver',
            out_shape=[jax.ShapeDtypeStruct(r.shape, F32) for r in results],
            in_specs=[in_vmem] * 12,
            out_specs=[hbm] * 12,
            scratch_shapes=[pltpu.SemaphoreType.DMA((12,))],
            compiler_params=pltpu.CompilerParams(vmem_limit_bytes=10 ** 6),
        )(*(pltpu.with_memory_space_constraint(a, pltpu.VMEM) for a in kept))
        return (w_in_new, row_in_new, col_in_new, w_out_new.transpose(0, 2, 1), row_out_new, col_out_new,
                w_qkv_new.transpose(0, 2, 1), row_qkv_new, col_qkv_new.T, w_o_new, row_o_new, col_o_new)

    in_specs = rows_data + rows_model + rows_data + rows_model
    out_specs = rows_data[1:] + rows_model[1:] + rows_data[1:] + rows_model[1:]
    return jax.shard_map(step_all, mesh=mesh, in_specs=in_specs, out_specs=out_specs, check_vma=False)
```

```python
import functools

import jax
import jax.numpy as jnp
from jax import lax
from jax.experimental import pallas as pl
from jax.experimental.pallas import tpu as pltpu
from jax.sharding import PartitionSpec as P

OPT_STEP = 4
EPS_SQ = 1e-30
BETA_TWO = 1.0 - OPT_STEP ** -0.8
GAIN = 1.0 - BETA_TWO
LR_BASE = min(1e-2, OPT_STEP ** -0.5)
F32 = jnp.float32
LANES, ROWS, WIDE = 128, 64, 32
VMEM_LIMIT = 60 * 10 ** 6

N_IN, N_B, N_OUT = 24, 18, 12
N_SUP = N_IN + N_B + N_OUT
FIRST_B, FIRST_IN, FIRST_OUT = 0, N_B, N_B + N_IN
N_QKV, N_O = 54, 18
N_OUT_B = 2
N_OUT_A = N_OUT - N_OUT_B
ROW_IN, ROW_OUT, ROW_B = 0, 24, 40
GROUPS = {'b': ('b', FIRST_B, N_B), 'in': ('in', FIRST_IN, N_IN), 'out_a': ('out', FIRST_OUT, N_OUT_A), 'out_b': ('out', FIRST_OUT + N_OUT_A, N_OUT_B)}
SIZES = (('b', (2, 4, 6, 6)), ('in', (6, 6, 6, 6)), ('out_a', (4, 4, 2)), ('out_b', (2,)))


def cut():
    chunks, at = [], 0
    for group, sizes in SIZES:
        for n in sizes:
            chunks.append((group, at, n))
            at += n
    return tuple(chunks)


CHUNKS = cut()
N_CH = len(CHUNKS)
LAST_CHUNK = {g: max(i for i, c in enumerate(CHUNKS) if c[0] == g) for g in GROUPS}
D2D, OPP_A, OPP_B, OWN_R, OWN_L, MRG_R, MRG_L = range(7)
SEND = (0, 1, 1, 2, 3, 2, 3)
OPP, LAST = 1, 2
RECV = (D2D, OPP, OPP, LAST, LAST, LAST, LAST)
SLOT = {'b': 0, 'in': 1, 'out_a': 2, 'out_b': 3, 'w': 4}
LANE_ROW = {'b': 0, 'in': 24, 'out_a': 48, 'out_b': 48 + N_OUT_A}
TAB_ROW = {'b': ROW_B, 'in': ROW_IN, 'out_a': ROW_OUT, 'out_b': ROW_OUT + N_OUT_A}
AHEAD, EARLY_OWN, LAG_MERGE, LAG_FINISH = 2, 3, 2, 3


def kernel(n_data, n_model, gin_h, gout_h, gq_h, go_h, win_h, wout_h, wq_h, wo_h,
           row_in_h, col_in_h, row_out_h, col_out_h, row_q_h, col_q_h, row_o_h, col_o_h,
           w_in, w_out, w_q, w_o, row_in_o, col_in_o, row_out_o, col_out_o, row_q_o, col_q_o, row_o_o, col_o_o,
           row_in, col_in, row_out, col_out, row_q, col_q, row_o, col_o, lane_b, turn,
           gin, gout, gb, part, peer, opp_in, left_in, right_in, grad, w_all, ht,
           sum_b, sum_in, sum_a, sum_o, near_b, near_in, both_b, both_in, full_b, full_in, rlane, acc_t, comp_b, tab, rtab, rsub, wtab, vtab,
           mod_b, mod_in, mod_a, mod_o, mod_w, scal, dat_b, dat_in, dat_a, dat_o, got_b, got_in, got_a, got_o, got_w, got_s,
           raw_a, raw_o, graw_a, graw_o, wcol, krow,
           load_sem, w_sem, small_sem, first_sem, snd, rcv, psnd, prcv, bsnd, brcv, dsnd, drcv, msnd, mrcv, ssnd, srcv):
    me = lax.axis_index('data')
    mod = lax.axis_index('model')
    n_chips = n_data // 2
    x, c = lax.div(me, 2), lax.rem(me, 2)
    xr, xl, xo = lax.rem(x + 1, n_chips), lax.rem(x + 3, n_chips), lax.rem(x + 2, n_chips)
    partner, right, left = 2 * x + 1 - c, 2 * xr + c, 2 * xl + c
    full = {'in': n_model * LANES, 'out': n_model * LANES, 'b': n_model * WIDE}
    lane_sum = {'b': sum_b, 'in': sum_in, 'out_a': sum_a, 'out_b': sum_o}
    near = {'b': near_b, 'in': near_in}
    both = {'b': both_b, 'in': both_in}
    whole = {'b': full_b, 'in': full_in}
    dat_got = {'b': dat_b, 'in': dat_in, 'out_a': dat_a, 'out_b': dat_o}
    mod_blk = {'b': mod_b, 'in': mod_in, 'out_a': mod_a, 'out_b': mod_o}
    raw = {'out_a': raw_a, 'out_b': raw_o}
    raw_got = {'out_a': graw_a, 'out_b': graw_o}
    mod_got = {'b': got_b, 'in': got_in, 'out_a': got_a, 'out_b': got_o}

    loads = [pltpu.make_async_copy(gq_h.at[pl.ds(0, 8)], gb.at[pl.ds(0, 8)], load_sem.at[0]),
             pltpu.make_async_copy(gq_h.at[pl.ds(8, 46)], gb.at[pl.ds(8, 46)], load_sem.at[1]),
             pltpu.make_async_copy(go_h, gb.at[pl.ds(54, 18)], load_sem.at[2]),
             pltpu.make_async_copy(gin_h, gin, load_sem.at[3]),
             pltpu.make_async_copy(gout_h, gout, load_sem.at[4])]
    w_loads = [pltpu.make_async_copy(win_h, w_in, w_sem.at[0]),
               pltpu.make_async_copy(wout_h, w_out, w_sem.at[1]),
               pltpu.make_async_copy(wq_h, w_q, w_sem.at[2]),
               pltpu.make_async_copy(wo_h, w_o, w_sem.at[3])]
    small = [pltpu.make_async_copy(src, dst, small_sem.at[i]) for i, (src, dst) in enumerate((
        (row_in_h, row_in), (col_in_h, col_in), (row_out_h, row_out), (col_out_h, col_out),
        (row_q_h, row_q), (col_q_h, col_q), (row_o_h, row_o), (col_o_h, col_o)))]
    for cp in loads:
        cp.start()

    barrier = pltpu.get_barrier_semaphore()

    def others(axis):
        side = 4 if axis == 'model' else 2
        n, rank = (n_model, mod) if axis == 'model' else (n_data, me)
        high, low, rows = lax.div(rank, side), lax.rem(rank, side), n // side

        def hops(d):
            up, over = d // side, d % side
            return min(up, rows - up) * (side - 1) + min(over, side - over)

        for d in sorted(range(1, n), key=lambda d: -hops(d)):
            if axis != 'chip' or d % side == 0:
                yield lax.rem(high + d // side, rows) * side + lax.rem(low + d % side, side)

    for axis in ('model', 'data'):
        for who in others(axis):
            pl.semaphore_signal(barrier, inc=1, device_id={axis: who}, device_id_type=pl.DeviceIdType.MESH)

    def remote(src, dst, ssem, rsem, axis, who):
        return pltpu.make_async_remote_copy(src_ref=src, dst_ref=dst, send_sem=ssem, recv_sem=rsem,
                                            device_id={axis: who}, device_id_type=pl.DeviceIdType.MESH)

    def transfer(kind, ch):
        _, b0, n = CHUNKS[ch]
        n_a = n // 2
        every, half_a, half_b = pl.ds(b0, n), pl.ds(b0, n_a), pl.ds(b0 + n_a, n - n_a)
        src, dst, who = {
            D2D: lambda: (part.at[1 - c, :, every], peer.at[:, every], partner),
            OPP_A: lambda: (part.at[c, xo, half_a], opp_in.at[half_a], right),
            OPP_B: lambda: (part.at[c, xo, half_b], opp_in.at[half_b], left),
            OWN_R: lambda: (part.at[c, xr, half_b], left_in.at[half_b], right),
            OWN_L: lambda: (part.at[c, xl, half_a], right_in.at[half_a], left),
            MRG_R: lambda: (part.at[c, xr, half_a], left_in.at[half_a], right),
            MRG_L: lambda: (part.at[c, xl, half_b], right_in.at[half_b], left),
        }[kind]()
        return remote(src, dst, snd.at[SEND[kind]], rcv.at[RECV[kind], ch], 'data', who)

    def convert(ch):
        group, b0, n = CHUNKS[ch]
        family = GROUPS[group][0]
        if ch == 0:
            loads[0].wait()
        elif ch == 1:
            loads[1].wait()
            loads[2].wait()
        elif b0 == FIRST_IN:
            loads[3].wait()
        elif b0 == FIRST_OUT:
            loads[4].wait()

        def body(i, carry):
            b = b0 + i
            for t in range(n_chips):
                if family == 'in':
                    tile = gin[b - FIRST_IN, pl.ds(LANES * t, LANES), :].astype(F32)
                elif family == 'out':
                    tile = gout[b - FIRST_OUT, :, pl.ds(LANES * t, LANES)].astype(F32).T
                else:
                    four = gb[pl.ds(4 * (b - FIRST_B), 4), :, pl.ds(LANES * t, LANES)].astype(F32)
                    tile = four.reshape(LANES, LANES).T
                part[0, t, b] = tile[:ROWS]
                part[1, t, b] = tile[ROWS:]
            return carry

        lax.fori_loop(0, n, body, 0)

    def first_pair(dest, sem):
        every = pl.ds(0, CHUNKS[0][2])
        return remote(part.at[1 - c, dest, every], peer.at[dest, every], snd.at[0], sem, 'data', partner)

    def first_pairs():
        first_pair(xo, first_sem.at[0]).start()
        for dest in (xr, xl, x):
            first_pair(dest, rcv.at[D2D, 0]).start()

    def add_peer(ch, dest):
        _, b0, n = CHUNKS[ch]

        def body(i, carry):
            b = b0 + i
            part[c, dest, b] = part[c, dest, b] + peer[dest, b]
            return carry
        lax.fori_loop(0, n, body, 0, unroll=2)

    def opposite(ch):
        if ch == 0:
            first_pair(xo, first_sem.at[0]).wait_recv()
        else:
            transfer(D2D, ch).wait_recv()
        add_peer(ch, xo)
        transfer(OPP_A, ch).start()
        transfer(OPP_B, ch).start()
        if ch == 0:
            rest = peer.at[pl.ds(0, n_chips - 1), pl.ds(0, CHUNKS[0][2])]
            remote(rest, rest, snd.at[0], rcv.at[D2D, 0], 'data', partner).wait_recv()
        add_peer(ch, xr)
        add_peer(ch, xl)
        if ch < EARLY_OWN:
            own(ch)
        add_peer(ch, x)

    def own(ch):
        transfer(OWN_R, ch).start()
        transfer(OWN_L, ch).start()

    def merge(ch):
        _, b0, n = CHUNKS[ch]
        n_a = n // 2

        def add(dest, lo, hi):
            def body(b, carry):
                part[c, dest, b] = part[c, dest, b] + opp_in[b]
                return carry
            lax.fori_loop(lo, hi, body, 0)

        every = opp_in.at[pl.ds(b0, n)]
        remote(every, every, snd.at[1], rcv.at[OPP, ch], 'data', left).wait_recv()
        add(xr, b0, b0 + n_a)
        transfer(MRG_R, ch).start()
        add(xl, b0 + n_a, b0 + n)
        transfer(MRG_L, ch).start()
        if ch >= EARLY_OWN:
            own(ch)

    lane_iota = lax.broadcasted_iota(jnp.int32, (ROWS, LANES), 1)

    def finish(ch):
        group, b0, n = CHUNKS[ch]
        family, g0, _ = GROUPS[group]
        every = pl.ds(b0, n)
        two = peer.at[pl.ds(0, 2), every]
        remote(two, two, snd.at[2], rcv.at[LAST, ch], 'data', right).wait_recv()

        def block(b):
            g = (part[c, x, b] + left_in[b] + right_in[b]) * (1.0 / n_data)
            grad[b] = g
            sq = g * g + EPS_SQ
            sums = jnp.sum(sq, axis=0, keepdims=True)
            if group in near:
                half = lane_sum[group].shape[1]
                lane_sum[group][lax.div(b - g0, half), pl.ds(lax.rem(b - g0, half), 1), :] = sums
            else:
                lane_sum[group][pl.ds(b - g0, 1), :] = sums
            return g, sq

        if family == 'b':
            def body(i, carry):
                b = b0 + i
                g, _ = block(b)
                gt = g.T
                st = (gt * gt + EPS_SQ).reshape(4, WIDE, ROWS)
                comp_b[pl.ds(b - FIRST_B, 1), :, 0:ROWS] = jnp.sum(st, axis=1)[None]
                return carry
            lax.fori_loop(0, n, body, 0, unroll=2)
        else:
            which = 0 if family == 'in' else 1

            def body(i, acc):
                b = b0 + i
                _, sq = block(b)
                return jnp.where(lane_iota == b - (FIRST_IN if family == 'in' else FIRST_OUT), jnp.sum(sq, axis=1, keepdims=True), acc)
            acc_t[which] = lax.fori_loop(0, n, body, acc_t[which], unroll=2)

    def gather(src, dst, sems, slot, axis, op):
        send, recv = sems[0].at[slot], sems[1].at[slot]
        rank, n = {'data': (me, n_data), 'model': (mod, n_model), 'chip': (x, n_chips)}[axis]
        mesh_axis = 'model' if axis == 'model' else 'data'
        if op == 'start':
            dst[rank] = src[...]
            for who in others(axis):
                remote(src, dst.at[rank], send, recv, mesh_axis, who).start()
            return
        rest = dst.at[pl.ds(0, n - 1)]
        done = remote(rest, rest, send, recv, mesh_axis, partner if mesh_axis == 'data' else mod)
        if op == 'recv':
            done.wait_recv()
        else:
            done.wait_send()

    def total(dst, n):
        acc = dst[0]
        for r in range(1, n):
            acc = acc + dst[r]
        return acc

    d_sems, m_sems, s_sems = (dsnd, drcv), (msnd, mrcv), (ssnd, srcv)

    def pair_ex(group):
        i = SLOT[group]
        return remote(lane_sum[group], near[group], psnd.at[i], prcv.at[i], 'data', partner)

    def lane_ex(group, op):
        pairs = group in near
        gather(both[group].at[c] if pairs else lane_sum[group], dat_got[group], d_sems, SLOT[group], 'chip' if pairs else 'data', op)

    def back_ex(group):
        i = SLOT[group]
        return remote(whole[group].at[c], whole[group].at[c], bsnd.at[i], brcv.at[i], 'data', partner)

    def lane_back(group):
        lane_ex(group, 'recv')
        whole[group][c] = total(dat_got[group], n_chips)
        back_ex(group).start()

    def lane_start(group):
        if group in near:
            pair_ex(group).start()
        else:
            lane_ex(group, 'start')

    def lane_pair(group):
        pair_ex(group).wait_recv()
        both[group][...] = lane_sum[group][...] + near[group][...]
        lane_ex(group, 'start')

    def model_ex(group, op):
        gather(mod_blk[group], mod_got[group], m_sems, SLOT[group], 'model', op)

    def scal_ex(name, op):
        i = SLOT[name]
        src, dst = (raw[name], raw_got[name]) if name in raw else (scal.at[i], got_s.at[i])
        gather(src, dst, s_sems, i, 'data', op)

    def weights_start():
        for cp in w_loads + small:
            cp.wait()
        turn[...] = jnp.zeros_like(turn)
        turn[0:WIDE, 0:N_QKV] = col_q[...]
        turn[...] = turn[...].T
        turn[N_QKV:N_QKV + N_O, 0:WIDE] = row_o[...]
        row = turn[pl.ds(0, N_B, stride=4), :]
        for q in range(1, 4):
            row = row + pltpu.roll(turn[pl.ds(q, N_B, stride=4), :], WIDE * q, 1)
        lane_b[...] = row
        wtab[...] = jnp.zeros_like(wtab)
        vtab[...] = jnp.zeros_like(vtab)

        def squares(ref, row, width):
            def body(b, carry):
                w = ref[b]
                wtab[pl.ds(row + b, 1), 0:width] = jnp.sum(w * w, axis=0, keepdims=True)
                return carry
            lax.fori_loop(0, ref.shape[0], body, 0, unroll=6)

        squares(w_in, ROW_IN, LANES)
        squares(w_out, ROW_OUT, LANES)
        squares(w_q, ROW_B, ROWS)
        squares(w_o, ROW_B + N_QKV, ROWS)
        vtab[ROW_OUT:ROW_OUT + N_OUT, :] = row_out[...]
        vtab[ROW_B + 54:ROW_B + 72, 0:WIDE] = row_o[...]
        mod_w[0:1, :] = jnp.sum(wtab[...].T, axis=0, keepdims=True)
        mod_w[1:2, :] = jnp.sum(vtab[...].T, axis=0, keepdims=True) / n_data
        gather(mod_w, got_w, m_sems, SLOT['w'], 'model', 'start')

    def weights_next():
        gather(mod_w, got_w, m_sems, SLOT['w'], 'model', 'recv')
        scal[SLOT['w']] = total(got_w, n_model)
        scal_ex('w', 'start')

    def weights_done():
        scal_ex('w', 'recv')
        w_all[...] = total(got_s.at[SLOT['w']], n_data)
        turn[0:2, :] = w_all[...]
        wcol[...] = turn[...].T

    def after_lanes(group):
        family, g0, n = GROUPS[group]
        r0 = LANE_ROW[group]
        if group in near:
            back_ex(group).wait_recv()
            sums = jnp.concatenate([whole[group][0], whole[group][1]], axis=0)
        else:
            lane_ex(group, 'recv')
            sums = total(dat_got[group], n_data)
        lo = g0 - (FIRST_OUT if family == 'out' else g0)
        if family == 'b':
            mom = lane_b[...]
        else:
            mom = (col_in if family == 'in' else row_out)[lo:lo + n, :]
        new = BETA_TWO * mom + GAIN * (sums / 512.0)
        rlane[r0:r0 + n, :] = lax.rsqrt(new)
        if family == 'b':
            def body(s, carry):
                h = grad[FIRST_B + s] * rlane[pl.ds(r0 + s, 1), :]
                t = h.T.reshape(4, WIDE, ROWS)
                ht[pl.ds(4 * s, 4)] = t
                comp_b[pl.ds(s, 1), :, ROWS:LANES] = jnp.sum(t * t, axis=1)[None]
                return carry
            lax.fori_loop(0, n, body, 0, unroll=3)
            mod_b[...] = comp_b[...].reshape(4 * N_B, LANES)
        else:
            def body(b, acc):
                h = grad[g0 + b] * rlane[pl.ds(r0 + b, 1), :]
                grad[g0 + b] = h
                return jnp.where(lane_iota == lo + b, jnp.sum(h * h, axis=1, keepdims=True), acc)
            acc_z = lax.fori_loop(0, n, body, jnp.zeros((ROWS, LANES), F32), unroll=4)
            turned = jnp.concatenate([acc_t[0 if family == 'in' else 1], acc_z], axis=0).T
            mod_blk[group][...] = turned[lo:lo + n]
        model_ex(group, 'start')
        if family == 'b':
            turn[...] = jnp.zeros_like(turn)
            for q in range(4):
                turn[pl.ds(q, N_B, stride=4), :] = pltpu.roll(new, (LANES - WIDE * q) % LANES, 1)
            row_o_o[...] = turn[N_QKV:N_QKV + N_O, 0:WIDE]
            turn[...] = turn[...].T
            col_q_o[...] = turn[0:WIDE, 0:N_QKV]
        else:
            (col_in_o if family == 'in' else row_out_o)[lo:lo + n, :] = new

    def after_model(group):
        family, g0, n = GROUPS[group]
        lo = g0 - (FIRST_OUT if family == 'out' else g0)
        model_ex(group, 'recv')
        sums_z = total(mod_got[group], n_model)
        sums, z = sums_z[:, 0:ROWS], sums_z[:, ROWS:LANES]
        if family == 'b':
            mom = jnp.concatenate([row_q[...], col_o[...]], axis=0)
        else:
            mom = (row_in if family == 'in' else col_out)[lo:lo + n, :]
        new = BETA_TWO * mom + GAIN * (sums / full[family])
        mean_part = GAIN * (sums / 512.0)
        if family == 'in':
            term = new
        elif family == 'out':
            term = mean_part
        else:
            term = jnp.where(lax.broadcasted_iota(jnp.int32, new.shape, 0) < N_QKV, new, mean_part)
        r0 = TAB_ROW[group]
        r1 = r0 + new.shape[0]
        if family == 'out':
            raw[group][:, 0:ROWS] = z / new
            raw[group][:, ROWS:LANES] = term
            scal_ex(group, 'start')
        else:
            tab[r0:r1, 0:ROWS] = z / new
            tab[r0:r1, ROWS:LANES] = term
        rtab[r0:r1, 0:ROWS] = lax.rsqrt(new)
        if family == 'b':
            row_q_o[...] = new[:N_QKV]
            col_o_o[...] = new[N_QKV:]
        else:
            (row_in_o if family == 'in' else col_out_o)[lo:lo + n, :] = new

    def scalars_start(family):
        e = SLOT[family]
        turned = tab[...].T
        scal[e, 0:1, :] = jnp.sum(turned[:ROWS], axis=0, keepdims=True)
        scal[e, 1:2, :] = jnp.sum(turned[ROWS:], axis=0, keepdims=True)
        scal_ex(family, 'start')
        if family != 'b':
            rsub[...] = rtab[:, 0:ROWS].T

    def factor(q, s, w, v, family):
        rows = 512.0 if family == 'in' else float(full[family])
        size = 512.0 * full[family]
        m = (s if family == 'in' else BETA_TWO * v + s) / rows
        return jnp.sqrt(m) * (LR_BASE * jnp.maximum(1e-3, jnp.sqrt(w / size))) / jnp.maximum(1.0, jnp.sqrt(m * q / size))

    def after_scalars(family):
        e = SLOT[family]
        scal_ex(family, 'recv')
        tot = total(got_s.at[e], n_data)
        scale = factor(tot[0:1], tot[1:2], w_all[0:1, :], w_all[1:2, :], family)
        if family == 'b':
            turn[...] = jnp.broadcast_to(scale, (LANES, LANES)).T
            rtab[ROW_B:ROW_B + 72, 0:ROWS] = rtab[ROW_B:ROW_B + 72, 0:ROWS] * turn[ROW_B:ROW_B + 72, 0:ROWS]
            for ref, b0 in ((w_q, 0), (w_o, N_QKV)):
                def body(b, carry, ref=ref, b0=b0):
                    ref[b] = ref[b] - ht[b0 + b] * rtab[pl.ds(ROW_B + b0 + b, 1), 0:ROWS]
                    return carry
                lax.fori_loop(0, ref.shape[0], body, 0, unroll=6)
        else:
            fac = rsub[...] * scale

            def body(b, carry):
                f = jnp.sum(jnp.where(lane_iota == ROW_IN + b, fac, 0.0), axis=1, keepdims=True)
                w_in[b] = w_in[b] - grad[FIRST_IN + b] * f
                return carry
            lax.fori_loop(0, N_IN, body, 0, unroll=4)

    def prepare_out():
        fac = rtab[:, 0:ROWS].T

        def body(b, carry):
            f = jnp.sum(jnp.where(lane_iota == ROW_OUT + b, fac, 0.0), axis=1, keepdims=True)
            grad[FIRST_OUT + b] = grad[FIRST_OUT + b] * f
            return carry
        lax.fori_loop(0, N_OUT, body, 0, unroll=4)

    def apply_out(group):
        _, g0, n = GROUPS[group]
        lo, r0 = g0 - FIRST_OUT, TAB_ROW[group]
        scal_ex(group, 'recv')
        tot = total(raw_got[group], n_data)
        q = jnp.sum(tot[:, 0:ROWS], axis=1, keepdims=True)
        s = jnp.sum(tot[:, ROWS:LANES], axis=1, keepdims=True)
        scale = factor(q, s, wcol[r0:r0 + n, 0:1], wcol[r0:r0 + n, 1:2], 'out')
        krow[lo:lo + n, :] = jnp.broadcast_to(scale, (n, LANES))
        for b in range(lo, lo + n):
            w_out[b] = w_out[b] - grad[FIRST_OUT + b] * krow[b:b + 1, :]

    def sent_early():
        for i, ref in enumerate((peer, opp_in, left_in, right_in)):
            remote(ref, ref, snd.at[i], rcv.at[0, 0], 'data', partner).wait_send()
        gather(mod_w, got_w, m_sems, SLOT['w'], 'model', 'send')
        for group in near:
            pair_ex(group).wait_send()
            back_ex(group).wait_send()
        for group in GROUPS:
            lane_ex(group, 'send')
        model_ex('b', 'send')
        scal_ex('w', 'send')
        scal_ex('b', 'send')

    def sent_mid():
        for group in ('in', 'out_a', 'out_b'):
            model_ex(group, 'send')
        scal_ex('in', 'send')
        scal_ex('out_a', 'send')

    def sent_late():
        scal_ex('out_b', 'send')

    acc_t[...] = jnp.zeros_like(acc_t)
    tab[...] = jnp.zeros_like(tab)
    rtab[...] = jnp.zeros_like(rtab)

    convert(0)
    for cp in small + w_loads:
        cp.start()
    pl.semaphore_wait(barrier, n_data - 1 + n_model - 1)
    first_pairs()
    last = N_CH - 1 + LAG_FINISH
    steps = {}

    def at(k, do, *args):
        steps.setdefault(k, []).append((do, args))

    at(4, weights_start)
    at(6, weights_next)
    at(8, weights_done)
    k_b, k_in, k_a = (LAST_CHUNK[g] + LAG_FINISH for g in ('b', 'in', 'out_a'))
    at(k_b + 1, lane_pair, 'b')
    at(k_b + 3, lane_back, 'b')
    at(k_b + 4, after_lanes, 'b')
    at(k_b + 6, after_model, 'b')
    at(k_b + 6, scalars_start, 'b')
    at(k_in + 1, lane_pair, 'in')
    at(k_in + 3, lane_back, 'in')
    tail = ((after_lanes, 'in'), (after_lanes, 'out_a'), (after_lanes, 'out_b'), (after_scalars, 'b'), (sent_early,), (after_model, 'in'),
            (scalars_start, 'in'), (after_model, 'out_a'), (after_model, 'out_b'), (prepare_out,), (sent_mid,), (after_scalars, 'in'),
            (apply_out, 'out_a'), (apply_out, 'out_b'), (sent_late,))
    for k in range(1 - AHEAD, last + 1):
        if 0 <= k < N_CH:
            opposite(k)
        if k + AHEAD < N_CH:
            convert(k + AHEAD)
            transfer(D2D, k + AHEAD).start()
        for ch in range(N_CH):
            if k == ch + (LAG_MERGE if ch < N_CH - 1 else 1):
                merge(ch)
        for do, args in steps.get(k, ()):
            do(*args)
        if 0 <= k - LAG_FINISH < N_CH:
            finish(k - LAG_FINISH)
        for group in GROUPS:
            if k == LAST_CHUNK[group] + LAG_FINISH:
                lane_start(group)
    for do, *args in tail:
        do(*args)


def deliver(*refs):
    srcs, dsts, sem = refs[:12], refs[12:24], refs[24]
    copies = [pltpu.make_async_copy(src, dst, sem.at[i]) for i, (src, dst) in enumerate(zip(srcs, dsts))]
    for cp in copies:
        cp.start()
    for cp in copies:
        cp.wait()


def solution(mesh):
    axis_sizes = dict(mesh.shape)
    n_data, n_model = axis_sizes['data'], axis_sizes['model']
    n_chips = n_data // 2
    rows_data = (P('data', None, None, 'model'), P(None, 'data', 'model'), P(None, 'data'), P(None, 'model'))
    rows_model = (P('data', None, 'model', None), P(None, 'model', 'data'), P(None, 'model'), P(None, 'data'))

    def vmem(*dims):
        return pltpu.VMEM(dims, F32)

    small = (vmem(24, ROWS), vmem(24, LANES), vmem(12, LANES), vmem(12, ROWS), vmem(54, ROWS), vmem(WIDE, 54), vmem(18, WIDE), vmem(18, ROWS))
    results = (vmem(24, ROWS, LANES), vmem(12, ROWS, LANES), vmem(54, WIDE, ROWS), vmem(18, WIDE, ROWS), *small)
    scratch = [
        *small, vmem(N_B, LANES), vmem(LANES, LANES),
        pltpu.VMEM((24, 512, LANES), jnp.bfloat16), pltpu.VMEM((12, LANES, 512), jnp.bfloat16),
        pltpu.VMEM((72, WIDE, 512), jnp.bfloat16),
        vmem(2, n_chips, N_SUP, ROWS, LANES), vmem(n_chips, N_SUP, ROWS, LANES),
        vmem(N_SUP, ROWS, LANES), vmem(N_SUP, ROWS, LANES), vmem(N_SUP, ROWS, LANES), vmem(N_SUP, ROWS, LANES),
        vmem(2, LANES), vmem(72, WIDE, ROWS),
        vmem(2, 9, LANES), vmem(2, 12, LANES), vmem(N_OUT_A, LANES), vmem(N_OUT_B, LANES),
        *(vmem(2, n, LANES) for n in (9, 12, 9, 12, 9, 12)),
        vmem(ROWS, LANES), vmem(2, ROWS, LANES), vmem(N_B, 4, LANES),
        vmem(LANES, LANES), vmem(LANES, LANES), vmem(ROWS, LANES), vmem(LANES, LANES), vmem(LANES, LANES),
        vmem(72, LANES), vmem(24, LANES), vmem(N_OUT_A, LANES), vmem(N_OUT_B, LANES), vmem(2, LANES), vmem(5, 2, LANES),
        vmem(n_chips, 9, LANES), vmem(n_chips, 12, LANES), vmem(n_data, N_OUT_A, LANES), vmem(n_data, N_OUT_B, LANES),
        vmem(n_model, 72, LANES), vmem(n_model, 24, LANES), vmem(n_model, N_OUT_A, LANES), vmem(n_model, N_OUT_B, LANES),
        vmem(n_model, 2, LANES), vmem(5, n_data, 2, LANES),
        vmem(N_OUT_A, LANES), vmem(N_OUT_B, LANES), vmem(n_data, N_OUT_A, LANES), vmem(n_data, N_OUT_B, LANES), vmem(LANES, LANES), vmem(12, LANES),
        pltpu.SemaphoreType.DMA((5,)), pltpu.SemaphoreType.DMA((4,)), pltpu.SemaphoreType.DMA((8,)), pltpu.SemaphoreType.DMA((1,)),
        pltpu.SemaphoreType.DMA((4,)), pltpu.SemaphoreType.DMA((3, N_CH)),
        *(pltpu.SemaphoreType.DMA((n,)) for n in (2, 2, 2, 2, 4, 4, 5, 5, 5, 5)),
    ]
    hbm, in_vmem = pl.BlockSpec(memory_space=pltpu.HBM), pl.BlockSpec(memory_space=pltpu.VMEM)

    def step_all(grad_in, w_in, row_in, col_in, grad_out, w_out, row_out, col_out,
                 grad_qkv, w_qkv, row_qkv, col_qkv, grad_o, w_o, row_o, col_o):
        kept = pl.pallas_call(
            functools.partial(kernel, n_data, n_model),
            name='adafactor_step',
            out_shape=results,
            in_specs=[hbm] * 16,
            out_specs=[in_vmem] * 12,
            scratch_shapes=scratch,
            compiler_params=pltpu.CompilerParams(collective_id=0, has_side_effects=True, vmem_limit_bytes=VMEM_LIMIT),
        )(grad_in[0], grad_out[0], grad_qkv[0].transpose(0, 2, 1), grad_o[0],
          w_in, w_out.transpose(0, 2, 1), w_qkv.transpose(0, 2, 1), w_o,
          row_in, col_in, row_out, col_out, row_qkv, col_qkv.T, row_o, col_o)
        (w_in_new, w_out_new, w_qkv_new, w_o_new, row_in_new, col_in_new, row_out_new, col_out_new,
         row_qkv_new, col_qkv_new, row_o_new, col_o_new) = pl.pallas_call(
            deliver,
            name='deliver',
            out_shape=[jax.ShapeDtypeStruct(r.shape, F32) for r in results],
            in_specs=[in_vmem] * 12,
            out_specs=[hbm] * 12,
            scratch_shapes=[pltpu.SemaphoreType.DMA((12,))],
            compiler_params=pltpu.CompilerParams(vmem_limit_bytes=10 ** 6),
        )(*(pltpu.with_memory_space_constraint(a, pltpu.VMEM) for a in kept))
        return (w_in_new, row_in_new, col_in_new, w_out_new.transpose(0, 2, 1), row_out_new, col_out_new,
                w_qkv_new.transpose(0, 2, 1), row_qkv_new, col_qkv_new.T, w_o_new, row_o_new, col_o_new)

    in_specs = rows_data + rows_model + rows_data + rows_model
    out_specs = rows_data[1:] + rows_model[1:] + rows_data[1:] + rows_model[1:]
    return jax.shard_map(step_all, mesh=mesh, in_specs=in_specs, out_specs=out_specs, check_vma=False)
```

```python
import functools

import jax
import jax.numpy as jnp
from jax import lax
from jax.experimental import pallas as pl
from jax.experimental.pallas import tpu as pltpu
from jax.sharding import PartitionSpec as P

OPT_STEP = 4
EPS_SQ = 1e-30
BETA_TWO = 1.0 - OPT_STEP ** -0.8
GAIN = 1.0 - BETA_TWO
LR_BASE = min(1e-2, OPT_STEP ** -0.5)
F32 = jnp.float32
LANES, ROWS, WIDE = 128, 64, 32
VMEM_LIMIT = 60 * 10 ** 6

N_IN, N_B, N_OUT = 24, 18, 12
N_SUP = N_IN + N_B + N_OUT
FIRST_B, FIRST_IN, FIRST_OUT = 0, N_B, N_B + N_IN
N_QKV, N_O = 54, 18
N_OUT_B = 2
N_OUT_A = N_OUT - N_OUT_B
ROW_IN, ROW_OUT, ROW_B = 0, 24, 40
GROUPS = {'b': ('b', FIRST_B, N_B), 'in': ('in', FIRST_IN, N_IN), 'out_a': ('out', FIRST_OUT, N_OUT_A), 'out_b': ('out', FIRST_OUT + N_OUT_A, N_OUT_B)}
SIZES = (('b', (2, 4, 6, 6)), ('in', (6, 6, 6, 6)), ('out_a', (4, 4, 2)), ('out_b', (2,)))


def cut():
    chunks, at = [], 0
    for group, sizes in SIZES:
        for n in sizes:
            chunks.append((group, at, n))
            at += n
    return tuple(chunks)


CHUNKS = cut()
N_CH = len(CHUNKS)
LAST_CHUNK = {g: max(i for i, c in enumerate(CHUNKS) if c[0] == g) for g in GROUPS}
D2D, OPP_A, OPP_B, OWN_R, OWN_L, MRG_R, MRG_L = range(7)
SEND = (0, 1, 1, 2, 3, 2, 3)
OPP, LAST = 1, 2
RECV = (D2D, OPP, OPP, LAST, LAST, LAST, LAST)
SLOT = {'b': 0, 'in': 1, 'out_a': 2, 'out_b': 3, 'w': 4}
LANE_ROW = {'b': 0, 'in': 24, 'out_a': 48, 'out_b': 48 + N_OUT_A}
TAB_ROW = {'b': ROW_B, 'in': ROW_IN, 'out_a': ROW_OUT, 'out_b': ROW_OUT + N_OUT_A}
AHEAD, EARLY_OWN, LAG_MERGE, LAG_FINISH = 2, 3, 2, 3


def kernel(n_data, n_model, gin_h, gout_h, gq_h, go_h, win_h, wout_h, wq_h, wo_h,
           row_in_h, col_in_h, row_out_h, col_out_h, row_q_h, col_q_h, row_o_h, col_o_h,
           w_in, w_out, w_q, w_o, row_in_o, col_in_o, row_out_o, col_out_o, row_q_o, col_q_o, row_o_o, col_o_o,
           row_in, col_in, row_out, col_out, row_q, col_q, row_o, col_o, lane_b, turn,
           gin, gout, gb, part, peer, opp_in, left_in, right_in, grad, w_all, ht,
           sum_b, sum_in, sum_a, sum_o, near_b, near_in, both_b, both_in, full_b, full_in, rlane, acc_t, comp_b, tab, rtab, rsub, wtab, vtab,
           mod_b, mod_in, mod_a, mod_o, mod_w, scal, dat_b, dat_in, dat_a, dat_o, got_b, got_in, got_a, got_o, got_w, got_s,
           raw_a, raw_o, graw_a, graw_o, wcol, krow,
           load_sem, w_sem, small_sem, first_sem, meet, snd, rcv, psnd, prcv, bsnd, brcv, dsnd, drcv, msnd, mrcv, ssnd, srcv):
    me = lax.axis_index('data')
    mod = lax.axis_index('model')
    n_chips = n_data // 2
    x, c = lax.div(me, 2), lax.rem(me, 2)
    xr, xl, xo = lax.rem(x + 1, n_chips), lax.rem(x + 3, n_chips), lax.rem(x + 2, n_chips)
    partner, right, left = 2 * x + 1 - c, 2 * xr + c, 2 * xl + c
    full = {'in': n_model * LANES, 'out': n_model * LANES, 'b': n_model * WIDE}
    lane_sum = {'b': sum_b, 'in': sum_in, 'out_a': sum_a, 'out_b': sum_o}
    near = {'b': near_b, 'in': near_in}
    both = {'b': both_b, 'in': both_in}
    whole = {'b': full_b, 'in': full_in}
    dat_got = {'b': dat_b, 'in': dat_in, 'out_a': dat_a, 'out_b': dat_o}
    mod_blk = {'b': mod_b, 'in': mod_in, 'out_a': mod_a, 'out_b': mod_o}
    raw = {'out_a': raw_a, 'out_b': raw_o}
    raw_got = {'out_a': graw_a, 'out_b': graw_o}
    mod_got = {'b': got_b, 'in': got_in, 'out_a': got_a, 'out_b': got_o}

    loads = [pltpu.make_async_copy(gq_h.at[pl.ds(0, 8)], gb.at[pl.ds(0, 8)], load_sem.at[0]),
             pltpu.make_async_copy(gq_h.at[pl.ds(8, 46)], gb.at[pl.ds(8, 46)], load_sem.at[1]),
             pltpu.make_async_copy(go_h, gb.at[pl.ds(54, 18)], load_sem.at[2]),
             pltpu.make_async_copy(gin_h, gin, load_sem.at[3]),
             pltpu.make_async_copy(gout_h, gout, load_sem.at[4])]
    w_loads = [pltpu.make_async_copy(win_h, w_in, w_sem.at[0]),
               pltpu.make_async_copy(wout_h, w_out, w_sem.at[1]),
               pltpu.make_async_copy(wq_h, w_q, w_sem.at[2]),
               pltpu.make_async_copy(wo_h, w_o, w_sem.at[3])]
    small = [pltpu.make_async_copy(src, dst, small_sem.at[i]) for i, (src, dst) in enumerate((
        (row_in_h, row_in), (col_in_h, col_in), (row_out_h, row_out), (col_out_h, col_out),
        (row_q_h, row_q), (col_q_h, col_q), (row_o_h, row_o), (col_o_h, col_o)))]
    for cp in loads:
        cp.start()

    barrier = pltpu.get_barrier_semaphore()

    def others(axis):
        side = 4 if axis == 'model' else 2
        n, rank = (n_model, mod) if axis == 'model' else (n_data, me)
        high, low, rows = lax.div(rank, side), lax.rem(rank, side), n // side

        def hops(d):
            up, over = d // side, d % side
            return min(up, rows - up) * (side - 1) + min(over, side - over)

        for d in sorted(range(1, n), key=lambda d: -hops(d)):
            if axis != 'chip' or d % side == 0:
                yield lax.rem(high + d // side, rows) * side + lax.rem(low + d % side, side)

    side = 4
    z, y = lax.div(mod, side), lax.rem(mod, side)
    neighbours = [('data', who) for who in (partner, right, left)]
    for step in (1, side - 1):
        neighbours.append(('model', side * z + lax.rem(y + step, side)))
        neighbours.append(('model', side * lax.rem(z + step, n_model // side) + y))

    def greet(sem):
        for axis, who in neighbours:
            pl.semaphore_signal(sem, inc=1, device_id={axis: who}, device_id_type=pl.DeviceIdType.MESH)

    greet(barrier)

    def remote(src, dst, ssem, rsem, axis, who):
        return pltpu.make_async_remote_copy(src_ref=src, dst_ref=dst, send_sem=ssem, recv_sem=rsem,
                                            device_id={axis: who}, device_id_type=pl.DeviceIdType.MESH)

    def transfer(kind, ch):
        _, b0, n = CHUNKS[ch]
        n_a = n // 2
        every, half_a, half_b = pl.ds(b0, n), pl.ds(b0, n_a), pl.ds(b0 + n_a, n - n_a)
        src, dst, who = {
            D2D: lambda: (part.at[1 - c, :, every], peer.at[:, every], partner),
            OPP_A: lambda: (part.at[c, xo, half_a], opp_in.at[half_a], right),
            OPP_B: lambda: (part.at[c, xo, half_b], opp_in.at[half_b], left),
            OWN_R: lambda: (part.at[c, xr, half_b], left_in.at[half_b], right),
            OWN_L: lambda: (part.at[c, xl, half_a], right_in.at[half_a], left),
            MRG_R: lambda: (part.at[c, xr, half_a], left_in.at[half_a], right),
            MRG_L: lambda: (part.at[c, xl, half_b], right_in.at[half_b], left),
        }[kind]()
        return remote(src, dst, snd.at[SEND[kind]], rcv.at[RECV[kind], ch], 'data', who)

    def convert(ch):
        group, b0, n = CHUNKS[ch]
        family = GROUPS[group][0]
        if ch == 0:
            loads[0].wait()
        elif ch == 1:
            loads[1].wait()
            loads[2].wait()
        elif b0 == FIRST_IN:
            loads[3].wait()
        elif b0 == FIRST_OUT:
            loads[4].wait()

        def body(i, carry):
            b = b0 + i
            for t in range(n_chips):
                if family == 'in':
                    tile = gin[b - FIRST_IN, pl.ds(LANES * t, LANES), :].astype(F32)
                elif family == 'out':
                    tile = gout[b - FIRST_OUT, :, pl.ds(LANES * t, LANES)].astype(F32).T
                else:
                    four = gb[pl.ds(4 * (b - FIRST_B), 4), :, pl.ds(LANES * t, LANES)].astype(F32)
                    tile = four.reshape(LANES, LANES).T
                part[0, t, b] = tile[:ROWS]
                part[1, t, b] = tile[ROWS:]
            return carry

        lax.fori_loop(0, n, body, 0)

    def first_pair(dest, sem):
        every = pl.ds(0, CHUNKS[0][2])
        return remote(part.at[1 - c, dest, every], peer.at[dest, every], snd.at[0], sem, 'data', partner)

    def first_pairs():
        first_pair(xo, first_sem.at[0]).start()
        for dest in (xr, xl, x):
            first_pair(dest, rcv.at[D2D, 0]).start()

    def add_peer(ch, dest):
        _, b0, n = CHUNKS[ch]

        def body(i, carry):
            b = b0 + i
            part[c, dest, b] = part[c, dest, b] + peer[dest, b]
            return carry
        lax.fori_loop(0, n, body, 0, unroll=2)

    def opposite(ch):
        if ch == 0:
            first_pair(xo, first_sem.at[0]).wait_recv()
        else:
            transfer(D2D, ch).wait_recv()
        add_peer(ch, xo)
        transfer(OPP_A, ch).start()
        transfer(OPP_B, ch).start()
        if ch == 0:
            rest = peer.at[pl.ds(0, n_chips - 1), pl.ds(0, CHUNKS[0][2])]
            remote(rest, rest, snd.at[0], rcv.at[D2D, 0], 'data', partner).wait_recv()
        add_peer(ch, xr)
        add_peer(ch, xl)
        if ch < EARLY_OWN:
            own(ch)
        add_peer(ch, x)

    def own(ch):
        transfer(OWN_R, ch).start()
        transfer(OWN_L, ch).start()

    def merge(ch):
        _, b0, n = CHUNKS[ch]
        n_a = n // 2

        def add(dest, lo, hi):
            def body(b, carry):
                part[c, dest, b] = part[c, dest, b] + opp_in[b]
                return carry
            lax.fori_loop(lo, hi, body, 0)

        every = opp_in.at[pl.ds(b0, n)]
        remote(every, every, snd.at[1], rcv.at[OPP, ch], 'data', left).wait_recv()
        add(xr, b0, b0 + n_a)
        transfer(MRG_R, ch).start()
        add(xl, b0 + n_a, b0 + n)
        transfer(MRG_L, ch).start()
        if ch >= EARLY_OWN:
            own(ch)

    lane_iota = lax.broadcasted_iota(jnp.int32, (ROWS, LANES), 1)

    def finish(ch):
        group, b0, n = CHUNKS[ch]
        family, g0, _ = GROUPS[group]
        every = pl.ds(b0, n)
        two = peer.at[pl.ds(0, 2), every]
        remote(two, two, snd.at[2], rcv.at[LAST, ch], 'data', right).wait_recv()

        def block(b):
            g = (part[c, x, b] + left_in[b] + right_in[b]) * (1.0 / n_data)
            grad[b] = g
            sq = g * g + EPS_SQ
            sums = jnp.sum(sq, axis=0, keepdims=True)
            if group in near:
                half = lane_sum[group].shape[1]
                lane_sum[group][lax.div(b - g0, half), pl.ds(lax.rem(b - g0, half), 1), :] = sums
            else:
                lane_sum[group][pl.ds(b - g0, 1), :] = sums
            return g, sq

        if family == 'b':
            def body(i, carry):
                b = b0 + i
                g, _ = block(b)
                gt = g.T
                st = (gt * gt + EPS_SQ).reshape(4, WIDE, ROWS)
                comp_b[pl.ds(b - FIRST_B, 1), :, 0:ROWS] = jnp.sum(st, axis=1)[None]
                return carry
            lax.fori_loop(0, n, body, 0, unroll=2)
        else:
            which = 0 if family == 'in' else 1

            def body(i, acc):
                b = b0 + i
                _, sq = block(b)
                return jnp.where(lane_iota == b - (FIRST_IN if family == 'in' else FIRST_OUT), jnp.sum(sq, axis=1, keepdims=True), acc)
            acc_t[which] = lax.fori_loop(0, n, body, acc_t[which], unroll=2)

    def gather(src, dst, sems, slot, axis, op):
        send, recv = sems[0].at[slot], sems[1].at[slot]
        rank, n = {'data': (me, n_data), 'model': (mod, n_model), 'chip': (x, n_chips)}[axis]
        mesh_axis = 'model' if axis == 'model' else 'data'
        if op == 'start':
            dst[rank] = src[...]
            for who in others(axis):
                remote(src, dst.at[rank], send, recv, mesh_axis, who).start()
            return
        rest = dst.at[pl.ds(0, n - 1)]
        done = remote(rest, rest, send, recv, mesh_axis, partner if mesh_axis == 'data' else mod)
        if op == 'recv':
            done.wait_recv()
        else:
            done.wait_send()

    def total(dst, n):
        acc = dst[0]
        for r in range(1, n):
            acc = acc + dst[r]
        return acc

    d_sems, m_sems, s_sems = (dsnd, drcv), (msnd, mrcv), (ssnd, srcv)

    def pair_ex(group):
        i = SLOT[group]
        return remote(lane_sum[group], near[group], psnd.at[i], prcv.at[i], 'data', partner)

    def lane_ex(group, op):
        pairs = group in near
        gather(both[group].at[c] if pairs else lane_sum[group], dat_got[group], d_sems, SLOT[group], 'chip' if pairs else 'data', op)

    def back_ex(group):
        i = SLOT[group]
        return remote(whole[group].at[c], whole[group].at[c], bsnd.at[i], brcv.at[i], 'data', partner)

    def lane_back(group):
        lane_ex(group, 'recv')
        whole[group][c] = total(dat_got[group], n_chips)
        back_ex(group).start()

    def lane_start(group):
        if group in near:
            pair_ex(group).start()
        else:
            lane_ex(group, 'start')

    def lane_pair(group):
        pair_ex(group).wait_recv()
        both[group][...] = lane_sum[group][...] + near[group][...]
        lane_ex(group, 'start')

    def model_ex(group, op):
        gather(mod_blk[group], mod_got[group], m_sems, SLOT[group], 'model', op)

    def scal_ex(name, op):
        i = SLOT[name]
        src, dst = (raw[name], raw_got[name]) if name in raw else (scal.at[i], got_s.at[i])
        gather(src, dst, s_sems, i, 'data', op)

    def weights_start():
        for cp in w_loads + small:
            cp.wait()
        turn[...] = jnp.zeros_like(turn)
        turn[0:WIDE, 0:N_QKV] = col_q[...]
        turn[...] = turn[...].T
        turn[N_QKV:N_QKV + N_O, 0:WIDE] = row_o[...]
        row = turn[pl.ds(0, N_B, stride=4), :]
        for q in range(1, 4):
            row = row + pltpu.roll(turn[pl.ds(q, N_B, stride=4), :], WIDE * q, 1)
        lane_b[...] = row
        wtab[...] = jnp.zeros_like(wtab)
        vtab[...] = jnp.zeros_like(vtab)

        def squares(ref, row, width):
            def body(b, carry):
                w = ref[b]
                wtab[pl.ds(row + b, 1), 0:width] = jnp.sum(w * w, axis=0, keepdims=True)
                return carry
            lax.fori_loop(0, ref.shape[0], body, 0, unroll=6)

        squares(w_in, ROW_IN, LANES)
        squares(w_out, ROW_OUT, LANES)
        squares(w_q, ROW_B, ROWS)
        squares(w_o, ROW_B + N_QKV, ROWS)
        vtab[ROW_OUT:ROW_OUT + N_OUT, :] = row_out[...]
        vtab[ROW_B + 54:ROW_B + 72, 0:WIDE] = row_o[...]
        mod_w[0:1, :] = jnp.sum(wtab[...].T, axis=0, keepdims=True)
        mod_w[1:2, :] = jnp.sum(vtab[...].T, axis=0, keepdims=True) / n_data
        gather(mod_w, got_w, m_sems, SLOT['w'], 'model', 'start')

    def weights_next():
        gather(mod_w, got_w, m_sems, SLOT['w'], 'model', 'recv')
        scal[SLOT['w']] = total(got_w, n_model)
        scal_ex('w', 'start')

    def weights_done():
        scal_ex('w', 'recv')
        w_all[...] = total(got_s.at[SLOT['w']], n_data)
        turn[0:2, :] = w_all[...]
        wcol[...] = turn[...].T

    def after_lanes(group):
        family, g0, n = GROUPS[group]
        r0 = LANE_ROW[group]
        if group in near:
            back_ex(group).wait_recv()
            sums = jnp.concatenate([whole[group][0], whole[group][1]], axis=0)
        else:
            lane_ex(group, 'recv')
            sums = total(dat_got[group], n_data)
        lo = g0 - (FIRST_OUT if family == 'out' else g0)
        if family == 'b':
            mom = lane_b[...]
        else:
            mom = (col_in if family == 'in' else row_out)[lo:lo + n, :]
        new = BETA_TWO * mom + GAIN * (sums / 512.0)
        rlane[r0:r0 + n, :] = lax.rsqrt(new)
        if family == 'b':
            def body(s, carry):
                h = grad[FIRST_B + s] * rlane[pl.ds(r0 + s, 1), :]
                t = h.T.reshape(4, WIDE, ROWS)
                ht[pl.ds(4 * s, 4)] = t
                comp_b[pl.ds(s, 1), :, ROWS:LANES] = jnp.sum(t * t, axis=1)[None]
                return carry
            lax.fori_loop(0, n, body, 0, unroll=3)
            mod_b[...] = comp_b[...].reshape(4 * N_B, LANES)
        else:
            def body(b, acc):
                h = grad[g0 + b] * rlane[pl.ds(r0 + b, 1), :]
                grad[g0 + b] = h
                return jnp.where(lane_iota == lo + b, jnp.sum(h * h, axis=1, keepdims=True), acc)
            acc_z = lax.fori_loop(0, n, body, jnp.zeros((ROWS, LANES), F32), unroll=4)
            turned = jnp.concatenate([acc_t[0 if family == 'in' else 1], acc_z], axis=0).T
            mod_blk[group][...] = turned[lo:lo + n]
        model_ex(group, 'start')
        if family == 'b':
            turn[...] = jnp.zeros_like(turn)
            for q in range(4):
                turn[pl.ds(q, N_B, stride=4), :] = pltpu.roll(new, (LANES - WIDE * q) % LANES, 1)
            row_o_o[...] = turn[N_QKV:N_QKV + N_O, 0:WIDE]
            turn[...] = turn[...].T
            col_q_o[...] = turn[0:WIDE, 0:N_QKV]
        else:
            (col_in_o if family == 'in' else row_out_o)[lo:lo + n, :] = new

    def after_model(group):
        family, g0, n = GROUPS[group]
        lo = g0 - (FIRST_OUT if family == 'out' else g0)
        model_ex(group, 'recv')
        sums_z = total(mod_got[group], n_model)
        sums, z = sums_z[:, 0:ROWS], sums_z[:, ROWS:LANES]
        if family == 'b':
            mom = jnp.concatenate([row_q[...], col_o[...]], axis=0)
        else:
            mom = (row_in if family == 'in' else col_out)[lo:lo + n, :]
        new = BETA_TWO * mom + GAIN * (sums / full[family])
        mean_part = GAIN * (sums / 512.0)
        if family == 'in':
            term = new
        elif family == 'out':
            term = mean_part
        else:
            term = jnp.where(lax.broadcasted_iota(jnp.int32, new.shape, 0) < N_QKV, new, mean_part)
        r0 = TAB_ROW[group]
        r1 = r0 + new.shape[0]
        if family == 'out':
            raw[group][:, 0:ROWS] = z / new
            raw[group][:, ROWS:LANES] = term
            scal_ex(group, 'start')
        else:
            tab[r0:r1, 0:ROWS] = z / new
            tab[r0:r1, ROWS:LANES] = term
        rtab[r0:r1, 0:ROWS] = lax.rsqrt(new)
        if family == 'b':
            row_q_o[...] = new[:N_QKV]
            col_o_o[...] = new[N_QKV:]
        else:
            (row_in_o if family == 'in' else col_out_o)[lo:lo + n, :] = new

    def scalars_start(family):
        e = SLOT[family]
        turned = tab[...].T
        scal[e, 0:1, :] = jnp.sum(turned[:ROWS], axis=0, keepdims=True)
        scal[e, 1:2, :] = jnp.sum(turned[ROWS:], axis=0, keepdims=True)
        scal_ex(family, 'start')
        if family != 'b':
            rsub[...] = rtab[:, 0:ROWS].T

    def factor(q, s, w, v, family):
        rows = 512.0 if family == 'in' else float(full[family])
        size = 512.0 * full[family]
        m = (s if family == 'in' else BETA_TWO * v + s) / rows
        return jnp.sqrt(m) * (LR_BASE * jnp.maximum(1e-3, jnp.sqrt(w / size))) / jnp.maximum(1.0, jnp.sqrt(m * q / size))

    def after_scalars(family):
        e = SLOT[family]
        scal_ex(family, 'recv')
        tot = total(got_s.at[e], n_data)
        scale = factor(tot[0:1], tot[1:2], w_all[0:1, :], w_all[1:2, :], family)
        if family == 'b':
            turn[...] = jnp.broadcast_to(scale, (LANES, LANES)).T
            rtab[ROW_B:ROW_B + 72, 0:ROWS] = rtab[ROW_B:ROW_B + 72, 0:ROWS] * turn[ROW_B:ROW_B + 72, 0:ROWS]
            for ref, b0 in ((w_q, 0), (w_o, N_QKV)):
                def body(b, carry, ref=ref, b0=b0):
                    ref[b] = ref[b] - ht[b0 + b] * rtab[pl.ds(ROW_B + b0 + b, 1), 0:ROWS]
                    return carry
                lax.fori_loop(0, ref.shape[0], body, 0, unroll=6)
        else:
            fac = rsub[...] * scale

            def body(b, carry):
                f = jnp.sum(jnp.where(lane_iota == ROW_IN + b, fac, 0.0), axis=1, keepdims=True)
                w_in[b] = w_in[b] - grad[FIRST_IN + b] * f
                return carry
            lax.fori_loop(0, N_IN, body, 0, unroll=4)

    def prepare_out():
        fac = rtab[:, 0:ROWS].T

        def body(b, carry):
            f = jnp.sum(jnp.where(lane_iota == ROW_OUT + b, fac, 0.0), axis=1, keepdims=True)
            grad[FIRST_OUT + b] = grad[FIRST_OUT + b] * f
            return carry
        lax.fori_loop(0, N_OUT, body, 0, unroll=4)

    def apply_out(group):
        _, g0, n = GROUPS[group]
        lo, r0 = g0 - FIRST_OUT, TAB_ROW[group]
        scal_ex(group, 'recv')
        tot = total(raw_got[group], n_data)
        q = jnp.sum(tot[:, 0:ROWS], axis=1, keepdims=True)
        s = jnp.sum(tot[:, ROWS:LANES], axis=1, keepdims=True)
        scale = factor(q, s, wcol[r0:r0 + n, 0:1], wcol[r0:r0 + n, 1:2], 'out')
        krow[lo:lo + n, :] = jnp.broadcast_to(scale, (n, LANES))
        for b in range(lo, lo + n):
            w_out[b] = w_out[b] - grad[FIRST_OUT + b] * krow[b:b + 1, :]

    def sent_early():
        for i, ref in enumerate((peer, opp_in, left_in, right_in)):
            remote(ref, ref, snd.at[i], rcv.at[0, 0], 'data', partner).wait_send()
        gather(mod_w, got_w, m_sems, SLOT['w'], 'model', 'send')
        for group in near:
            pair_ex(group).wait_send()
            back_ex(group).wait_send()
        for group in GROUPS:
            lane_ex(group, 'send')
        model_ex('b', 'send')
        scal_ex('w', 'send')
        scal_ex('b', 'send')

    def sent_mid():
        for group in ('in', 'out_a', 'out_b'):
            model_ex(group, 'send')
        scal_ex('in', 'send')
        scal_ex('out_a', 'send')

    def sent_late():
        scal_ex('out_b', 'send')

    acc_t[...] = jnp.zeros_like(acc_t)
    tab[...] = jnp.zeros_like(tab)
    rtab[...] = jnp.zeros_like(rtab)

    convert(0)
    for cp in small + w_loads:
        cp.start()
    pl.semaphore_wait(barrier, len(neighbours))
    first_pairs()
    greet(meet.at[0])
    last = N_CH - 1 + LAG_FINISH
    steps = {}

    def at(k, do, *args):
        steps.setdefault(k, []).append((do, args))

    def pass_on(i):
        pl.semaphore_wait(meet.at[i], len(neighbours))
        if i < 2:
            greet(meet.at[i + 1])

    at(2, pass_on, 0)
    at(3, pass_on, 1)
    at(4, pass_on, 2)
    at(4, weights_start)
    at(6, weights_next)
    at(8, weights_done)
    k_b, k_in, k_a = (LAST_CHUNK[g] + LAG_FINISH for g in ('b', 'in', 'out_a'))
    at(k_b + 1, lane_pair, 'b')
    at(k_b + 3, lane_back, 'b')
    at(k_b + 4, after_lanes, 'b')
    at(k_b + 6, after_model, 'b')
    at(k_b + 6, scalars_start, 'b')
    at(k_in + 1, lane_pair, 'in')
    at(k_in + 3, lane_back, 'in')
    tail = ((after_lanes, 'in'), (after_lanes, 'out_a'), (after_lanes, 'out_b'), (after_scalars, 'b'), (sent_early,), (after_model, 'in'),
            (scalars_start, 'in'), (after_model, 'out_a'), (after_model, 'out_b'), (prepare_out,), (sent_mid,), (after_scalars, 'in'),
            (apply_out, 'out_a'), (apply_out, 'out_b'), (sent_late,))
    for k in range(1 - AHEAD, last + 1):
        if 0 <= k < N_CH:
            opposite(k)
        if k + AHEAD < N_CH:
            convert(k + AHEAD)
            transfer(D2D, k + AHEAD).start()
        for ch in range(N_CH):
            if k == ch + (LAG_MERGE if ch < N_CH - 1 else 1):
                merge(ch)
        for do, args in steps.get(k, ()):
            do(*args)
        if 0 <= k - LAG_FINISH < N_CH:
            finish(k - LAG_FINISH)
        for group in GROUPS:
            if k == LAST_CHUNK[group] + LAG_FINISH:
                lane_start(group)
    for do, *args in tail:
        do(*args)


def deliver(*refs):
    srcs, dsts, sem = refs[:12], refs[12:24], refs[24]
    copies = [pltpu.make_async_copy(src, dst, sem.at[i]) for i, (src, dst) in enumerate(zip(srcs, dsts))]
    for cp in copies:
        cp.start()
    for cp in copies:
        cp.wait()


def solution(mesh):
    axis_sizes = dict(mesh.shape)
    n_data, n_model = axis_sizes['data'], axis_sizes['model']
    n_chips = n_data // 2
    rows_data = (P('data', None, None, 'model'), P(None, 'data', 'model'), P(None, 'data'), P(None, 'model'))
    rows_model = (P('data', None, 'model', None), P(None, 'model', 'data'), P(None, 'model'), P(None, 'data'))

    def vmem(*dims):
        return pltpu.VMEM(dims, F32)

    small = (vmem(24, ROWS), vmem(24, LANES), vmem(12, LANES), vmem(12, ROWS), vmem(54, ROWS), vmem(WIDE, 54), vmem(18, WIDE), vmem(18, ROWS))
    results = (vmem(24, ROWS, LANES), vmem(12, ROWS, LANES), vmem(54, WIDE, ROWS), vmem(18, WIDE, ROWS), *small)
    scratch = [
        *small, vmem(N_B, LANES), vmem(LANES, LANES),
        pltpu.VMEM((24, 512, LANES), jnp.bfloat16), pltpu.VMEM((12, LANES, 512), jnp.bfloat16),
        pltpu.VMEM((72, WIDE, 512), jnp.bfloat16),
        vmem(2, n_chips, N_SUP, ROWS, LANES), vmem(n_chips, N_SUP, ROWS, LANES),
        vmem(N_SUP, ROWS, LANES), vmem(N_SUP, ROWS, LANES), vmem(N_SUP, ROWS, LANES), vmem(N_SUP, ROWS, LANES),
        vmem(2, LANES), vmem(72, WIDE, ROWS),
        vmem(2, 9, LANES), vmem(2, 12, LANES), vmem(N_OUT_A, LANES), vmem(N_OUT_B, LANES),
        *(vmem(2, n, LANES) for n in (9, 12, 9, 12, 9, 12)),
        vmem(ROWS, LANES), vmem(2, ROWS, LANES), vmem(N_B, 4, LANES),
        vmem(LANES, LANES), vmem(LANES, LANES), vmem(ROWS, LANES), vmem(LANES, LANES), vmem(LANES, LANES),
        vmem(72, LANES), vmem(24, LANES), vmem(N_OUT_A, LANES), vmem(N_OUT_B, LANES), vmem(2, LANES), vmem(5, 2, LANES),
        vmem(n_chips, 9, LANES), vmem(n_chips, 12, LANES), vmem(n_data, N_OUT_A, LANES), vmem(n_data, N_OUT_B, LANES),
        vmem(n_model, 72, LANES), vmem(n_model, 24, LANES), vmem(n_model, N_OUT_A, LANES), vmem(n_model, N_OUT_B, LANES),
        vmem(n_model, 2, LANES), vmem(5, n_data, 2, LANES),
        vmem(N_OUT_A, LANES), vmem(N_OUT_B, LANES), vmem(n_data, N_OUT_A, LANES), vmem(n_data, N_OUT_B, LANES), vmem(LANES, LANES), vmem(12, LANES),
        pltpu.SemaphoreType.DMA((5,)), pltpu.SemaphoreType.DMA((4,)), pltpu.SemaphoreType.DMA((8,)), pltpu.SemaphoreType.DMA((1,)),
        pltpu.SemaphoreType.REGULAR((3,)),
        pltpu.SemaphoreType.DMA((4,)), pltpu.SemaphoreType.DMA((3, N_CH)),
        *(pltpu.SemaphoreType.DMA((n,)) for n in (2, 2, 2, 2, 4, 4, 5, 5, 5, 5)),
    ]
    hbm, in_vmem = pl.BlockSpec(memory_space=pltpu.HBM), pl.BlockSpec(memory_space=pltpu.VMEM)

    def step_all(grad_in, w_in, row_in, col_in, grad_out, w_out, row_out, col_out,
                 grad_qkv, w_qkv, row_qkv, col_qkv, grad_o, w_o, row_o, col_o):
        kept = pl.pallas_call(
            functools.partial(kernel, n_data, n_model),
            name='adafactor_step',
            out_shape=results,
            in_specs=[hbm] * 16,
            out_specs=[in_vmem] * 12,
            scratch_shapes=scratch,
            compiler_params=pltpu.CompilerParams(collective_id=0, has_side_effects=True, vmem_limit_bytes=VMEM_LIMIT),
        )(grad_in[0], grad_out[0], grad_qkv[0].transpose(0, 2, 1), grad_o[0],
          w_in, w_out.transpose(0, 2, 1), w_qkv.transpose(0, 2, 1), w_o,
          row_in, col_in, row_out, col_out, row_qkv, col_qkv.T, row_o, col_o)
        (w_in_new, w_out_new, w_qkv_new, w_o_new, row_in_new, col_in_new, row_out_new, col_out_new,
         row_qkv_new, col_qkv_new, row_o_new, col_o_new) = pl.pallas_call(
            deliver,
            name='deliver',
            out_shape=[jax.ShapeDtypeStruct(r.shape, F32) for r in results],
            in_specs=[in_vmem] * 12,
            out_specs=[hbm] * 12,
            scratch_shapes=[pltpu.SemaphoreType.DMA((12,))],
            compiler_params=pltpu.CompilerParams(vmem_limit_bytes=10 ** 6),
        )(*(pltpu.with_memory_space_constraint(a, pltpu.VMEM) for a in kept))
        return (w_in_new, row_in_new, col_in_new, w_out_new.transpose(0, 2, 1), row_out_new, col_out_new,
                w_qkv_new.transpose(0, 2, 1), row_qkv_new, col_qkv_new.T, w_o_new, row_o_new, col_o_new)

    in_specs = rows_data + rows_model + rows_data + rows_model
    out_specs = rows_data[1:] + rows_model[1:] + rows_data[1:] + rows_model[1:]
    return jax.shard_map(step_all, mesh=mesh, in_specs=in_specs, out_specs=out_specs, check_vma=False)
```

```python
import functools

import jax
import jax.numpy as jnp
from jax import lax
from jax.experimental import pallas as pl
from jax.experimental.pallas import tpu as pltpu
from jax.sharding import PartitionSpec as P

OPT_STEP = 4
EPS_SQ = 1e-30
BETA_TWO = 1.0 - OPT_STEP ** -0.8
GAIN = 1.0 - BETA_TWO
LR_BASE = min(1e-2, OPT_STEP ** -0.5)
F32 = jnp.float32
LANES, ROWS, WIDE = 128, 64, 32
VMEM_LIMIT = 60 * 10 ** 6

N_IN, N_B, N_OUT = 24, 18, 12
N_SUP = N_IN + N_B + N_OUT
FIRST_B, FIRST_IN, FIRST_OUT = 0, N_B, N_B + N_IN
N_QKV, N_O = 54, 18
N_OUT_B = 2
N_OUT_A = N_OUT - N_OUT_B
ROW_IN, ROW_OUT, ROW_B = 0, 24, 40
GROUPS = {'b': ('b', FIRST_B, N_B), 'in': ('in', FIRST_IN, N_IN), 'out_a': ('out', FIRST_OUT, N_OUT_A), 'out_b': ('out', FIRST_OUT + N_OUT_A, N_OUT_B)}
SIZES = (('b', (2, 4, 6, 6)), ('in', (6, 6, 6, 6)), ('out_a', (4, 4, 2)), ('out_b', (2,)))


def cut():
    chunks, at = [], 0
    for group, sizes in SIZES:
        for n in sizes:
            chunks.append((group, at, n))
            at += n
    return tuple(chunks)


CHUNKS = cut()
N_CH = len(CHUNKS)
LAST_CHUNK = {g: max(i for i, c in enumerate(CHUNKS) if c[0] == g) for g in GROUPS}
D2D, OPP_A, OPP_B, OWN_R, OWN_L, MRG_R, MRG_L = range(7)
SEND = (0, 1, 1, 2, 3, 2, 3)
OPP, LAST = 1, 2
RECV = (D2D, OPP, OPP, LAST, LAST, LAST, LAST)
SLOT = {'b': 0, 'in': 1, 'out_a': 2, 'out_b': 3, 'w': 4}
LANE_ROW = {'b': 0, 'in': 24, 'out_a': 48, 'out_b': 48 + N_OUT_A}
TAB_ROW = {'b': ROW_B, 'in': ROW_IN, 'out_a': ROW_OUT, 'out_b': ROW_OUT + N_OUT_A}
AHEAD, EARLY_OWN, LAG_MERGE, LAG_FINISH = 2, 3, 2, 3


def kernel(n_data, n_model, gin_h, gout_h, gq_h, go_h, win_h, wout_h, wq_h, wo_h,
           row_in_h, col_in_h, row_out_h, col_out_h, row_q_h, col_q_h, row_o_h, col_o_h,
           w_in, w_out, w_q, w_o, row_in_o, col_in_o, row_out_o, col_out_o, row_q_o, col_q_o, row_o_o, col_o_o,
           row_in, col_in, row_out, col_out, row_q, col_q, row_o, col_o, lane_b, turn,
           gin, gout, gb, part, peer, opp_in, left_in, right_in, grad, w_all, ht,
           sum_b, sum_in, sum_a, sum_o, near_b, near_in, both_b, both_in, full_b, full_in, rlane, acc_t, comp_b, tab, rtab, rsub, wtab, vtab,
           mod_b, mod_in, mod_a, mod_o, mod_w, scal, dat_b, dat_in, dat_a, dat_o, got_b, got_in, got_a, got_o, got_w, got_s,
           pair_mom, raw_o, graw_o, wcol, krow,
           load_sem, w_sem, small_sem, first_sem, meet, snd, rcv, psnd, prcv, bsnd, brcv, dsnd, drcv, msnd, mrcv, ssnd, srcv):
    me = lax.axis_index('data')
    mod = lax.axis_index('model')
    n_chips = n_data // 2
    x, c = lax.div(me, 2), lax.rem(me, 2)
    xr, xl, xo = lax.rem(x + 1, n_chips), lax.rem(x + 3, n_chips), lax.rem(x + 2, n_chips)
    partner, right, left = 2 * x + 1 - c, 2 * xr + c, 2 * xl + c
    full = {'in': n_model * LANES, 'out': n_model * LANES, 'b': n_model * WIDE}
    lane_sum = {'b': sum_b, 'in': sum_in, 'out_a': sum_a, 'out_b': sum_o}
    near = {'b': near_b, 'in': near_in}
    both = {'b': both_b, 'in': both_in}
    whole = {'b': full_b, 'in': full_in}
    dat_got = {'b': dat_b, 'in': dat_in, 'out_a': dat_a, 'out_b': dat_o}
    mod_blk = {'b': mod_b, 'in': mod_in, 'out_a': mod_a, 'out_b': mod_o}
    mod_got = {'b': got_b, 'in': got_in, 'out_a': got_a, 'out_b': got_o}

    loads = [pltpu.make_async_copy(gq_h.at[pl.ds(0, 8)], gb.at[pl.ds(0, 8)], load_sem.at[0]),
             pltpu.make_async_copy(gq_h.at[pl.ds(8, 46)], gb.at[pl.ds(8, 46)], load_sem.at[1]),
             pltpu.make_async_copy(go_h, gb.at[pl.ds(54, 18)], load_sem.at[2]),
             pltpu.make_async_copy(gin_h, gin, load_sem.at[3]),
             pltpu.make_async_copy(gout_h, gout, load_sem.at[4])]
    w_loads = [pltpu.make_async_copy(win_h, w_in, w_sem.at[0]),
               pltpu.make_async_copy(wout_h, w_out, w_sem.at[1]),
               pltpu.make_async_copy(wq_h, w_q, w_sem.at[2]),
               pltpu.make_async_copy(wo_h, w_o, w_sem.at[3])]
    small = [pltpu.make_async_copy(src, dst, small_sem.at[i]) for i, (src, dst) in enumerate((
        (row_in_h, row_in), (col_in_h, col_in), (row_out_h, row_out), (col_out_h, col_out),
        (row_q_h, row_q), (col_q_h, col_q), (row_o_h, row_o), (col_o_h, col_o)))]
    loads[0].start()

    barrier = pltpu.get_barrier_semaphore()

    def others(axis):
        side = 4 if axis == 'model' else 2
        n, rank = (n_model, mod) if axis == 'model' else (n_data, me)
        high, low, rows = lax.div(rank, side), lax.rem(rank, side), n // side

        def hops(d):
            up, over = d // side, d % side
            return min(up, rows - up) * (side - 1) + min(over, side - over)

        for d in sorted(range(1, n), key=lambda d: -hops(d)):
            if axis != 'chip' or d % side == 0:
                yield lax.rem(high + d // side, rows) * side + lax.rem(low + d % side, side)

    side = 4
    z, y = lax.div(mod, side), lax.rem(mod, side)
    neighbours = [('data', who) for who in (partner, right, left)]
    for step in (1, side - 1):
        neighbours.append(('model', side * z + lax.rem(y + step, side)))
        neighbours.append(('model', side * lax.rem(z + step, n_model // side) + y))

    def greet(sem):
        for axis, who in neighbours:
            pl.semaphore_signal(sem, inc=1, device_id={axis: who}, device_id_type=pl.DeviceIdType.MESH)

    greet(barrier)
    for cp in loads[1:]:
        cp.start()

    def remote(src, dst, ssem, rsem, axis, who):
        return pltpu.make_async_remote_copy(src_ref=src, dst_ref=dst, send_sem=ssem, recv_sem=rsem,
                                            device_id={axis: who}, device_id_type=pl.DeviceIdType.MESH)

    def transfer(kind, ch):
        _, b0, n = CHUNKS[ch]
        n_a = n // 2
        every, half_a, half_b = pl.ds(b0, n), pl.ds(b0, n_a), pl.ds(b0 + n_a, n - n_a)
        src, dst, who = {
            D2D: lambda: (part.at[1 - c, :, every], peer.at[:, every], partner),
            OPP_A: lambda: (part.at[c, xo, half_a], opp_in.at[half_a], right),
            OPP_B: lambda: (part.at[c, xo, half_b], opp_in.at[half_b], left),
            OWN_R: lambda: (part.at[c, xr, half_b], left_in.at[half_b], right),
            OWN_L: lambda: (part.at[c, xl, half_a], right_in.at[half_a], left),
            MRG_R: lambda: (part.at[c, xr, half_a], left_in.at[half_a], right),
            MRG_L: lambda: (part.at[c, xl, half_b], right_in.at[half_b], left),
        }[kind]()
        return remote(src, dst, snd.at[SEND[kind]], rcv.at[RECV[kind], ch], 'data', who)

    def convert(ch):
        group, b0, n = CHUNKS[ch]
        family = GROUPS[group][0]
        if ch == 0:
            loads[0].wait()
        elif ch == 1:
            loads[1].wait()
            loads[2].wait()
        elif b0 == FIRST_IN:
            loads[3].wait()
        elif b0 == FIRST_OUT:
            loads[4].wait()

        def body(i, carry):
            b = b0 + i
            for t in range(n_chips):
                if family == 'in':
                    tile = gin[b - FIRST_IN, pl.ds(LANES * t, LANES), :].astype(F32)
                elif family == 'out':
                    tile = gout[b - FIRST_OUT, :, pl.ds(LANES * t, LANES)].astype(F32).T
                else:
                    four = gb[pl.ds(4 * (b - FIRST_B), 4), :, pl.ds(LANES * t, LANES)].astype(F32)
                    tile = four.reshape(LANES, LANES).T
                part[0, t, b] = tile[:ROWS]
                part[1, t, b] = tile[ROWS:]
            return carry

        lax.fori_loop(0, n, body, 0)

    def first_pair(dest, sem):
        every = pl.ds(0, CHUNKS[0][2])
        return remote(part.at[1 - c, dest, every], peer.at[dest, every], snd.at[0], sem, 'data', partner)

    def first_pairs():
        first_pair(xo, first_sem.at[0]).start()
        for dest in (xr, xl, x):
            first_pair(dest, rcv.at[D2D, 0]).start()

    def add_peer(ch, dest):
        _, b0, n = CHUNKS[ch]

        def body(i, carry):
            b = b0 + i
            part[c, dest, b] = part[c, dest, b] + peer[dest, b]
            return carry
        lax.fori_loop(0, n, body, 0, unroll=2)

    def opposite(ch):
        if ch == 0:
            first_pair(xo, first_sem.at[0]).wait_recv()
        else:
            transfer(D2D, ch).wait_recv()
        add_peer(ch, xo)
        transfer(OPP_A, ch).start()
        transfer(OPP_B, ch).start()
        if ch == 0:
            rest = peer.at[pl.ds(0, n_chips - 1), pl.ds(0, CHUNKS[0][2])]
            remote(rest, rest, snd.at[0], rcv.at[D2D, 0], 'data', partner).wait_recv()
        add_peer(ch, xr)
        add_peer(ch, xl)
        if ch < EARLY_OWN:
            own(ch)
        add_peer(ch, x)

    def own(ch):
        transfer(OWN_R, ch).start()
        transfer(OWN_L, ch).start()

    def merge(ch):
        _, b0, n = CHUNKS[ch]
        n_a = n // 2

        def add(dest, lo, hi):
            def body(b, carry):
                part[c, dest, b] = part[c, dest, b] + opp_in[b]
                return carry
            lax.fori_loop(lo, hi, body, 0)

        every = opp_in.at[pl.ds(b0, n)]
        remote(every, every, snd.at[1], rcv.at[OPP, ch], 'data', left).wait_recv()
        add(xr, b0, b0 + n_a)
        transfer(MRG_R, ch).start()
        add(xl, b0 + n_a, b0 + n)
        transfer(MRG_L, ch).start()
        if ch >= EARLY_OWN:
            own(ch)

    lane_iota = lax.broadcasted_iota(jnp.int32, (ROWS, LANES), 1)

    def row_sums(first, second):
        return jnp.sum(jnp.concatenate([first, second], axis=0).T, axis=0, keepdims=True)

    def finish(ch):
        group, b0, n = CHUNKS[ch]
        family, g0, _ = GROUPS[group]
        every = pl.ds(b0, n)
        two = peer.at[pl.ds(0, 2), every]
        remote(two, two, snd.at[2], rcv.at[LAST, ch], 'data', right).wait_recv()

        def block(b):
            g = (part[c, x, b] + left_in[b] + right_in[b]) * (1.0 / n_data)
            grad[b] = g
            sq = g * g + EPS_SQ
            sums = jnp.sum(sq, axis=0, keepdims=True)
            if group in near:
                half = lane_sum[group].shape[1]
                lane_sum[group][lax.div(b - g0, half), pl.ds(lax.rem(b - g0, half), 1), :] = sums
            else:
                lane_sum[group][pl.ds(b - g0, 1), :] = sums
            return g, sq

        if family == 'b':
            def body(i, carry):
                b = b0 + i
                g, _ = block(b)
                gt = g.T
                st = (gt * gt + EPS_SQ).reshape(4, WIDE, ROWS)
                comp_b[pl.ds(b - FIRST_B, 1), :, 0:ROWS] = jnp.sum(st, axis=1)[None]
                return carry
            lax.fori_loop(0, n, body, 0, unroll=2)
        elif group == 'out_b':
            first, second = (block(b0 + i)[1] for i in range(N_OUT_B))
            lane_start(group)
            mod_o[0:1, :] = row_sums(first, second)
        else:
            which = 0 if family == 'in' else 1

            def body(i, acc):
                b = b0 + i
                _, sq = block(b)
                return jnp.where(lane_iota == b - (FIRST_IN if family == 'in' else FIRST_OUT), jnp.sum(sq, axis=1, keepdims=True), acc)
            acc_t[which] = lax.fori_loop(0, n, body, acc_t[which], unroll=2)

    def gather(src, dst, sems, slot, axis, op):
        send, recv = sems[0].at[slot], sems[1].at[slot]
        rank, n = {'data': (me, n_data), 'model': (mod, n_model), 'chip': (x, n_chips)}[axis]
        mesh_axis = 'model' if axis == 'model' else 'data'
        if op == 'start':
            dst[rank] = src[...]
            for who in others(axis):
                remote(src, dst.at[rank], send, recv, mesh_axis, who).start()
            return
        rest = dst.at[pl.ds(0, n - 1)]
        done = remote(rest, rest, send, recv, mesh_axis, partner if mesh_axis == 'data' else mod)
        if op == 'recv':
            done.wait_recv()
        else:
            done.wait_send()

    def total(dst, n):
        acc = dst[0]
        for r in range(1, n):
            acc = acc + dst[r]
        return acc

    d_sems, m_sems, s_sems = (dsnd, drcv), (msnd, mrcv), (ssnd, srcv)

    def pair_ex(group):
        i = SLOT[group]
        return remote(lane_sum[group], near[group], psnd.at[i], prcv.at[i], 'data', partner)

    def lane_ex(group, op):
        pairs = group in near
        gather(both[group].at[c] if pairs else lane_sum[group], dat_got[group], d_sems, SLOT[group], 'chip' if pairs else 'data', op)

    def back_ex(group):
        i = SLOT[group]
        return remote(whole[group].at[c], whole[group].at[c], bsnd.at[i], brcv.at[i], 'data', partner)

    def lane_back(group):
        lane_ex(group, 'recv')
        whole[group][c] = total(dat_got[group], n_chips)
        back_ex(group).start()

    def lane_start(group):
        if group in near:
            pair_ex(group).start()
        else:
            lane_ex(group, 'start')

    def lane_pair(group):
        pair_ex(group).wait_recv()
        both[group][...] = lane_sum[group][...] + near[group][...]
        lane_ex(group, 'start')

    def model_ex(group, op):
        gather(mod_blk[group], mod_got[group], m_sems, SLOT[group], 'model', op)

    def scal_ex(name, op):
        i = SLOT[name]
        src, dst = (raw_o, graw_o) if name == 'out_b' else (scal.at[i], got_s.at[i])
        gather(src, dst, s_sems, i, 'data', op)

    def weights_start():
        for cp in w_loads + small:
            cp.wait()
        turn[...] = jnp.zeros_like(turn)
        turn[0:WIDE, 0:N_QKV] = col_q[...]
        turn[...] = turn[...].T
        turn[N_QKV:N_QKV + N_O, 0:WIDE] = row_o[...]
        row = turn[pl.ds(0, N_B, stride=4), :]
        for q in range(1, 4):
            row = row + pltpu.roll(turn[pl.ds(q, N_B, stride=4), :], WIDE * q, 1)
        lane_b[...] = row
        wtab[...] = jnp.zeros_like(wtab)
        vtab[...] = jnp.zeros_like(vtab)

        def squares(ref, row, width):
            def body(b, carry):
                w = ref[b]
                wtab[pl.ds(row + b, 1), 0:width] = jnp.sum(w * w, axis=0, keepdims=True)
                return carry
            lax.fori_loop(0, ref.shape[0], body, 0, unroll=6)

        squares(w_in, ROW_IN, LANES)
        squares(w_out, ROW_OUT, LANES)
        squares(w_q, ROW_B, ROWS)
        squares(w_o, ROW_B + N_QKV, ROWS)
        vtab[ROW_OUT:ROW_OUT + N_OUT, :] = row_out[...]
        vtab[ROW_B + 54:ROW_B + 72, 0:WIDE] = row_o[...]
        mod_w[0:1, :] = jnp.sum(wtab[...].T, axis=0, keepdims=True)
        mod_w[1:2, :] = jnp.sum(vtab[...].T, axis=0, keepdims=True) / n_data
        gather(mod_w, got_w, m_sems, SLOT['w'], 'model', 'start')

    def weights_next():
        gather(mod_w, got_w, m_sems, SLOT['w'], 'model', 'recv')
        scal[SLOT['w']] = total(got_w, n_model)
        scal_ex('w', 'start')

    def weights_done():
        scal_ex('w', 'recv')
        w_all[...] = total(got_s.at[SLOT['w']], n_data)
        turn[0:2, :] = w_all[...]
        wcol[...] = turn[...].T

    def after_lanes(group):
        family, g0, n = GROUPS[group]
        r0 = LANE_ROW[group]
        if group in near:
            back_ex(group).wait_recv()
            sums = jnp.concatenate([whole[group][0], whole[group][1]], axis=0)
        else:
            lane_ex(group, 'recv')
            sums = total(dat_got[group], n_data)
        lo = g0 - (FIRST_OUT if family == 'out' else g0)
        if family == 'b':
            mom = lane_b[...]
        else:
            mom = (col_in if family == 'in' else row_out)[lo:lo + n, :]
        new = BETA_TWO * mom + GAIN * (sums / 512.0)
        rlane[r0:r0 + n, :] = lax.rsqrt(new)
        if family == 'b':
            def body(s, carry):
                h = grad[FIRST_B + s] * rlane[pl.ds(r0 + s, 1), :]
                t = h.T.reshape(4, WIDE, ROWS)
                ht[pl.ds(4 * s, 4)] = t
                comp_b[pl.ds(s, 1), :, ROWS:LANES] = jnp.sum(t * t, axis=1)[None]
                return carry
            lax.fori_loop(0, n, body, 0, unroll=3)
            mod_b[...] = comp_b[...].reshape(4 * N_B, LANES)
        else:
            def body(b, acc):
                h = grad[g0 + b] * rlane[pl.ds(r0 + b, 1), :]
                grad[g0 + b] = h
                return jnp.where(lane_iota == lo + b, jnp.sum(h * h, axis=1, keepdims=True), acc)
            acc_z = lax.fori_loop(0, n, body, jnp.zeros((ROWS, LANES), F32), unroll=4)
            turned = jnp.concatenate([acc_t[0 if family == 'in' else 1], acc_z], axis=0).T
            mod_blk[group][...] = turned[lo:lo + n]
        model_ex(group, 'start')
        if family == 'b':
            turn[...] = jnp.zeros_like(turn)
            for q in range(4):
                turn[pl.ds(q, N_B, stride=4), :] = pltpu.roll(new, (LANES - WIDE * q) % LANES, 1)
            row_o_o[...] = turn[N_QKV:N_QKV + N_O, 0:WIDE]
            turn[...] = turn[...].T
            col_q_o[...] = turn[0:WIDE, 0:N_QKV]
        else:
            (col_in_o if family == 'in' else row_out_o)[lo:lo + n, :] = new

    def after_model(group):
        family, g0, n = GROUPS[group]
        lo = g0 - (FIRST_OUT if family == 'out' else g0)
        model_ex(group, 'recv')
        sums_z = total(mod_got[group], n_model)
        sums, z = sums_z[:, 0:ROWS], sums_z[:, ROWS:LANES]
        if family == 'b':
            mom = jnp.concatenate([row_q[...], col_o[...]], axis=0)
        else:
            mom = (row_in if family == 'in' else col_out)[lo:lo + n, :]
        new = BETA_TWO * mom + GAIN * (sums / full[family])
        mean_part = GAIN * (sums / 512.0)
        if family == 'in':
            term = new
        elif family == 'out':
            term = mean_part
        else:
            term = jnp.where(lax.broadcasted_iota(jnp.int32, new.shape, 0) < N_QKV, new, mean_part)
        r0 = TAB_ROW[group]
        r1 = r0 + new.shape[0]
        tab[r0:r1, 0:ROWS] = z / new
        tab[r0:r1, ROWS:LANES] = term
        rtab[r0:r1, 0:ROWS] = lax.rsqrt(new)
        if family == 'b':
            row_q_o[...] = new[:N_QKV]
            col_o_o[...] = new[N_QKV:]
        else:
            (row_in_o if family == 'in' else col_out_o)[lo:lo + n, :] = new

    def scalars_start(family):
        e = SLOT[family]
        turned = tab[...].T
        scal[e, 0:1, :] = jnp.sum(turned[:ROWS], axis=0, keepdims=True)
        scal[e, 1:2, :] = jnp.sum(turned[ROWS:], axis=0, keepdims=True)
        scal_ex(family, 'start')
        if family == 'in':
            rsub[...] = rtab[:, 0:ROWS].T

    def factor(q, s, w, v, family):
        rows = 512.0 if family == 'in' else float(full[family])
        size = 512.0 * full[family]
        m = (s if family == 'in' else BETA_TWO * v + s) / rows
        return jnp.sqrt(m) * (LR_BASE * jnp.maximum(1e-3, jnp.sqrt(w / size))) / jnp.maximum(1.0, jnp.sqrt(m * q / size))

    def after_scalars(family):
        e = SLOT[family]
        scal_ex(family, 'recv')
        tot = total(got_s.at[e], n_data)
        scale = factor(tot[0:1], tot[1:2], w_all[0:1, :], w_all[1:2, :], family)
        if family == 'b':
            turn[...] = jnp.broadcast_to(scale, (LANES, LANES)).T
            rtab[ROW_B:ROW_B + 72, 0:ROWS] = rtab[ROW_B:ROW_B + 72, 0:ROWS] * turn[ROW_B:ROW_B + 72, 0:ROWS]
            for ref, b0 in ((w_q, 0), (w_o, N_QKV)):
                def body(b, carry, ref=ref, b0=b0):
                    ref[b] = ref[b] - ht[b0 + b] * rtab[pl.ds(ROW_B + b0 + b, 1), 0:ROWS]
                    return carry
                lax.fori_loop(0, ref.shape[0], body, 0, unroll=6)
        else:
            fac = rsub[...] * scale

            def body(b, carry):
                f = jnp.sum(jnp.where(lane_iota == ROW_IN + b, fac, 0.0), axis=1, keepdims=True)
                w_in[b] = w_in[b] - grad[FIRST_IN + b] * f
                return carry
            lax.fori_loop(0, N_IN, body, 0, unroll=4)

    def prepare_out():
        fac = rtab[:, 0:ROWS].T

        def body(b, carry):
            f = jnp.sum(jnp.where(lane_iota == ROW_OUT + b, fac, 0.0), axis=1, keepdims=True)
            grad[FIRST_OUT + b] = grad[FIRST_OUT + b] * f
            return carry
        lax.fori_loop(0, N_OUT, body, 0, unroll=4)

    def apply_out(group):
        _, g0, n = GROUPS[group]
        lo, r0, e = g0 - FIRST_OUT, TAB_ROW[group], SLOT[group]
        scal_ex(group, 'recv')
        tot = total(got_s.at[e], n_data)
        scale = factor(tot[0:1], tot[1:2], w_all[0:1, :], w_all[1:2, :], 'out')
        krow[...] = jnp.broadcast_to(scale, (LANES, LANES)).T
        for b in range(lo, lo + n):
            w_out[b] = w_out[b] - grad[FIRST_OUT + b] * krow[r0 + b - lo:r0 + b - lo + 1, :]

    def last_lanes():
        _, g0, n = GROUPS['out_b']
        lo = g0 - FIRST_OUT
        lane_ex('out_b', 'recv')
        new = BETA_TWO * row_out[lo:lo + n, :] + GAIN * (total(dat_o, n_data) / 512.0)
        r = lax.rsqrt(new)
        first, second = grad[g0] * r[0:1], grad[g0 + 1] * r[1:2]
        mod_o[1:2, :] = row_sums(first * first, second * second)
        model_ex('out_b', 'start')
        grad[g0], grad[g0 + 1] = first, second
        row_out_o[lo:lo + n, :] = new
        pair_mom[0:1, 0:ROWS] = col_out[lo:lo + 1, :]
        pair_mom[0:1, ROWS:LANES] = col_out[lo + 1:lo + 2, :]

    def last_model():
        lo, r0 = GROUPS['out_b'][1] - FIRST_OUT, TAB_ROW['out_b']
        model_ex('out_b', 'recv')
        sums_z = total(got_o, n_model)
        sums, z = sums_z[0:1], sums_z[1:2]
        new = BETA_TWO * pair_mom[...] + GAIN * (sums / full['out'])
        raw_o[0:1, :] = z / new
        raw_o[1:2, :] = GAIN * (sums / 512.0)
        scal_ex('out_b', 'start')
        root = lax.rsqrt(new)
        for i in range(N_OUT_B):
            own_lanes = slice(ROWS * i, ROWS * i + ROWS)
            rtab[r0 + i:r0 + i + 1, 0:ROWS] = root[:, own_lanes]
            col_out_o[lo + i:lo + i + 1, :] = new[:, own_lanes]

    def last_apply():
        _, g0, n = GROUPS['out_b']
        lo, r0 = g0 - FIRST_OUT, TAB_ROW['out_b']
        mine = lax.div(lax.broadcasted_iota(jnp.int32, (n, LANES), 1), ROWS) == lax.broadcasted_iota(jnp.int32, (n, LANES), 0)
        scal_ex('out_b', 'recv')
        tot = total(graw_o, n_data)
        q = jnp.sum(jnp.where(mine, tot[0:1], 0.0), axis=1, keepdims=True)
        s = jnp.sum(jnp.where(mine, tot[1:2], 0.0), axis=1, keepdims=True)
        scale = factor(q, s, wcol[r0:r0 + n, 0:1], wcol[r0:r0 + n, 1:2], 'out')
        for i in range(n):
            w_out[lo + i] = w_out[lo + i] - grad[g0 + i] * scale[i:i + 1]

    def sent_early():
        for i, ref in enumerate((peer, opp_in, left_in, right_in)):
            remote(ref, ref, snd.at[i], rcv.at[0, 0], 'data', partner).wait_send()
        gather(mod_w, got_w, m_sems, SLOT['w'], 'model', 'send')
        for group in near:
            pair_ex(group).wait_send()
            back_ex(group).wait_send()
        for group in GROUPS:
            lane_ex(group, 'send')
        model_ex('b', 'send')
        scal_ex('w', 'send')
        scal_ex('b', 'send')

    def sent_mid():
        for group in ('in', 'out_a', 'out_b'):
            model_ex(group, 'send')
        scal_ex('in', 'send')
        scal_ex('out_a', 'send')

    def sent_late():
        scal_ex('out_b', 'send')

    acc_t[...] = jnp.zeros_like(acc_t)
    tab[...] = jnp.zeros_like(tab)
    rtab[...] = jnp.zeros_like(rtab)

    convert(0)
    for cp in small + w_loads:
        cp.start()
    pl.semaphore_wait(barrier, len(neighbours))
    first_pairs()
    greet(meet.at[0])
    last = N_CH - 1 + LAG_FINISH
    steps = {}

    def at(k, do, *args):
        steps.setdefault(k, []).append((do, args))

    def pass_on(i):
        pl.semaphore_wait(meet.at[i], len(neighbours))
        if i < 2:
            greet(meet.at[i + 1])

    at(2, pass_on, 0)
    at(3, pass_on, 1)
    at(4, pass_on, 2)
    at(4, weights_start)
    at(6, weights_next)
    at(8, weights_done)
    k_b, k_in, k_a = (LAST_CHUNK[g] + LAG_FINISH for g in ('b', 'in', 'out_a'))
    at(k_b + 1, lane_pair, 'b')
    at(k_b + 3, lane_back, 'b')
    at(k_b + 4, after_lanes, 'b')
    at(k_b + 6, after_model, 'b')
    at(k_b + 6, scalars_start, 'b')
    at(k_in + 1, lane_pair, 'in')
    at(k_in + 3, lane_back, 'in')
    tail = ((after_lanes, 'in'), (after_lanes, 'out_a'), (last_lanes,), (after_scalars, 'b'), (sent_early,), (after_model, 'in'),
            (scalars_start, 'in'), (after_model, 'out_a'), (scalars_start, 'out_a'), (last_model,), (prepare_out,), (sent_mid,), (after_scalars, 'in'),
            (apply_out, 'out_a'), (last_apply,), (sent_late,))
    for k in range(1 - AHEAD, last + 1):
        if 0 <= k < N_CH:
            opposite(k)
        if k + AHEAD < N_CH:
            convert(k + AHEAD)
            transfer(D2D, k + AHEAD).start()
        for ch in range(N_CH):
            if k == ch + (LAG_MERGE if ch < N_CH - 1 else 1):
                merge(ch)
        for do, args in steps.get(k, ()):
            do(*args)
        if 0 <= k - LAG_FINISH < N_CH:
            finish(k - LAG_FINISH)
        for group in GROUPS:
            if k == LAST_CHUNK[group] + LAG_FINISH and group != 'out_b':
                lane_start(group)
    for do, *args in tail:
        do(*args)


def deliver(*refs):
    srcs, dsts, sem = refs[:12], refs[12:24], refs[24]
    copies = [pltpu.make_async_copy(src, dst, sem.at[i]) for i, (src, dst) in enumerate(zip(srcs, dsts))]
    for cp in copies:
        cp.start()
    for cp in copies:
        cp.wait()


def solution(mesh):
    axis_sizes = dict(mesh.shape)
    n_data, n_model = axis_sizes['data'], axis_sizes['model']
    n_chips = n_data // 2
    rows_data = (P('data', None, None, 'model'), P(None, 'data', 'model'), P(None, 'data'), P(None, 'model'))
    rows_model = (P('data', None, 'model', None), P(None, 'model', 'data'), P(None, 'model'), P(None, 'data'))

    def vmem(*dims):
        return pltpu.VMEM(dims, F32)

    small = (vmem(24, ROWS), vmem(24, LANES), vmem(12, LANES), vmem(12, ROWS), vmem(54, ROWS), vmem(WIDE, 54), vmem(18, WIDE), vmem(18, ROWS))
    results = (vmem(24, ROWS, LANES), vmem(12, ROWS, LANES), vmem(54, WIDE, ROWS), vmem(18, WIDE, ROWS), *small)
    scratch = [
        *small, vmem(N_B, LANES), vmem(LANES, LANES),
        pltpu.VMEM((24, 512, LANES), jnp.bfloat16), pltpu.VMEM((12, LANES, 512), jnp.bfloat16),
        pltpu.VMEM((72, WIDE, 512), jnp.bfloat16),
        vmem(2, n_chips, N_SUP, ROWS, LANES), vmem(n_chips, N_SUP, ROWS, LANES),
        vmem(N_SUP, ROWS, LANES), vmem(N_SUP, ROWS, LANES), vmem(N_SUP, ROWS, LANES), vmem(N_SUP, ROWS, LANES),
        vmem(2, LANES), vmem(72, WIDE, ROWS),
        vmem(2, 9, LANES), vmem(2, 12, LANES), vmem(N_OUT_A, LANES), vmem(N_OUT_B, LANES),
        *(vmem(2, n, LANES) for n in (9, 12, 9, 12, 9, 12)),
        vmem(ROWS, LANES), vmem(2, ROWS, LANES), vmem(N_B, 4, LANES),
        vmem(LANES, LANES), vmem(LANES, LANES), vmem(ROWS, LANES), vmem(LANES, LANES), vmem(LANES, LANES),
        vmem(72, LANES), vmem(24, LANES), vmem(N_OUT_A, LANES), vmem(N_OUT_B, LANES), vmem(2, LANES), vmem(5, 2, LANES),
        vmem(n_chips, 9, LANES), vmem(n_chips, 12, LANES), vmem(n_data, N_OUT_A, LANES), vmem(n_data, N_OUT_B, LANES),
        vmem(n_model, 72, LANES), vmem(n_model, 24, LANES), vmem(n_model, N_OUT_A, LANES), vmem(n_model, N_OUT_B, LANES),
        vmem(n_model, 2, LANES), vmem(5, n_data, 2, LANES),
        vmem(1, LANES), vmem(N_OUT_B, LANES), vmem(n_data, N_OUT_B, LANES), vmem(LANES, LANES), vmem(LANES, LANES),
        pltpu.SemaphoreType.DMA((5,)), pltpu.SemaphoreType.DMA((4,)), pltpu.SemaphoreType.DMA((8,)), pltpu.SemaphoreType.DMA((1,)),
        pltpu.SemaphoreType.REGULAR((3,)),
        pltpu.SemaphoreType.DMA((4,)), pltpu.SemaphoreType.DMA((3, N_CH)),
        *(pltpu.SemaphoreType.DMA((n,)) for n in (2, 2, 2, 2, 4, 4, 5, 5, 5, 5)),
    ]
    hbm, in_vmem = pl.BlockSpec(memory_space=pltpu.HBM), pl.BlockSpec(memory_space=pltpu.VMEM)

    def step_all(grad_in, w_in, row_in, col_in, grad_out, w_out, row_out, col_out,
                 grad_qkv, w_qkv, row_qkv, col_qkv, grad_o, w_o, row_o, col_o):
        kept = pl.pallas_call(
            functools.partial(kernel, n_data, n_model),
            name='adafactor_step',
            out_shape=results,
            in_specs=[hbm] * 16,
            out_specs=[in_vmem] * 12,
            scratch_shapes=scratch,
            compiler_params=pltpu.CompilerParams(collective_id=0, has_side_effects=True, vmem_limit_bytes=VMEM_LIMIT),
        )(grad_in[0], grad_out[0], grad_qkv[0].transpose(0, 2, 1), grad_o[0],
          w_in, w_out.transpose(0, 2, 1), w_qkv.transpose(0, 2, 1), w_o,
          row_in, col_in, row_out, col_out, row_qkv, col_qkv.T, row_o, col_o)
        (w_in_new, w_out_new, w_qkv_new, w_o_new, row_in_new, col_in_new, row_out_new, col_out_new,
         row_qkv_new, col_qkv_new, row_o_new, col_o_new) = pl.pallas_call(
            deliver,
            name='deliver',
            out_shape=[jax.ShapeDtypeStruct(r.shape, F32) for r in results],
            in_specs=[in_vmem] * 12,
            out_specs=[hbm] * 12,
            scratch_shapes=[pltpu.SemaphoreType.DMA((12,))],
            compiler_params=pltpu.CompilerParams(vmem_limit_bytes=10 ** 6),
        )(*(pltpu.with_memory_space_constraint(a, pltpu.VMEM) for a in kept))
        return (w_in_new, row_in_new, col_in_new, w_out_new.transpose(0, 2, 1), row_out_new, col_out_new,
                w_qkv_new.transpose(0, 2, 1), row_qkv_new, col_qkv_new.T, w_o_new, row_o_new, col_o_new)

    in_specs = rows_data + rows_model + rows_data + rows_model
    out_specs = rows_data[1:] + rows_model[1:] + rows_data[1:] + rows_model[1:]
    return jax.shard_map(step_all, mesh=mesh, in_specs=in_specs, out_specs=out_specs, check_vma=False)
```

```python
import functools

import jax
import jax.numpy as jnp
from jax import lax
from jax.experimental import pallas as pl
from jax.experimental.pallas import tpu as pltpu
from jax.sharding import PartitionSpec as P

OPT_STEP = 4
EPS_SQ = 1e-30
BETA_TWO = 1.0 - OPT_STEP ** -0.8
GAIN = 1.0 - BETA_TWO
LR_BASE = min(1e-2, OPT_STEP ** -0.5)
F32 = jnp.float32
LANES, ROWS, WIDE = 128, 64, 32
VMEM_LIMIT = 60 * 10 ** 6

N_IN, N_B, N_OUT = 24, 18, 12
N_SUP = N_IN + N_B + N_OUT
FIRST_B, FIRST_IN, FIRST_OUT = 0, N_B, N_B + N_IN
N_QKV, N_O = 54, 18
N_MAT = N_QKV + N_O
N_OUT_B = 2
N_OUT_A = N_OUT - N_OUT_B
ROW_IN, ROW_OUT, ROW_B = 0, N_IN, 40
GROUPS = {'b': ('b', FIRST_B, N_B), 'in': ('in', FIRST_IN, N_IN), 'out_a': ('out', FIRST_OUT, N_OUT_A), 'out_b': ('out', FIRST_OUT + N_OUT_A, N_OUT_B)}
SIZES = (('b', (2, 4, 6, 6)), ('in', (6, 6, 6, 6)), ('out_a', (4, 4, 2)), ('out_b', (2,)))


def cut():
    chunks, at = [], 0
    for group, sizes in SIZES:
        for n in sizes:
            chunks.append((group, at, n))
            at += n
    return tuple(chunks)


CHUNKS = cut()
N_CH = len(CHUNKS)
LAST_CHUNK = {g: max(i for i, c in enumerate(CHUNKS) if c[0] == g) for g in GROUPS}
D2D, OPP_A, OPP_B, OWN_R, OWN_L, MRG_R, MRG_L = range(7)
SEND = (0, 1, 1, 2, 3, 2, 3)
OPP, LAST = 1, 2
RECV = (D2D, OPP, OPP, LAST, LAST, LAST, LAST)
SLOT = {'b': 0, 'in': 1, 'out_a': 2, 'out_b': 3, 'w': 4}
LANE_ROW = {'b': 0, 'in': N_IN, 'out_a': 48, 'out_b': 48 + N_OUT_A}
TAB_ROW = {'b': ROW_B, 'in': ROW_IN, 'out_a': ROW_OUT, 'out_b': ROW_OUT + N_OUT_A}
AHEAD, EARLY_OWN, LAG_MERGE, LAG_FINISH = 2, 3, 2, 3


def loop(n, body, unroll):
    lax.fori_loop(0, n, body, 0, unroll=unroll)


def kernel(n_data, n_model, gin_h, gout_h, gq_h, go_h, win_h, wout_h, wq_h, wo_h,
           row_in_h, col_in_h, row_out_h, col_out_h, row_q_h, col_q_h, row_o_h, col_o_h,
           w_in, w_out, w_q, w_o, row_in_o, col_in_o, row_out_o, col_out_o, row_q_o, col_q_o, row_o_o, col_o_o,
           row_in, col_in, row_out, col_out, row_q, col_q, row_o, col_o, lane_b, turn,
           gin, gout, gb, part, peer, opp_in, left_in, right_in, grad, w_all, ht,
           sum_b, sum_in, sum_a, sum_o, near_b, near_in, both_b, both_in, full_b, full_in, rlane, acc_t, comp_b, tab, rtab, rsub, wtab, vtab,
           mod_b, mod_in, mod_a, mod_o, mod_w, scal, dat_b, dat_in, dat_a, dat_o, got_b, got_in, got_a, got_o, got_w, got_s,
           pair_mom, raw_o, graw_o, wcol, krow,
           load_sem, w_sem, small_sem, first_sem, meet, snd, rcv, psnd, prcv, bsnd, brcv, dsnd, drcv, msnd, mrcv, ssnd, srcv):
    me = lax.axis_index('data')
    mod = lax.axis_index('model')
    n_chips = n_data // 2
    x, c = lax.div(me, 2), lax.rem(me, 2)
    xr, xl, xo = lax.rem(x + 1, n_chips), lax.rem(x + 3, n_chips), lax.rem(x + 2, n_chips)
    partner, right, left = 2 * x + 1 - c, 2 * xr + c, 2 * xl + c
    full = {'in': n_model * LANES, 'out': n_model * LANES, 'b': n_model * WIDE}
    lane_sum = {'b': sum_b, 'in': sum_in, 'out_a': sum_a, 'out_b': sum_o}
    near = {'b': near_b, 'in': near_in}
    both = {'b': both_b, 'in': both_in}
    whole = {'b': full_b, 'in': full_in}
    dat_got = {'b': dat_b, 'in': dat_in, 'out_a': dat_a, 'out_b': dat_o}
    mod_blk = {'b': mod_b, 'in': mod_in, 'out_a': mod_a, 'out_b': mod_o}
    mod_got = {'b': got_b, 'in': got_in, 'out_a': got_a, 'out_b': got_o}

    loads = [pltpu.make_async_copy(gq_h.at[pl.ds(0, 8)], gb.at[pl.ds(0, 8)], load_sem.at[0]),
             pltpu.make_async_copy(gq_h.at[pl.ds(8, 46)], gb.at[pl.ds(8, 46)], load_sem.at[1]),
             pltpu.make_async_copy(go_h, gb.at[pl.ds(N_QKV, N_O)], load_sem.at[2]),
             pltpu.make_async_copy(gin_h, gin, load_sem.at[3]),
             pltpu.make_async_copy(gout_h, gout, load_sem.at[4])]
    w_loads = [pltpu.make_async_copy(win_h, w_in, w_sem.at[0]),
               pltpu.make_async_copy(wout_h, w_out, w_sem.at[1]),
               pltpu.make_async_copy(wq_h, w_q, w_sem.at[2]),
               pltpu.make_async_copy(wo_h, w_o, w_sem.at[3])]
    small = [pltpu.make_async_copy(src, dst, small_sem.at[i]) for i, (src, dst) in enumerate((
        (row_in_h, row_in), (col_in_h, col_in), (row_out_h, row_out), (col_out_h, col_out),
        (row_q_h, row_q), (col_q_h, col_q), (row_o_h, row_o), (col_o_h, col_o)))]
    loads[0].start()

    barrier = pltpu.get_barrier_semaphore()

    def others(axis):
        side = 4 if axis == 'model' else 2
        n, rank = (n_model, mod) if axis == 'model' else (n_data, me)
        high, low, rows = lax.div(rank, side), lax.rem(rank, side), n // side

        def hops(d):
            up, over = d // side, d % side
            return min(up, rows - up) * (side - 1) + min(over, side - over)

        for d in sorted(range(1, n), key=lambda d: -hops(d)):
            if axis != 'chip' or d % side == 0:
                yield lax.rem(high + d // side, rows) * side + lax.rem(low + d % side, side)

    side = 4
    z, y = lax.div(mod, side), lax.rem(mod, side)
    neighbours = [('data', who) for who in (partner, right, left)]
    for step in (1, side - 1):
        neighbours.append(('model', side * z + lax.rem(y + step, side)))
        neighbours.append(('model', side * lax.rem(z + step, n_model // side) + y))

    def greet(sem):
        for axis, who in neighbours:
            pl.semaphore_signal(sem, inc=1, device_id={axis: who}, device_id_type=pl.DeviceIdType.MESH)

    greet(barrier)
    for cp in loads[1:]:
        cp.start()

    def remote(src, dst, ssem, rsem, axis, who):
        return pltpu.make_async_remote_copy(src_ref=src, dst_ref=dst, send_sem=ssem, recv_sem=rsem,
                                            device_id={axis: who}, device_id_type=pl.DeviceIdType.MESH)

    def transfer(kind, ch):
        _, b0, n = CHUNKS[ch]
        n_a = n // 2
        every, half_a, half_b = pl.ds(b0, n), pl.ds(b0, n_a), pl.ds(b0 + n_a, n - n_a)
        src, dst, who = {
            D2D: lambda: (part.at[1 - c, :, every], peer.at[:, every], partner),
            OPP_A: lambda: (part.at[c, xo, half_a], opp_in.at[half_a], right),
            OPP_B: lambda: (part.at[c, xo, half_b], opp_in.at[half_b], left),
            OWN_R: lambda: (part.at[c, xr, half_b], left_in.at[half_b], right),
            OWN_L: lambda: (part.at[c, xl, half_a], right_in.at[half_a], left),
            MRG_R: lambda: (part.at[c, xr, half_a], left_in.at[half_a], right),
            MRG_L: lambda: (part.at[c, xl, half_b], right_in.at[half_b], left),
        }[kind]()
        return remote(src, dst, snd.at[SEND[kind]], rcv.at[RECV[kind], ch], 'data', who)

    def convert(ch):
        group, b0, n = CHUNKS[ch]
        family = GROUPS[group][0]
        if ch == 0:
            loads[0].wait()
        elif ch == 1:
            loads[1].wait()
            loads[2].wait()
        elif b0 == FIRST_IN:
            loads[3].wait()
        elif b0 == FIRST_OUT:
            loads[4].wait()

        def body(i, carry):
            b = b0 + i
            for t in range(n_chips):
                if family == 'in':
                    tile = gin[b - FIRST_IN, pl.ds(LANES * t, LANES), :].astype(F32)
                elif family == 'out':
                    tile = gout[b - FIRST_OUT, :, pl.ds(LANES * t, LANES)].astype(F32).T
                else:
                    four = gb[pl.ds(4 * (b - FIRST_B), 4), :, pl.ds(LANES * t, LANES)].astype(F32)
                    tile = four.reshape(LANES, LANES).T
                part[0, t, b] = tile[:ROWS]
                part[1, t, b] = tile[ROWS:]
            return carry

        lax.fori_loop(0, n, body, 0)

    def first_pair(dest, sem):
        every = pl.ds(0, CHUNKS[0][2])
        return remote(part.at[1 - c, dest, every], peer.at[dest, every], snd.at[0], sem, 'data', partner)

    def first_pairs():
        first_pair(xo, first_sem.at[0]).start()
        for dest in (xr, xl, x):
            first_pair(dest, rcv.at[D2D, 0]).start()

    def add_peer(ch, dest):
        _, b0, n = CHUNKS[ch]

        def body(i, carry):
            b = b0 + i
            part[c, dest, b] = part[c, dest, b] + peer[dest, b]
            return carry
        loop(n, body, 2)

    def opposite(ch):
        if ch == 0:
            first_pair(xo, first_sem.at[0]).wait_recv()
        else:
            transfer(D2D, ch).wait_recv()
        add_peer(ch, xo)
        transfer(OPP_A, ch).start()
        transfer(OPP_B, ch).start()
        if ch == 0:
            rest = peer.at[pl.ds(0, n_chips - 1), pl.ds(0, CHUNKS[0][2])]
            remote(rest, rest, snd.at[0], rcv.at[D2D, 0], 'data', partner).wait_recv()
        add_peer(ch, xr)
        add_peer(ch, xl)
        if ch < EARLY_OWN:
            own(ch)
        add_peer(ch, x)

    def own(ch):
        transfer(OWN_R, ch).start()
        transfer(OWN_L, ch).start()

    def merge(ch):
        _, b0, n = CHUNKS[ch]
        n_a = n // 2

        def add(dest, lo, hi):
            def body(b, carry):
                part[c, dest, b] = part[c, dest, b] + opp_in[b]
                return carry
            lax.fori_loop(lo, hi, body, 0)

        every = opp_in.at[pl.ds(b0, n)]
        remote(every, every, snd.at[1], rcv.at[OPP, ch], 'data', left).wait_recv()
        add(xr, b0, b0 + n_a)
        transfer(MRG_R, ch).start()
        add(xl, b0 + n_a, b0 + n)
        transfer(MRG_L, ch).start()
        if ch >= EARLY_OWN:
            own(ch)

    lane_iota = lax.broadcasted_iota(jnp.int32, (ROWS, LANES), 1)

    def row_sums(first, second):
        return jnp.sum(jnp.concatenate([first, second], axis=0).T, axis=0, keepdims=True)

    def finish(ch):
        group, b0, n = CHUNKS[ch]
        family, g0, _ = GROUPS[group]
        every = pl.ds(b0, n)
        two = peer.at[pl.ds(0, 2), every]
        remote(two, two, snd.at[2], rcv.at[LAST, ch], 'data', right).wait_recv()

        def block(b):
            g = (part[c, x, b] + left_in[b] + right_in[b]) * (1.0 / n_data)
            grad[b] = g
            sq = g * g + EPS_SQ
            sums = jnp.sum(sq, axis=0, keepdims=True)
            if group in near:
                half = lane_sum[group].shape[1]
                lane_sum[group][lax.div(b - g0, half), pl.ds(lax.rem(b - g0, half), 1), :] = sums
            else:
                lane_sum[group][pl.ds(b - g0, 1), :] = sums
            return g, sq

        if family == 'b':
            def body(i, carry):
                b = b0 + i
                g, _ = block(b)
                gt = g.T
                st = (gt * gt + EPS_SQ).reshape(4, WIDE, ROWS)
                comp_b[pl.ds(b - FIRST_B, 1), :, :ROWS] = jnp.sum(st, axis=1)[None]
                return carry
            loop(n, body, 2)
        elif group == 'out_b':
            first, second = (block(b0 + i)[1] for i in range(N_OUT_B))
            lane_start(group)
            mod_o[:1, :] = row_sums(first, second)
        else:
            which = 0 if family == 'in' else 1

            def body(i, acc):
                b = b0 + i
                _, sq = block(b)
                return jnp.where(lane_iota == b - (FIRST_IN if family == 'in' else FIRST_OUT), jnp.sum(sq, axis=1, keepdims=True), acc)
            acc_t[which] = lax.fori_loop(0, n, body, acc_t[which], unroll=2)

    def gather(src, dst, sems, slot, axis, op):
        send, recv = sems[0].at[slot], sems[1].at[slot]
        rank, n = {'data': (me, n_data), 'model': (mod, n_model), 'chip': (x, n_chips)}[axis]
        mesh_axis = 'model' if axis == 'model' else 'data'
        if op == 'start':
            dst[rank] = src[...]
            for who in others(axis):
                remote(src, dst.at[rank], send, recv, mesh_axis, who).start()
            return
        rest = dst.at[pl.ds(0, n - 1)]
        done = remote(rest, rest, send, recv, mesh_axis, partner if mesh_axis == 'data' else mod)
        if op == 'recv':
            done.wait_recv()
        else:
            done.wait_send()

    def total(dst, n):
        acc = dst[0]
        for r in range(1, n):
            acc = acc + dst[r]
        return acc

    d_sems, m_sems, s_sems = (dsnd, drcv), (msnd, mrcv), (ssnd, srcv)

    def pair_ex(group):
        i = SLOT[group]
        return remote(lane_sum[group], near[group], psnd.at[i], prcv.at[i], 'data', partner)

    def lane_ex(group, op):
        pairs = group in near
        gather(both[group].at[c] if pairs else lane_sum[group], dat_got[group], d_sems, SLOT[group], 'chip' if pairs else 'data', op)

    def back_ex(group):
        i = SLOT[group]
        return remote(whole[group].at[c], whole[group].at[c], bsnd.at[i], brcv.at[i], 'data', partner)

    def lane_back(group):
        lane_ex(group, 'recv')
        whole[group][c] = total(dat_got[group], n_chips)
        back_ex(group).start()

    def lane_start(group):
        if group in near:
            pair_ex(group).start()
        else:
            lane_ex(group, 'start')

    def lane_pair(group):
        pair_ex(group).wait_recv()
        both[group][...] = lane_sum[group][...] + near[group][...]
        lane_ex(group, 'start')

    def model_ex(group, op):
        gather(mod_blk[group], mod_got[group], m_sems, SLOT[group], 'model', op)

    def scal_ex(name, op):
        i = SLOT[name]
        src, dst = (raw_o, graw_o) if name == 'out_b' else (scal.at[i], got_s.at[i])
        gather(src, dst, s_sems, i, 'data', op)

    def weights_start():
        for cp in w_loads + small:
            cp.wait()
        turn[...] = jnp.zeros_like(turn)
        turn[:WIDE, :N_QKV] = col_q[...]
        turn[...] = turn[...].T
        turn[N_QKV:N_QKV + N_O, :WIDE] = row_o[...]
        row = turn[pl.ds(0, N_B, stride=4), :]
        for q in range(1, 4):
            row = row + pltpu.roll(turn[pl.ds(q, N_B, stride=4), :], WIDE * q, 1)
        lane_b[...] = row
        wtab[...] = jnp.zeros_like(wtab)
        vtab[...] = jnp.zeros_like(vtab)

        def squares(ref, row, width):
            def body(b, carry):
                w = ref[b]
                wtab[pl.ds(row + b, 1), 0:width] = jnp.sum(w * w, axis=0, keepdims=True)
                return carry
            loop(ref.shape[0], body, 6)

        squares(w_in, ROW_IN, LANES)
        squares(w_out, ROW_OUT, LANES)
        squares(w_q, ROW_B, ROWS)
        squares(w_o, ROW_B + N_QKV, ROWS)
        vtab[ROW_OUT:ROW_OUT + N_OUT, :] = row_out[...]
        vtab[ROW_B + N_QKV:ROW_B + N_MAT, :WIDE] = row_o[...]
        mod_w[:1, :] = jnp.sum(wtab[...].T, axis=0, keepdims=True)
        mod_w[1:2, :] = jnp.sum(vtab[...].T, axis=0, keepdims=True) / n_data
        gather(mod_w, got_w, m_sems, SLOT['w'], 'model', 'start')

    def weights_next():
        gather(mod_w, got_w, m_sems, SLOT['w'], 'model', 'recv')
        scal[SLOT['w']] = total(got_w, n_model)
        scal_ex('w', 'start')

    def weights_done():
        scal_ex('w', 'recv')
        w_all[...] = total(got_s.at[SLOT['w']], n_data)
        turn[:2, :] = w_all[...]
        wcol[...] = turn[...].T

    def after_lanes(group):
        family, g0, n = GROUPS[group]
        r0 = LANE_ROW[group]
        if group in near:
            back_ex(group).wait_recv()
            sums = jnp.concatenate([whole[group][0], whole[group][1]], axis=0)
        else:
            lane_ex(group, 'recv')
            sums = total(dat_got[group], n_data)
        lo = g0 - (FIRST_OUT if family == 'out' else g0)
        if family == 'b':
            mom = lane_b[...]
        else:
            mom = (col_in if family == 'in' else row_out)[lo:lo + n, :]
        new = BETA_TWO * mom + GAIN * (sums / 512.0)
        rlane[r0:r0 + n, :] = lax.rsqrt(new)
        if family == 'b':
            def body(s, carry):
                h = grad[FIRST_B + s] * rlane[pl.ds(r0 + s, 1), :]
                t = h.T.reshape(4, WIDE, ROWS)
                ht[pl.ds(4 * s, 4)] = t
                comp_b[pl.ds(s, 1), :, ROWS:LANES] = jnp.sum(t * t, axis=1)[None]
                return carry
            loop(n, body, 3)
            mod_b[...] = comp_b[...].reshape(4 * N_B, LANES)
        else:
            def body(b, acc):
                h = grad[g0 + b] * rlane[pl.ds(r0 + b, 1), :]
                grad[g0 + b] = h
                return jnp.where(lane_iota == lo + b, jnp.sum(h * h, axis=1, keepdims=True), acc)
            acc_z = lax.fori_loop(0, n, body, jnp.zeros((ROWS, LANES), F32), unroll=4)
            turned = jnp.concatenate([acc_t[0 if family == 'in' else 1], acc_z], axis=0).T
            mod_blk[group][...] = turned[lo:lo + n]
        model_ex(group, 'start')
        if family == 'b':
            turn[...] = jnp.zeros_like(turn)
            for q in range(4):
                turn[pl.ds(q, N_B, stride=4), :] = pltpu.roll(new, (LANES - WIDE * q) % LANES, 1)
            row_o_o[...] = turn[N_QKV:N_QKV + N_O, :WIDE]
            turn[...] = turn[...].T
            col_q_o[...] = turn[:WIDE, :N_QKV]
        else:
            (col_in_o if family == 'in' else row_out_o)[lo:lo + n, :] = new

    def after_model(group):
        family, g0, n = GROUPS[group]
        lo = g0 - (FIRST_OUT if family == 'out' else g0)
        model_ex(group, 'recv')
        sums_z = total(mod_got[group], n_model)
        sums, z = sums_z[:, :ROWS], sums_z[:, ROWS:LANES]
        if family == 'b':
            mom = jnp.concatenate([row_q[...], col_o[...]], axis=0)
        else:
            mom = (row_in if family == 'in' else col_out)[lo:lo + n, :]
        new = BETA_TWO * mom + GAIN * (sums / full[family])
        mean_part = GAIN * (sums / 512.0)
        if family == 'in':
            term = new
        elif family == 'out':
            term = mean_part
        else:
            term = jnp.where(lax.broadcasted_iota(jnp.int32, new.shape, 0) < N_QKV, new, mean_part)
        r0 = TAB_ROW[group]
        r1 = r0 + new.shape[0]
        tab[r0:r1, :ROWS] = z / new
        tab[r0:r1, ROWS:LANES] = term
        rtab[r0:r1, :ROWS] = lax.rsqrt(new)
        if family == 'b':
            row_q_o[...] = new[:N_QKV]
            col_o_o[...] = new[N_QKV:]
        else:
            (row_in_o if family == 'in' else col_out_o)[lo:lo + n, :] = new

    def scalars_start(family):
        e = SLOT[family]
        turned = tab[...].T
        scal[e, :1, :] = jnp.sum(turned[:ROWS], axis=0, keepdims=True)
        scal[e, 1:2, :] = jnp.sum(turned[ROWS:], axis=0, keepdims=True)
        scal_ex(family, 'start')
        if family == 'in':
            rsub[...] = rtab[:, :ROWS].T

    def factor(q, s, w, v, family):
        rows = 512.0 if family == 'in' else float(full[family])
        size = 512.0 * full[family]
        m = (s if family == 'in' else BETA_TWO * v + s) / rows
        return jnp.sqrt(m) * (LR_BASE * jnp.maximum(1e-3, jnp.sqrt(w / size))) / jnp.maximum(1.0, jnp.sqrt(m * q / size))

    def after_scalars(family):
        e = SLOT[family]
        scal_ex(family, 'recv')
        tot = total(got_s.at[e], n_data)
        scale = factor(tot[:1], tot[1:2], w_all[:1, :], w_all[1:2, :], family)
        if family == 'b':
            turn[...] = jnp.broadcast_to(scale, (LANES, LANES)).T
            rtab[ROW_B:ROW_B + N_MAT, :ROWS] = rtab[ROW_B:ROW_B + N_MAT, :ROWS] * turn[ROW_B:ROW_B + N_MAT, :ROWS]
            for ref, b0 in ((w_q, 0), (w_o, N_QKV)):
                def body(b, carry, ref=ref, b0=b0):
                    ref[b] = ref[b] - ht[b0 + b] * rtab[pl.ds(ROW_B + b0 + b, 1), :ROWS]
                    return carry
                loop(ref.shape[0], body, 6)
        else:
            fac = rsub[...] * scale

            def body(b, carry):
                f = jnp.sum(jnp.where(lane_iota == ROW_IN + b, fac, 0.0), axis=1, keepdims=True)
                w_in[b] = w_in[b] - grad[FIRST_IN + b] * f
                return carry
            loop(N_IN, body, 4)

    def prepare_out():
        fac = rtab[:, :ROWS].T

        def body(b, carry):
            f = jnp.sum(jnp.where(lane_iota == ROW_OUT + b, fac, 0.0), axis=1, keepdims=True)
            grad[FIRST_OUT + b] = grad[FIRST_OUT + b] * f
            return carry
        loop(N_OUT, body, 4)

    def apply_out(group):
        _, g0, n = GROUPS[group]
        lo, r0, e = g0 - FIRST_OUT, TAB_ROW[group], SLOT[group]
        scal_ex(group, 'recv')
        tot = total(got_s.at[e], n_data)
        scale = factor(tot[:1], tot[1:2], w_all[:1, :], w_all[1:2, :], 'out')
        krow[...] = jnp.broadcast_to(scale, (LANES, LANES)).T
        for b in range(lo, lo + n):
            w_out[b] = w_out[b] - grad[FIRST_OUT + b] * krow[r0 + b - lo:r0 + b - lo + 1, :]

    def last_lanes():
        _, g0, n = GROUPS['out_b']
        lo = g0 - FIRST_OUT
        lane_ex('out_b', 'recv')
        new = BETA_TWO * row_out[lo:lo + n, :] + GAIN * (total(dat_o, n_data) / 512.0)
        r = lax.rsqrt(new)
        first, second = grad[g0] * r[:1], grad[g0 + 1] * r[1:2]
        mod_o[1:2, :] = row_sums(first * first, second * second)
        model_ex('out_b', 'start')
        grad[g0], grad[g0 + 1] = first, second
        row_out_o[lo:lo + n, :] = new
        pair_mom[:1, :ROWS] = col_out[lo:lo + 1, :]
        pair_mom[:1, ROWS:LANES] = col_out[lo + 1:lo + 2, :]

    def last_model():
        lo, r0 = GROUPS['out_b'][1] - FIRST_OUT, TAB_ROW['out_b']
        model_ex('out_b', 'recv')
        sums_z = total(got_o, n_model)
        sums, z = sums_z[:1], sums_z[1:2]
        new = BETA_TWO * pair_mom[...] + GAIN * (sums / full['out'])
        raw_o[:1, :] = z / new
        raw_o[1:2, :] = GAIN * (sums / 512.0)
        scal_ex('out_b', 'start')
        root = lax.rsqrt(new)
        for i in range(N_OUT_B):
            own_lanes = slice(ROWS * i, ROWS * i + ROWS)
            rtab[r0 + i:r0 + i + 1, :ROWS] = root[:, own_lanes]
            col_out_o[lo + i:lo + i + 1, :] = new[:, own_lanes]

    def last_apply():
        _, g0, n = GROUPS['out_b']
        lo, r0 = g0 - FIRST_OUT, TAB_ROW['out_b']
        mine = lax.div(lax.broadcasted_iota(jnp.int32, (n, LANES), 1), ROWS) == lax.broadcasted_iota(jnp.int32, (n, LANES), 0)
        scal_ex('out_b', 'recv')
        tot = total(graw_o, n_data)
        q = jnp.sum(jnp.where(mine, tot[:1], 0.0), axis=1, keepdims=True)
        s = jnp.sum(jnp.where(mine, tot[1:2], 0.0), axis=1, keepdims=True)
        scale = factor(q, s, wcol[r0:r0 + n, :1], wcol[r0:r0 + n, 1:2], 'out')
        for i in range(n):
            w_out[lo + i] = w_out[lo + i] - grad[g0 + i] * scale[i:i + 1]

    def sent_early():
        for i, ref in enumerate((peer, opp_in, left_in, right_in)):
            remote(ref, ref, snd.at[i], rcv.at[0, 0], 'data', partner).wait_send()
        gather(mod_w, got_w, m_sems, SLOT['w'], 'model', 'send')
        for group in near:
            pair_ex(group).wait_send()
            back_ex(group).wait_send()
        for group in GROUPS:
            lane_ex(group, 'send')
        model_ex('b', 'send')
        scal_ex('w', 'send')
        scal_ex('b', 'send')

    def sent_mid():
        for group in ('in', 'out_a', 'out_b'):
            model_ex(group, 'send')
        scal_ex('in', 'send')
        scal_ex('out_a', 'send')

    def sent_late():
        scal_ex('out_b', 'send')

    acc_t[...] = jnp.zeros_like(acc_t)
    tab[...] = jnp.zeros_like(tab)
    rtab[...] = jnp.zeros_like(rtab)

    convert(0)
    for cp in small + w_loads:
        cp.start()
    pl.semaphore_wait(barrier, len(neighbours))
    first_pairs()
    greet(meet.at[0])
    last = N_CH - 1 + LAG_FINISH
    steps = {}

    def at(k, do, *args):
        steps.setdefault(k, []).append((do, args))

    def pass_on(i):
        pl.semaphore_wait(meet.at[i], len(neighbours))
        if i < 2:
            greet(meet.at[i + 1])

    at(2, pass_on, 0)
    at(3, pass_on, 1)
    at(4, pass_on, 2)
    at(4, weights_start)
    at(6, weights_next)
    at(8, weights_done)
    k_b, k_in, k_a = (LAST_CHUNK[g] + LAG_FINISH for g in ('b', 'in', 'out_a'))
    at(k_b + 1, lane_pair, 'b')
    at(k_b + 3, lane_back, 'b')
    at(k_b + 4, after_lanes, 'b')
    at(k_b + 6, after_model, 'b')
    at(k_b + 6, scalars_start, 'b')
    at(k_in + 1, lane_pair, 'in')
    at(k_in + 3, lane_back, 'in')
    tail = ((after_lanes, 'in'), (after_lanes, 'out_a'), (last_lanes,), (after_scalars, 'b'), (sent_early,), (after_model, 'in'),
            (scalars_start, 'in'), (after_model, 'out_a'), (scalars_start, 'out_a'), (last_model,), (prepare_out,), (sent_mid,), (after_scalars, 'in'),
            (apply_out, 'out_a'), (last_apply,), (sent_late,))
    for k in range(1 - AHEAD, last + 1):
        if 0 <= k < N_CH:
            opposite(k)
        if k + AHEAD < N_CH:
            convert(k + AHEAD)
            transfer(D2D, k + AHEAD).start()
        for ch in range(N_CH):
            if k == ch + (LAG_MERGE if ch < N_CH - 1 else 1):
                merge(ch)
        for do, args in steps.get(k, ()):
            do(*args)
        if 0 <= k - LAG_FINISH < N_CH:
            finish(k - LAG_FINISH)
        for group in GROUPS:
            if k == LAST_CHUNK[group] + LAG_FINISH and group != 'out_b':
                lane_start(group)
    for do, *args in tail:
        do(*args)


def deliver(*refs):
    srcs, dsts, sem = refs[:12], refs[12:N_IN], refs[N_IN]
    copies = [pltpu.make_async_copy(src, dst, sem.at[i]) for i, (src, dst) in enumerate(zip(srcs, dsts))]
    for cp in copies:
        cp.start()
    for cp in copies:
        cp.wait()


def solution(mesh):
    axis_sizes = dict(mesh.shape)
    n_data, n_model = axis_sizes['data'], axis_sizes['model']
    n_chips = n_data // 2
    rows_data = (P('data', None, None, 'model'), P(None, 'data', 'model'), P(None, 'data'), P(None, 'model'))
    rows_model = (P('data', None, 'model', None), P(None, 'model', 'data'), P(None, 'model'), P(None, 'data'))

    def vmem(*dims):
        return pltpu.VMEM(dims, F32)

    small = (vmem(N_IN, ROWS), vmem(N_IN, LANES), vmem(12, LANES), vmem(12, ROWS), vmem(N_QKV, ROWS), vmem(WIDE, N_QKV), vmem(N_O, WIDE), vmem(N_O, ROWS))
    results = (vmem(N_IN, ROWS, LANES), vmem(12, ROWS, LANES), vmem(N_QKV, WIDE, ROWS), vmem(N_O, WIDE, ROWS), *small)
    scratch = [
        *small, vmem(N_B, LANES), vmem(LANES, LANES),
        pltpu.VMEM((N_IN, 512, LANES), jnp.bfloat16), pltpu.VMEM((12, LANES, 512), jnp.bfloat16),
        pltpu.VMEM((N_MAT, WIDE, 512), jnp.bfloat16),
        vmem(2, n_chips, N_SUP, ROWS, LANES), vmem(n_chips, N_SUP, ROWS, LANES),
        vmem(N_SUP, ROWS, LANES), vmem(N_SUP, ROWS, LANES), vmem(N_SUP, ROWS, LANES), vmem(N_SUP, ROWS, LANES),
        vmem(2, LANES), vmem(N_MAT, WIDE, ROWS),
        vmem(2, 9, LANES), vmem(2, 12, LANES), vmem(N_OUT_A, LANES), vmem(N_OUT_B, LANES),
        *(vmem(2, n, LANES) for n in (9, 12, 9, 12, 9, 12)),
        vmem(ROWS, LANES), vmem(2, ROWS, LANES), vmem(N_B, 4, LANES),
        vmem(LANES, LANES), vmem(LANES, LANES), vmem(ROWS, LANES), vmem(LANES, LANES), vmem(LANES, LANES),
        vmem(N_MAT, LANES), vmem(N_IN, LANES), vmem(N_OUT_A, LANES), vmem(N_OUT_B, LANES), vmem(2, LANES), vmem(5, 2, LANES),
        vmem(n_chips, 9, LANES), vmem(n_chips, 12, LANES), vmem(n_data, N_OUT_A, LANES), vmem(n_data, N_OUT_B, LANES),
        vmem(n_model, N_MAT, LANES), vmem(n_model, N_IN, LANES), vmem(n_model, N_OUT_A, LANES), vmem(n_model, N_OUT_B, LANES),
        vmem(n_model, 2, LANES), vmem(5, n_data, 2, LANES),
        vmem(1, LANES), vmem(N_OUT_B, LANES), vmem(n_data, N_OUT_B, LANES), vmem(LANES, LANES), vmem(LANES, LANES),
        pltpu.SemaphoreType.DMA((5,)), pltpu.SemaphoreType.DMA((4,)), pltpu.SemaphoreType.DMA((8,)), pltpu.SemaphoreType.DMA((1,)),
        pltpu.SemaphoreType.REGULAR((3,)),
        pltpu.SemaphoreType.DMA((4,)), pltpu.SemaphoreType.DMA((3, N_CH)),
        *(pltpu.SemaphoreType.DMA((n,)) for n in (2, 2, 2, 2, 4, 4, 5, 5, 5, 5)),
    ]
    hbm, in_vmem = pl.BlockSpec(memory_space=pltpu.HBM), pl.BlockSpec(memory_space=pltpu.VMEM)

    def step_all(grad_in, w_in, row_in, col_in, grad_out, w_out, row_out, col_out,
                 grad_qkv, w_qkv, row_qkv, col_qkv, grad_o, w_o, row_o, col_o):
        kept = pl.pallas_call(
            functools.partial(kernel, n_data, n_model),
            name='adafactor_step',
            out_shape=results,
            in_specs=[hbm] * 16,
            out_specs=[in_vmem] * 12,
            scratch_shapes=scratch,
            compiler_params=pltpu.CompilerParams(collective_id=0, has_side_effects=True, vmem_limit_bytes=VMEM_LIMIT),
        )(grad_in[0], grad_out[0], grad_qkv[0].transpose(0, 2, 1), grad_o[0],
          w_in, w_out.transpose(0, 2, 1), w_qkv.transpose(0, 2, 1), w_o,
          row_in, col_in, row_out, col_out, row_qkv, col_qkv.T, row_o, col_o)
        (w_in_new, w_out_new, w_qkv_new, w_o_new, row_in_new, col_in_new, row_out_new, col_out_new,
         row_qkv_new, col_qkv_new, row_o_new, col_o_new) = pl.pallas_call(
            deliver,
            name='deliver',
            out_shape=[jax.ShapeDtypeStruct(r.shape, F32) for r in results],
            in_specs=[in_vmem] * 12,
            out_specs=[hbm] * 12,
            scratch_shapes=[pltpu.SemaphoreType.DMA((12,))],
            compiler_params=pltpu.CompilerParams(vmem_limit_bytes=10 ** 6),
        )(*(pltpu.with_memory_space_constraint(a, pltpu.VMEM) for a in kept))
        return (w_in_new, row_in_new, col_in_new, w_out_new.transpose(0, 2, 1), row_out_new, col_out_new,
                w_qkv_new.transpose(0, 2, 1), row_qkv_new, col_qkv_new.T, w_o_new, row_o_new, col_o_new)

    in_specs = rows_data + rows_model + rows_data + rows_model
    out_specs = rows_data[1:] + rows_model[1:] + rows_data[1:] + rows_model[1:]
    return jax.shard_map(step_all, mesh=mesh, in_specs=in_specs, out_specs=out_specs, check_vma=False)
```

```python
import functools

import jax
import jax.numpy as jnp
from jax import lax
from jax.experimental import pallas as pl
from jax.experimental.pallas import tpu as pltpu
from jax.sharding import PartitionSpec as P

OPT_STEP = 4
EPS_SQ = 1e-30
BETA_TWO = 1.0 - OPT_STEP ** -0.8
GAIN = 1.0 - BETA_TWO
LR_BASE = min(1e-2, OPT_STEP ** -0.5)
F32 = jnp.float32
LANES, ROWS, WIDE = 128, 64, 32
VMEM_LIMIT = 60 * 10 ** 6

N_IN, N_B, N_OUT = 24, 18, 12
N_SUP = N_IN + N_B + N_OUT
FIRST_B, FIRST_IN, FIRST_OUT = 0, N_B, N_B + N_IN
N_QKV, N_O = 54, 18
N_MAT = N_QKV + N_O
N_OUT_B = 2
N_OUT_A = N_OUT - N_OUT_B
ROW_IN, ROW_OUT, ROW_B = 0, N_IN, 40
GROUPS = {'b': ('b', FIRST_B, N_B), 'in': ('in', FIRST_IN, N_IN), 'out_a': ('out', FIRST_OUT, N_OUT_A), 'out_b': ('out', FIRST_OUT + N_OUT_A, N_OUT_B)}
SIZES = (('b', (2, 4, 6, 6)), ('in', (6, 6, 6, 6)), ('out_a', (4, 4, 2)), ('out_b', (2,)))


def cut():
    chunks, at = [], 0
    for group, sizes in SIZES:
        for n in sizes:
            chunks.append((group, at, n))
            at += n
    return tuple(chunks)


CHUNKS = cut()
N_CH = len(CHUNKS)
LAST_CHUNK = {g: max(i for i, c in enumerate(CHUNKS) if c[0] == g) for g in GROUPS}
D2D, OPP_A, OPP_B, OWN_R, OWN_L, MRG_R, MRG_L = range(7)
SEND = (0, 1, 1, 2, 3, 2, 3)
OPP, LAST = 1, 2
RECV = (D2D, OPP, OPP, LAST, LAST, LAST, LAST)
SLOT = {'b': 0, 'in': 1, 'out_a': 2, 'out_b': 3, 'w': 4}
LANE_ROW = {'b': 0, 'in': N_IN, 'out_a': 48, 'out_b': 48 + N_OUT_A}
TAB_ROW = {'b': ROW_B, 'in': ROW_IN, 'out_a': ROW_OUT, 'out_b': ROW_OUT + N_OUT_A}
AHEAD, EARLY_OWN, LAG_MERGE, LAG_FINISH = 2, 3, 2, 3


def loop(n, body, unroll):
    lax.fori_loop(0, n, body, 0, unroll=unroll)


def kernel(n_data, n_model, gin_h, gout_h, gq_h, go_h, win_h, wout_h, wq_h, wo_h,
           row_in_h, col_in_h, row_out_h, col_out_h, row_q_h, col_q_h, row_o_h, col_o_h,
           w_in, w_out, w_q, w_o, row_in_o, col_in_o, row_out_o, col_out_o, row_q_o, col_q_o, row_o_o, col_o_o,
           row_in, col_in, row_out, col_out, row_q, col_q, row_o, col_o, lane_b, turn,
           gin, gout, gb, part, peer, opp_in, left_in, right_in, grad, w_all, ht,
           sum_b, sum_in, sum_a, sum_o, near_b, near_in, both_b, both_in, full_b, full_in, rlane, acc_t, comp_b, tab, rtab, rsub, wtab, vtab,
           mod_b, mod_in, mod_a, mod_o, mod_w, scal, dat_b, dat_in, dat_a, dat_o, got_b, got_in, got_a, got_o, got_w, got_s,
           pair_mom, raw_o, graw_o, wcol, krow,
           load_sem, w_sem, small_sem, first_sem, meet, snd, rcv, psnd, prcv, bsnd, brcv, dsnd, drcv, msnd, mrcv, ssnd, srcv):
    me = lax.axis_index('data')
    mod = lax.axis_index('model')
    n_chips = n_data // 2
    x, c = lax.div(me, 2), lax.rem(me, 2)
    xr, xl, xo = lax.rem(x + 1, n_chips), lax.rem(x + 3, n_chips), lax.rem(x + 2, n_chips)
    partner, right, left = 2 * x + 1 - c, 2 * xr + c, 2 * xl + c
    full = {'in': n_model * LANES, 'out': n_model * LANES, 'b': n_model * WIDE}
    lane_sum = {'b': sum_b, 'in': sum_in, 'out_a': sum_a, 'out_b': sum_o}
    near = {'b': near_b, 'in': near_in}
    both = {'b': both_b, 'in': both_in}
    whole = {'b': full_b, 'in': full_in}
    dat_got = {'b': dat_b, 'in': dat_in, 'out_a': dat_a, 'out_b': dat_o}
    mod_blk = {'b': mod_b, 'in': mod_in, 'out_a': mod_a, 'out_b': mod_o}
    mod_got = {'b': got_b, 'in': got_in, 'out_a': got_a, 'out_b': got_o}

    loads = [pltpu.make_async_copy(gq_h.at[pl.ds(0, 8)], gb.at[pl.ds(0, 8)], load_sem.at[0]),
             pltpu.make_async_copy(gq_h.at[pl.ds(8, 46)], gb.at[pl.ds(8, 46)], load_sem.at[1]),
             pltpu.make_async_copy(go_h, gb.at[pl.ds(N_QKV, N_O)], load_sem.at[2]),
             pltpu.make_async_copy(gin_h, gin, load_sem.at[3]),
             pltpu.make_async_copy(gout_h, gout, load_sem.at[4])]
    w_loads = [pltpu.make_async_copy(win_h, w_in, w_sem.at[0]),
               pltpu.make_async_copy(wout_h, w_out, w_sem.at[1]),
               pltpu.make_async_copy(wq_h, w_q, w_sem.at[2]),
               pltpu.make_async_copy(wo_h, w_o, w_sem.at[3])]
    small = [pltpu.make_async_copy(src, dst, small_sem.at[i]) for i, (src, dst) in enumerate((
        (row_in_h, row_in), (col_in_h, col_in), (row_out_h, row_out), (col_out_h, col_out),
        (row_q_h, row_q), (col_q_h, col_q), (row_o_h, row_o), (col_o_h, col_o)))]
    loads[0].start()

    barrier = pltpu.get_barrier_semaphore()

    def others(axis):
        side = 4 if axis == 'model' else 2
        n, rank = (n_model, mod) if axis == 'model' else (n_data, me)
        high, low, rows = lax.div(rank, side), lax.rem(rank, side), n // side

        def hops(d):
            up, over = d // side, d % side
            return min(up, rows - up) * (side - 1) + min(over, side - over)

        for d in sorted(range(1, n), key=lambda d: -hops(d)):
            if axis != 'chip' or d % side == 0:
                yield lax.rem(high + d // side, rows) * side + lax.rem(low + d % side, side)

    side = 4
    z, y = lax.div(mod, side), lax.rem(mod, side)
    neighbours = [('data', who) for who in (partner, right, left)]
    for step in (1, side - 1):
        neighbours.append(('model', side * z + lax.rem(y + step, side)))
        neighbours.append(('model', side * lax.rem(z + step, n_model // side) + y))

    def greet(sem):
        for axis, who in neighbours:
            pl.semaphore_signal(sem, inc=1, device_id={axis: who}, device_id_type=pl.DeviceIdType.MESH)

    greet(barrier)
    for cp in loads[1:]:
        cp.start()

    def remote(src, dst, ssem, rsem, axis, who):
        return pltpu.make_async_remote_copy(src_ref=src, dst_ref=dst, send_sem=ssem, recv_sem=rsem,
                                            device_id={axis: who}, device_id_type=pl.DeviceIdType.MESH)

    def transfer(kind, ch):
        _, b0, n = CHUNKS[ch]
        n_a = n // 2
        every, half_a, half_b = pl.ds(b0, n), pl.ds(b0, n_a), pl.ds(b0 + n_a, n - n_a)
        src, dst, who = {
            D2D: lambda: (part.at[1 - c, :, every], peer.at[:, every], partner),
            OPP_A: lambda: (part.at[c, xo, half_a], opp_in.at[half_a], right),
            OPP_B: lambda: (part.at[c, xo, half_b], opp_in.at[half_b], left),
            OWN_R: lambda: (part.at[c, xr, half_b], left_in.at[half_b], right),
            OWN_L: lambda: (part.at[c, xl, half_a], right_in.at[half_a], left),
            MRG_R: lambda: (part.at[c, xr, half_a], left_in.at[half_a], right),
            MRG_L: lambda: (part.at[c, xl, half_b], right_in.at[half_b], left),
        }[kind]()
        return remote(src, dst, snd.at[SEND[kind]], rcv.at[RECV[kind], ch], 'data', who)

    def convert(ch):
        group, b0, n = CHUNKS[ch]
        family = GROUPS[group][0]
        if ch == 0:
            loads[0].wait()
        elif ch == 1:
            loads[1].wait()
            loads[2].wait()
        elif b0 == FIRST_IN:
            loads[3].wait()
        elif b0 == FIRST_OUT:
            loads[4].wait()

        def body(i, carry):
            b = b0 + i
            for t in range(n_chips):
                if family == 'in':
                    tile = gin[b - FIRST_IN, pl.ds(LANES * t, LANES), :].astype(F32)
                elif family == 'out':
                    tile = gout[b - FIRST_OUT, :, pl.ds(LANES * t, LANES)].astype(F32).T
                else:
                    four = gb[pl.ds(4 * (b - FIRST_B), 4), :, pl.ds(LANES * t, LANES)].astype(F32)
                    tile = four.reshape(LANES, LANES).T
                part[0, t, b] = tile[:ROWS]
                part[1, t, b] = tile[ROWS:]
            return carry

        lax.fori_loop(0, n, body, 0)

    def first_pair(dest, sem):
        every = pl.ds(0, CHUNKS[0][2])
        return remote(part.at[1 - c, dest, every], peer.at[dest, every], snd.at[0], sem, 'data', partner)

    def first_pairs():
        first_pair(xo, first_sem.at[0]).start()
        for dest in (xr, xl, x):
            first_pair(dest, rcv.at[D2D, 0]).start()

    def add_peer(ch, dest):
        _, b0, n = CHUNKS[ch]

        def body(i, carry):
            b = b0 + i
            part[c, dest, b] = part[c, dest, b] + peer[dest, b]
            return carry
        loop(n, body, 2)

    def opposite(ch):
        if ch == 0:
            first_pair(xo, first_sem.at[0]).wait_recv()
        else:
            transfer(D2D, ch).wait_recv()
        add_peer(ch, xo)
        transfer(OPP_A, ch).start()
        transfer(OPP_B, ch).start()
        if ch == 0:
            rest = peer.at[pl.ds(0, n_chips - 1), pl.ds(0, CHUNKS[0][2])]
            remote(rest, rest, snd.at[0], rcv.at[D2D, 0], 'data', partner).wait_recv()
        add_peer(ch, xr)
        add_peer(ch, xl)
        if ch < EARLY_OWN:
            own(ch)
        add_peer(ch, x)

    def own(ch):
        transfer(OWN_R, ch).start()
        transfer(OWN_L, ch).start()

    def merge(ch):
        _, b0, n = CHUNKS[ch]
        n_a = n // 2

        def add(dest, lo, hi):
            def body(b, carry):
                part[c, dest, b] = part[c, dest, b] + opp_in[b]
                return carry
            lax.fori_loop(lo, hi, body, 0)

        every = opp_in.at[pl.ds(b0, n)]
        remote(every, every, snd.at[1], rcv.at[OPP, ch], 'data', left).wait_recv()
        add(xr, b0, b0 + n_a)
        transfer(MRG_R, ch).start()
        add(xl, b0 + n_a, b0 + n)
        transfer(MRG_L, ch).start()
        if ch >= EARLY_OWN:
            own(ch)

    lane_iota = lax.broadcasted_iota(jnp.int32, (ROWS, LANES), 1)

    def row_sums(first, second):
        return jnp.sum(jnp.concatenate([first, second], axis=0).T, axis=0, keepdims=True)

    def finish(ch):
        group, b0, n = CHUNKS[ch]
        family, g0, _ = GROUPS[group]
        every = pl.ds(b0, n)
        two = peer.at[pl.ds(0, 2), every]
        remote(two, two, snd.at[2], rcv.at[LAST, ch], 'data', right).wait_recv()

        def block(b):
            g = (part[c, x, b] + left_in[b] + right_in[b]) * (1.0 / n_data)
            grad[b] = g
            sq = g * g + EPS_SQ
            sums = jnp.sum(sq, axis=0, keepdims=True)
            if group in near:
                half = lane_sum[group].shape[1]
                lane_sum[group][lax.div(b - g0, half), pl.ds(lax.rem(b - g0, half), 1), :] = sums
            else:
                lane_sum[group][pl.ds(b - g0, 1), :] = sums
            return g, sq

        if family == 'b':
            def body(i, carry):
                b = b0 + i
                g, _ = block(b)
                gt = g.T
                st = (gt * gt + EPS_SQ).reshape(4, WIDE, ROWS)
                comp_b[pl.ds(b - FIRST_B, 1), :, :ROWS] = jnp.sum(st, axis=1)[None]
                return carry
            loop(n, body, 2)
        elif group == 'out_b':
            first, second = (block(b0 + i)[1] for i in range(N_OUT_B))
            lane_start(group)
            mod_o[:1, :] = row_sums(first, second)
        else:
            which = 0 if family == 'in' else 1

            def body(i, acc):
                b = b0 + i
                _, sq = block(b)
                return jnp.where(lane_iota == b - (FIRST_IN if family == 'in' else FIRST_OUT), jnp.sum(sq, axis=1, keepdims=True), acc)
            acc_t[which] = lax.fori_loop(0, n, body, acc_t[which], unroll=2)

    def gather(src, dst, sems, slot, axis, op):
        send, recv = sems[0].at[slot], sems[1].at[slot]
        rank, n = {'data': (me, n_data), 'model': (mod, n_model), 'chip': (x, n_chips)}[axis]
        mesh_axis = 'model' if axis == 'model' else 'data'
        if op == 'start':
            dst[rank] = src[...]
            for who in others(axis):
                remote(src, dst.at[rank], send, recv, mesh_axis, who).start()
            return
        rest = dst.at[pl.ds(0, n - 1)]
        done = remote(rest, rest, send, recv, mesh_axis, partner if mesh_axis == 'data' else mod)
        if op == 'recv':
            done.wait_recv()
        else:
            done.wait_send()

    def total(dst, n):
        acc = dst[0]
        for r in range(1, n):
            acc = acc + dst[r]
        return acc

    d_sems, m_sems, s_sems = (dsnd, drcv), (msnd, mrcv), (ssnd, srcv)

    def pair_ex(group):
        i = SLOT[group]
        return remote(lane_sum[group], near[group], psnd.at[i], prcv.at[i], 'data', partner)

    def lane_ex(group, op):
        pairs = group in near
        gather(both[group].at[c] if pairs else lane_sum[group], dat_got[group], d_sems, SLOT[group], 'chip' if pairs else 'data', op)

    def back_ex(group):
        i = SLOT[group]
        return remote(whole[group].at[c], whole[group].at[c], bsnd.at[i], brcv.at[i], 'data', partner)

    def lane_back(group):
        lane_ex(group, 'recv')
        whole[group][c] = total(dat_got[group], n_chips)
        back_ex(group).start()

    def lane_start(group):
        if group in near:
            pair_ex(group).start()
        else:
            lane_ex(group, 'start')

    def lane_pair(group):
        pair_ex(group).wait_recv()
        both[group][...] = lane_sum[group][...] + near[group][...]
        lane_ex(group, 'start')

    def model_ex(group, op):
        gather(mod_blk[group], mod_got[group], m_sems, SLOT[group], 'model', op)

    def scal_ex(name, op):
        i = SLOT[name]
        src, dst = (raw_o, graw_o) if name == 'out_b' else (scal.at[i], got_s.at[i])
        gather(src, dst, s_sems, i, 'data', op)

    def weights_start():
        for cp in w_loads + small:
            cp.wait()
        turn[...] = jnp.zeros_like(turn)
        turn[:WIDE, :N_QKV] = col_q[...]
        turn[...] = turn[...].T
        turn[N_QKV:N_QKV + N_O, :WIDE] = row_o[...]
        row = turn[pl.ds(0, N_B, stride=4), :]
        for q in range(1, 4):
            row = row + pltpu.roll(turn[pl.ds(q, N_B, stride=4), :], WIDE * q, 1)
        lane_b[...] = row
        wtab[...] = jnp.zeros_like(wtab)
        vtab[...] = jnp.zeros_like(vtab)

        def squares(ref, row, width):
            def body(b, carry):
                w = ref[b]
                wtab[pl.ds(row + b, 1), 0:width] = jnp.sum(w * w, axis=0, keepdims=True)
                return carry
            loop(ref.shape[0], body, 6)

        squares(w_in, ROW_IN, LANES)
        squares(w_out, ROW_OUT, LANES)
        squares(w_q, ROW_B, ROWS)
        squares(w_o, ROW_B + N_QKV, ROWS)
        vtab[ROW_OUT:ROW_OUT + N_OUT, :] = row_out[...]
        vtab[ROW_B + N_QKV:ROW_B + N_MAT, :WIDE] = row_o[...]
        mod_w[:1, :] = jnp.sum(wtab[...].T, axis=0, keepdims=True)
        mod_w[1:2, :] = jnp.sum(vtab[...].T, axis=0, keepdims=True) / n_data
        gather(mod_w, got_w, m_sems, SLOT['w'], 'model', 'start')

    def weights_next():
        gather(mod_w, got_w, m_sems, SLOT['w'], 'model', 'recv')
        scal[SLOT['w']] = total(got_w, n_model)
        scal_ex('w', 'start')

    def weights_done():
        scal_ex('w', 'recv')
        w_all[...] = total(got_s.at[SLOT['w']], n_data)
        turn[:2, :] = w_all[...]
        wcol[...] = turn[...].T

    def after_lanes(group):
        family, g0, n = GROUPS[group]
        r0 = LANE_ROW[group]
        if group in near:
            back_ex(group).wait_recv()
            sums = jnp.concatenate([whole[group][0], whole[group][1]], axis=0)
        else:
            lane_ex(group, 'recv')
            sums = total(dat_got[group], n_data)
        lo = g0 - (FIRST_OUT if family == 'out' else g0)
        if family == 'b':
            mom = lane_b[...]
        else:
            mom = (col_in if family == 'in' else row_out)[lo:lo + n, :]
        new = BETA_TWO * mom + GAIN * (sums / 512.0)
        rlane[r0:r0 + n, :] = lax.rsqrt(new)
        if family == 'b':
            def body(s, carry):
                h = grad[FIRST_B + s] * rlane[pl.ds(r0 + s, 1), :]
                t = h.T.reshape(4, WIDE, ROWS)
                ht[pl.ds(4 * s, 4)] = t
                comp_b[pl.ds(s, 1), :, ROWS:LANES] = jnp.sum(t * t, axis=1)[None]
                return carry
            loop(n, body, 3)
            mod_b[...] = comp_b[...].reshape(4 * N_B, LANES)
        else:
            def body(b, acc):
                h = grad[g0 + b] * rlane[pl.ds(r0 + b, 1), :]
                grad[g0 + b] = h
                return jnp.where(lane_iota == lo + b, jnp.sum(h * h, axis=1, keepdims=True), acc)
            acc_z = lax.fori_loop(0, n, body, jnp.zeros((ROWS, LANES), F32), unroll=4)
            turned = jnp.concatenate([acc_t[0 if family == 'in' else 1], acc_z], axis=0).T
            mod_blk[group][...] = turned[lo:lo + n]
        model_ex(group, 'start')
        if family == 'b':
            turn[...] = jnp.zeros_like(turn)
            for q in range(4):
                turn[pl.ds(q, N_B, stride=4), :] = pltpu.roll(new, (LANES - WIDE * q) % LANES, 1)
            row_o_o[...] = turn[N_QKV:N_QKV + N_O, :WIDE]
            turn[...] = turn[...].T
            col_q_o[...] = turn[:WIDE, :N_QKV]
        else:
            (col_in_o if family == 'in' else row_out_o)[lo:lo + n, :] = new

    def after_model(group):
        family, g0, n = GROUPS[group]
        lo = g0 - (FIRST_OUT if family == 'out' else g0)
        model_ex(group, 'recv')
        sums_z = total(mod_got[group], n_model)
        sums, z = sums_z[:, :ROWS], sums_z[:, ROWS:LANES]
        if family == 'b':
            mom = jnp.concatenate([row_q[...], col_o[...]], axis=0)
        else:
            mom = (row_in if family == 'in' else col_out)[lo:lo + n, :]
        new = BETA_TWO * mom + GAIN * (sums / full[family])
        mean_part = GAIN * (sums / 512.0)
        if family == 'in':
            term = new
        elif family == 'out':
            term = mean_part
        else:
            term = jnp.where(lax.broadcasted_iota(jnp.int32, new.shape, 0) < N_QKV, new, mean_part)
        r0 = TAB_ROW[group]
        r1 = r0 + new.shape[0]
        tab[r0:r1, :ROWS] = z / new
        tab[r0:r1, ROWS:LANES] = term
        rtab[r0:r1, :ROWS] = lax.rsqrt(new)
        if family == 'b':
            row_q_o[...] = new[:N_QKV]
            col_o_o[...] = new[N_QKV:]
        else:
            (row_in_o if family == 'in' else col_out_o)[lo:lo + n, :] = new

    def scalars_start(family):
        e = SLOT[family]
        turned = tab[...].T
        scal[e, :1, :] = jnp.sum(turned[:ROWS], axis=0, keepdims=True)
        scal[e, 1:2, :] = jnp.sum(turned[ROWS:], axis=0, keepdims=True)
        scal_ex(family, 'start')

    def factor(q, s, w, v, family):
        rows = 512.0 if family == 'in' else float(full[family])
        size = 512.0 * full[family]
        m = (s if family == 'in' else BETA_TWO * v + s) / rows
        return jnp.sqrt(m) * (LR_BASE * jnp.maximum(1e-3, jnp.sqrt(w / size))) / jnp.maximum(1.0, jnp.sqrt(m * q / size))

    def after_scalars(family):
        e = SLOT[family]
        scal_ex(family, 'recv')
        tot = total(got_s.at[e], n_data)
        scale = factor(tot[:1], tot[1:2], w_all[:1, :], w_all[1:2, :], family)
        if family == 'b':
            turn[...] = jnp.broadcast_to(scale, (LANES, LANES)).T
            rtab[ROW_B:ROW_B + N_MAT, :ROWS] = rtab[ROW_B:ROW_B + N_MAT, :ROWS] * turn[ROW_B:ROW_B + N_MAT, :ROWS]
            for ref, b0 in ((w_q, 0), (w_o, N_QKV)):
                def body(b, carry, ref=ref, b0=b0):
                    ref[b] = ref[b] - ht[b0 + b] * rtab[pl.ds(ROW_B + b0 + b, 1), :ROWS]
                    return carry
                loop(ref.shape[0], body, 6)
        else:
            krow[...] = jnp.broadcast_to(scale, (LANES, LANES)).T

            def body(b, carry):
                w_in[b] = w_in[b] - grad[FIRST_IN + b] * krow[pl.ds(ROW_IN + b, 1), :]
                return carry
            loop(N_IN, body, 4)

    def prepare():
        fac = rtab[:, :ROWS].T

        for g0, r0, n in ((FIRST_OUT, ROW_OUT, N_OUT), (FIRST_IN, ROW_IN, N_IN)):
            def body(b, carry, g0=g0, r0=r0):
                f = jnp.sum(jnp.where(lane_iota == r0 + b, fac, 0.0), axis=1, keepdims=True)
                grad[g0 + b] = grad[g0 + b] * f
                return carry
            loop(n, body, 4)

    def apply_out(group):
        _, g0, n = GROUPS[group]
        lo, r0, e = g0 - FIRST_OUT, TAB_ROW[group], SLOT[group]
        scal_ex(group, 'recv')
        tot = total(got_s.at[e], n_data)
        scale = factor(tot[:1], tot[1:2], w_all[:1, :], w_all[1:2, :], 'out')
        krow[...] = jnp.broadcast_to(scale, (LANES, LANES)).T
        for b in range(lo, lo + n):
            w_out[b] = w_out[b] - grad[FIRST_OUT + b] * krow[r0 + b - lo:r0 + b - lo + 1, :]

    def last_lanes():
        _, g0, n = GROUPS['out_b']
        lo = g0 - FIRST_OUT
        lane_ex('out_b', 'recv')
        new = BETA_TWO * row_out[lo:lo + n, :] + GAIN * (total(dat_o, n_data) / 512.0)
        r = lax.rsqrt(new)
        first, second = grad[g0] * r[:1], grad[g0 + 1] * r[1:2]
        mod_o[1:2, :] = row_sums(first * first, second * second)
        model_ex('out_b', 'start')
        grad[g0], grad[g0 + 1] = first, second
        row_out_o[lo:lo + n, :] = new
        pair_mom[:1, :ROWS] = col_out[lo:lo + 1, :]
        pair_mom[:1, ROWS:LANES] = col_out[lo + 1:lo + 2, :]

    def last_model():
        lo, r0 = GROUPS['out_b'][1] - FIRST_OUT, TAB_ROW['out_b']
        model_ex('out_b', 'recv')
        sums_z = total(got_o, n_model)
        sums, z = sums_z[:1], sums_z[1:2]
        new = BETA_TWO * pair_mom[...] + GAIN * (sums / full['out'])
        raw_o[:1, :] = z / new
        raw_o[1:2, :] = GAIN * (sums / 512.0)
        scal_ex('out_b', 'start')
        root = lax.rsqrt(new)
        for i in range(N_OUT_B):
            own_lanes = slice(ROWS * i, ROWS * i + ROWS)
            rtab[r0 + i:r0 + i + 1, :ROWS] = root[:, own_lanes]
            col_out_o[lo + i:lo + i + 1, :] = new[:, own_lanes]

    def last_apply():
        _, g0, n = GROUPS['out_b']
        lo, r0 = g0 - FIRST_OUT, TAB_ROW['out_b']
        mine = lax.div(lax.broadcasted_iota(jnp.int32, (n, LANES), 1), ROWS) == lax.broadcasted_iota(jnp.int32, (n, LANES), 0)
        scal_ex('out_b', 'recv')
        tot = total(graw_o, n_data)
        q = jnp.sum(jnp.where(mine, tot[:1], 0.0), axis=1, keepdims=True)
        s = jnp.sum(jnp.where(mine, tot[1:2], 0.0), axis=1, keepdims=True)
        scale = factor(q, s, wcol[r0:r0 + n, :1], wcol[r0:r0 + n, 1:2], 'out')
        for i in range(n):
            w_out[lo + i] = w_out[lo + i] - grad[g0 + i] * scale[i:i + 1]

    def sent_early():
        for i, ref in enumerate((peer, opp_in, left_in, right_in)):
            remote(ref, ref, snd.at[i], rcv.at[0, 0], 'data', partner).wait_send()
        gather(mod_w, got_w, m_sems, SLOT['w'], 'model', 'send')
        for group in near:
            pair_ex(group).wait_send()
            back_ex(group).wait_send()
        for group in GROUPS:
            lane_ex(group, 'send')
        model_ex('b', 'send')
        scal_ex('w', 'send')
        scal_ex('b', 'send')

    def sent_mid():
        for group in ('in', 'out_a', 'out_b'):
            model_ex(group, 'send')
        scal_ex('in', 'send')
        scal_ex('out_a', 'send')

    def sent_late():
        scal_ex('out_b', 'send')

    acc_t[...] = jnp.zeros_like(acc_t)
    tab[...] = jnp.zeros_like(tab)
    rtab[...] = jnp.zeros_like(rtab)

    convert(0)
    for cp in small + w_loads:
        cp.start()
    pl.semaphore_wait(barrier, len(neighbours))
    first_pairs()
    greet(meet.at[0])
    last = N_CH - 1 + LAG_FINISH
    steps = {}

    def at(k, do, *args):
        steps.setdefault(k, []).append((do, args))

    def pass_on(i):
        pl.semaphore_wait(meet.at[i], len(neighbours))
        if i < 2:
            greet(meet.at[i + 1])

    at(2, pass_on, 0)
    at(3, pass_on, 1)
    at(4, pass_on, 2)
    at(4, weights_start)
    at(6, weights_next)
    at(8, weights_done)
    k_b, k_in, k_a = (LAST_CHUNK[g] + LAG_FINISH for g in ('b', 'in', 'out_a'))
    at(k_b + 1, lane_pair, 'b')
    at(k_b + 3, lane_back, 'b')
    at(k_b + 4, after_lanes, 'b')
    at(k_b + 6, after_model, 'b')
    at(k_b + 6, scalars_start, 'b')
    at(k_in + 1, lane_pair, 'in')
    at(k_in + 3, lane_back, 'in')
    tail = ((after_lanes, 'in'), (after_lanes, 'out_a'), (last_lanes,), (after_scalars, 'b'), (sent_early,), (after_model, 'in'),
            (scalars_start, 'in'), (after_model, 'out_a'), (scalars_start, 'out_a'), (last_model,), (prepare,), (sent_mid,), (after_scalars, 'in'),
            (apply_out, 'out_a'), (last_apply,), (sent_late,))
    for k in range(1 - AHEAD, last + 1):
        if 0 <= k < N_CH:
            opposite(k)
        if k + AHEAD < N_CH:
            convert(k + AHEAD)
            transfer(D2D, k + AHEAD).start()
        for ch in range(N_CH):
            if k == ch + (LAG_MERGE if ch < N_CH - 1 else 1):
                merge(ch)
        for do, args in steps.get(k, ()):
            do(*args)
        if 0 <= k - LAG_FINISH < N_CH:
            finish(k - LAG_FINISH)
        for group in GROUPS:
            if k == LAST_CHUNK[group] + LAG_FINISH and group != 'out_b':
                lane_start(group)
    for do, *args in tail:
        do(*args)


def deliver(*refs):
    srcs, dsts, sem = refs[:12], refs[12:N_IN], refs[N_IN]
    copies = [pltpu.make_async_copy(src, dst, sem.at[i]) for i, (src, dst) in enumerate(zip(srcs, dsts))]
    for cp in copies:
        cp.start()
    for cp in copies:
        cp.wait()


def solution(mesh):
    axis_sizes = dict(mesh.shape)
    n_data, n_model = axis_sizes['data'], axis_sizes['model']
    n_chips = n_data // 2
    rows_data = (P('data', None, None, 'model'), P(None, 'data', 'model'), P(None, 'data'), P(None, 'model'))
    rows_model = (P('data', None, 'model', None), P(None, 'model', 'data'), P(None, 'model'), P(None, 'data'))

    def vmem(*dims):
        return pltpu.VMEM(dims, F32)

    small = (vmem(N_IN, ROWS), vmem(N_IN, LANES), vmem(12, LANES), vmem(12, ROWS), vmem(N_QKV, ROWS), vmem(WIDE, N_QKV), vmem(N_O, WIDE), vmem(N_O, ROWS))
    results = (vmem(N_IN, ROWS, LANES), vmem(12, ROWS, LANES), vmem(N_QKV, WIDE, ROWS), vmem(N_O, WIDE, ROWS), *small)
    scratch = [
        *small, vmem(N_B, LANES), vmem(LANES, LANES),
        pltpu.VMEM((N_IN, 512, LANES), jnp.bfloat16), pltpu.VMEM((12, LANES, 512), jnp.bfloat16),
        pltpu.VMEM((N_MAT, WIDE, 512), jnp.bfloat16),
        vmem(2, n_chips, N_SUP, ROWS, LANES), vmem(n_chips, N_SUP, ROWS, LANES),
        vmem(N_SUP, ROWS, LANES), vmem(N_SUP, ROWS, LANES), vmem(N_SUP, ROWS, LANES), vmem(N_SUP, ROWS, LANES),
        vmem(2, LANES), vmem(N_MAT, WIDE, ROWS),
        vmem(2, 9, LANES), vmem(2, 12, LANES), vmem(N_OUT_A, LANES), vmem(N_OUT_B, LANES),
        *(vmem(2, n, LANES) for n in (9, 12, 9, 12, 9, 12)),
        vmem(ROWS, LANES), vmem(2, ROWS, LANES), vmem(N_B, 4, LANES),
        vmem(LANES, LANES), vmem(LANES, LANES), vmem(ROWS, LANES), vmem(LANES, LANES), vmem(LANES, LANES),
        vmem(N_MAT, LANES), vmem(N_IN, LANES), vmem(N_OUT_A, LANES), vmem(N_OUT_B, LANES), vmem(2, LANES), vmem(5, 2, LANES),
        vmem(n_chips, 9, LANES), vmem(n_chips, 12, LANES), vmem(n_data, N_OUT_A, LANES), vmem(n_data, N_OUT_B, LANES),
        vmem(n_model, N_MAT, LANES), vmem(n_model, N_IN, LANES), vmem(n_model, N_OUT_A, LANES), vmem(n_model, N_OUT_B, LANES),
        vmem(n_model, 2, LANES), vmem(5, n_data, 2, LANES),
        vmem(1, LANES), vmem(N_OUT_B, LANES), vmem(n_data, N_OUT_B, LANES), vmem(LANES, LANES), vmem(LANES, LANES),
        pltpu.SemaphoreType.DMA((5,)), pltpu.SemaphoreType.DMA((4,)), pltpu.SemaphoreType.DMA((8,)), pltpu.SemaphoreType.DMA((1,)),
        pltpu.SemaphoreType.REGULAR((3,)),
        pltpu.SemaphoreType.DMA((4,)), pltpu.SemaphoreType.DMA((3, N_CH)),
        *(pltpu.SemaphoreType.DMA((n,)) for n in (2, 2, 2, 2, 4, 4, 5, 5, 5, 5)),
    ]
    hbm, in_vmem = pl.BlockSpec(memory_space=pltpu.HBM), pl.BlockSpec(memory_space=pltpu.VMEM)

    def step_all(grad_in, w_in, row_in, col_in, grad_out, w_out, row_out, col_out,
                 grad_qkv, w_qkv, row_qkv, col_qkv, grad_o, w_o, row_o, col_o):
        kept = pl.pallas_call(
            functools.partial(kernel, n_data, n_model),
            name='adafactor_step',
            out_shape=results,
            in_specs=[hbm] * 16,
            out_specs=[in_vmem] * 12,
            scratch_shapes=scratch,
            compiler_params=pltpu.CompilerParams(collective_id=0, has_side_effects=True, vmem_limit_bytes=VMEM_LIMIT),
        )(grad_in[0], grad_out[0], grad_qkv[0].transpose(0, 2, 1), grad_o[0],
          w_in, w_out.transpose(0, 2, 1), w_qkv.transpose(0, 2, 1), w_o,
          row_in, col_in, row_out, col_out, row_qkv, col_qkv.T, row_o, col_o)
        (w_in_new, w_out_new, w_qkv_new, w_o_new, row_in_new, col_in_new, row_out_new, col_out_new,
         row_qkv_new, col_qkv_new, row_o_new, col_o_new) = pl.pallas_call(
            deliver,
            name='deliver',
            out_shape=[jax.ShapeDtypeStruct(r.shape, F32) for r in results],
            in_specs=[in_vmem] * 12,
            out_specs=[hbm] * 12,
            scratch_shapes=[pltpu.SemaphoreType.DMA((12,))],
            compiler_params=pltpu.CompilerParams(vmem_limit_bytes=10 ** 6),
        )(*(pltpu.with_memory_space_constraint(a, pltpu.VMEM) for a in kept))
        return (w_in_new, row_in_new, col_in_new, w_out_new.transpose(0, 2, 1), row_out_new, col_out_new,
                w_qkv_new.transpose(0, 2, 1), row_qkv_new, col_qkv_new.T, w_o_new, row_o_new, col_o_new)

    in_specs = rows_data + rows_model + rows_data + rows_model
    out_specs = rows_data[1:] + rows_model[1:] + rows_data[1:] + rows_model[1:]
    return jax.shard_map(step_all, mesh=mesh, in_specs=in_specs, out_specs=out_specs, check_vma=False)
```
